128 devices in a mesh: gx: 2 (over core), gy: 4 (over x), gz: 16 (over z, y).
Axes of the slice: x: 4, y: 4, z: 4, core: 2. Of those that a mesh axis runs over, the one named last changes fastest.
Arguments:
- permanent_field: float32 [12, 24, 96, 3], P('gx', 'gy', 'gz'), may hold values from -6 to 6
- polar: float32 [12, 24, 96], P('gx', 'gy', 'gz'), may hold values from 0.4 to 1.4
- jitter: float32 [12, 24, 96, 3], P('gx', 'gy', 'gz'), may hold values from -0.2 to 0.2
- neighbors: int32 [12, 24, 96, 56], P('gx', 'gy', 'gz'), may hold values from -1 to 987, as said below
Outputs:
- dipoles: float32 [12, 24, 96, 3], P('gx', 'gy', 'gz')
- residual: float32 [12, 24, 96, 3], P('gx', 'gy', 'gz')
- step_lengths: float32 [8], replicated
The draws below stay inside these ranges and needn't reach their ends.
Inputs may be any that keep to these rules, and one draw needn't show every extreme that they name: `neighbors`: each entry is -1 or the flat index of a neighbour in the device's block extended by two sites on every side, with an offset d of squared length 1 to 5 (each component -2 to 2), each offset at most once in a row; the -1 entries come after all others; if site j stands in site i's row with offset d then i stands in j's row with offset -d, the box being periodic.
All inputs are finite; a program needn't handle non-finite values.
Results may differ from the reference program's by a relative error of at most 0.0003.
Values sent between devices are 32-bit elements.
No kernel may reach another device: no remote copies, remote signals or barrier semaphores. Data moves between devices by JAX's collectives and lax.ppermute only.
A program may use at most 64 MiB of HBM per device.

```python
import math
import jax
import jax.numpy as jnp
from jax import lax

EDGE = 6
ITERS = 8
LX = 12
LY = 24
LZ = 96


def stencil_offsets():
    listed = []
    for shift_x in range(-2, 3):
        for shift_y in range(-2, 3):
            for shift_z in range(-2, 3):
                length = shift_x * shift_x + shift_y * shift_y + shift_z * shift_z
                if 1 <= length <= 5:
                    listed.append((shift_x, shift_y, shift_z))
    return listed


def draw_neighbors(key, part):
    listed = stencil_offsets()
    forward = [offset for offset in listed if offset > (0, 0, 0)]
    coin_bits = jax.random.randint(key, (LX, LY, LZ, len(forward)), 0, 4)
    bonded = (coin_bits < 3).astype(jnp.int32)
    padded_edge = EDGE + 4
    home_x = lax.broadcasted_iota(jnp.int32, (LX, LY, LZ), 0) % EDGE
    home_y = lax.broadcasted_iota(jnp.int32, (LX, LY, LZ), 1) % EDGE
    home_z = lax.broadcasted_iota(jnp.int32, (LX, LY, LZ), 2) % EDGE
    bond_flags = []
    places = []
    for offset in listed:
        if offset > (0, 0, 0):
            bond_flags.append(bonded[..., forward.index(offset)])
        else:
            mirror = (-offset[0], -offset[1], -offset[2])
            bond_flags.append(jnp.roll(bonded[..., forward.index(mirror)], mirror, axis=(0, 1, 2)))
        places.append(((home_x + 2 + offset[0]) * padded_edge + home_y + 2 + offset[1]) * padded_edge + home_z + 2 + offset[2])
    flagged = jnp.stack(bond_flags, axis=-1)
    located = jnp.stack(places, axis=-1)
    ranking = (1 - flagged) * 64 + lax.broadcasted_iota(jnp.int32, flagged.shape, 3)
    ordering = jnp.argsort(ranking, axis=-1, stable=True)
    flagged = jnp.take_along_axis(flagged, ordering, axis=-1)
    located = jnp.take_along_axis(located, ordering, axis=-1)
    return jnp.where(flagged == 1, located, -1).astype(jnp.int32)


def block_levels(own_key, dims, cuts, smallest, high):
    def one(dim, shards_of):
        steps = jax.random.uniform(jax.random.fold_in(jax.random.fold_in(own_key, 6), dim), (shards_of,), jnp.float32, smallest / len(cuts), high / len(cuts))
        return jnp.repeat(jnp.exp(steps), dims[dim] // shards_of).reshape((-1,) + (1,) * (len(dims) - dim - 1))

    factor_of = one(*cuts[0])
    for cut in cuts[1:]:
        factor_of = factor_of * one(*cut)
    return factor_of


def gaussian(rng, shape, width, most, pieces=(), kind=jnp.bfloat16):
    factor_of = block_levels(rng, shape, pieces, -0.22, 0.18) if pieces else 1.0
    result = jax.random.normal(rng, shape, jnp.float32) * width * factor_of
    return jnp.minimum(jnp.maximum(result, -most), most).astype(kind)


def setup_inputs(seed: int = 0) -> dict:
    key_of = jax.random.split(jax.random.key(seed), 5)
    return {
        "permanent_field": gaussian(key_of[0], (LX, LY, LZ, 3), 1.0, 6.0, ((0, 2), (1, 4), (2, 16)), jnp.float32),
        "polar": jnp.clip(jnp.exp(math.log(1.4) - 1.2527629 * jax.random.uniform(key_of[1], (LX, LY, LZ), jnp.float32) ** block_levels(key_of[1], (LX, LY, LZ), ((0, 2), (1, 4), (2, 16)), -0.2, 0.2)), 0.4, 1.4),
        "jitter": jnp.clip(jax.random.uniform(key_of[2], (LX, LY, LZ, 3), jnp.float32, -0.2, 0.2) * block_levels(key_of[2], (LX, LY, LZ, 3), ((0, 2), (1, 4), (2, 16)), -0.4, 0.0), -0.2, 0.2),
        "neighbors": draw_neighbors(jax.random.fold_in(key_of[4], 71), 0),
    }


thole_damping = 0.39
site_spacing = 3.5

def geometry(offsets, jit_self, jit_other, pol_self, pol_other, present):
    separation = (offsets + jit_other - jit_self) * site_spacing
    separation = jnp.where(present[..., None], separation, site_spacing)
    dist_sq = lax.optimization_barrier(jnp.sum(separation * separation, axis=-1))
    distance = jnp.sqrt(dist_sq)
    dist_cube = dist_sq * distance
    damping = thole_damping * dist_cube / jnp.sqrt(pol_self * pol_other)
    falloff = jnp.exp(-damping)
    lam_three = 1.0 - falloff
    lam_five = 1.0 - (1.0 + damping) * falloff
    isotropic = jnp.where(present, lam_three / dist_cube, 0.0)
    radial = jnp.where(present, 3.0 * lam_five / (dist_cube * dist_sq), 0.0)
    return (separation, isotropic, radial)

def couple(separation, isotropic, radial, values):
    projection = lax.optimization_barrier(jnp.sum(separation * values, axis=-1, keepdims=True))
    return lax.optimization_barrier(jnp.sum(radial[..., None] * projection * separation - isotropic[..., None] * values, axis=-2))

def reference(permanent_field, polar, jitter, neighbors):
    padded_edge = EDGE + 4
    flat_jit = jitter.reshape(-1, 3)
    flat_pol = polar.reshape(-1)

    def slab_geometry(inputs):
        row, links, jit_row, pol_row = inputs
        present = links >= 0
        clipped = jnp.where(present, links, 0)
        plane_a = clipped // (padded_edge * padded_edge)
        plane_b = clipped // padded_edge % padded_edge
        plane_c = clipped % padded_edge
        grid_y = lax.broadcasted_iota(jnp.int32, (LY, LZ, 1), 0)
        grid_z = lax.broadcasted_iota(jnp.int32, (LY, LZ, 1), 1)
        shift_x = plane_a - 2 - row % EDGE
        shift_y = plane_b - 2 - grid_y % EDGE
        shift_z = plane_c - 2 - grid_z % EDGE
        other_x = (row + shift_x) % LX
        other_y = (grid_y + shift_y) % LY
        other_z = (grid_z + shift_z) % LZ
        other = ((other_x * LY + other_y) * LZ + other_z).astype(jnp.int32)
        offsets = jnp.stack([shift_x, shift_y, shift_z], axis=-1).astype(jnp.float32)
        separation, isotropic, radial = geometry(offsets, jit_row[:, :, None, :], flat_jit[other], pol_row[:, :, None], flat_pol[other], present)
        return (separation, isotropic, radial, other)
    rows = jnp.arange(LX, dtype=jnp.int32)
    separations, isotropics, radials, others = lax.map(slab_geometry, (rows, neighbors, jitter, polar))

    def operate(vector):
        flat_vec = vector.reshape(-1, 3)

        def slab(inputs):
            separation, isotropic, radial, other = inputs
            return couple(separation, isotropic, radial, flat_vec[other])
        coupled = lax.map(slab, (separations, isotropics, radials, others))
        return vector / polar[..., None] - coupled
    weights = polar[..., None]
    dipoles = weights * permanent_field
    residual = permanent_field - operate(dipoles)
    scaled = weights * residual
    direction = scaled
    gamma_now = jnp.sum(residual * scaled)
    lengths = []
    for number in range(ITERS):
        image = operate(direction)
        step_len = gamma_now / jnp.sum(direction * image)
        dipoles = dipoles + step_len * direction
        residual = residual - step_len * image
        scaled = weights * residual
        gamma_next = jnp.sum(residual * scaled)
        direction = scaled + gamma_next / gamma_now * direction
        gamma_now = gamma_next
        lengths.append(step_len)
    return (dipoles, residual, jnp.stack(lengths))
```

```python
import jax
import jax.numpy as jnp
from jax import lax
from jax.experimental import pallas as pl
from jax.experimental.pallas import tpu as pltpu
from jax.sharding import Mesh
from jax.sharding import PartitionSpec as P

ITERS = 8
BASIS = ITERS + 1
THOLE = 0.39
SPACING = 3.5
EDGE = 6
NX = 12
WIDE = 42
GZ = ("gz_0", "gz_1")
F32 = jnp.float32

OFFSETS = [
    (a, b, c)
    for a in range(-2, 3)
    for b in range(-2, 3)
    for c in range(-2, 3)
    if 1 <= a * a + b * b + c * c <= 5
]
FORWARD = [d for d in OFFSETS if d > (0, 0, 0)]
PLANES = sorted({d[1:] for d in OFFSETS})
GROUPS, PER = 5, 7


def lane_iota():
    return lax.broadcasted_iota(jnp.int32, (8, 128), 1)


def third_masks():
    lane = lane_iota()
    return lane < WIDE, lane >= 2 * WIDE


def roll_lanes(v, ahead):
    ahead = ahead % 128
    return v if ahead == 0 else pltpu.roll(v, 128 - ahead, 1)


def roll_rows(v, ahead):
    return pltpu.roll(v, (-ahead) % 8, 0)


def shifted(v, dy, dz, first, last):
    if dy == 0:
        return roll_lanes(v, dz)
    if dy == 1:
        return jnp.where(
            last, roll_rows(roll_lanes(v, dz - 2 * WIDE), 1), roll_lanes(v, dz + WIDE)
        )
    if dy == 2:
        return jnp.where(
            first, roll_lanes(v, dz + 2 * WIDE), roll_rows(roll_lanes(v, dz - WIDE), 1)
        )
    if dy == -1:
        return jnp.where(
            first, roll_rows(roll_lanes(v, dz + 2 * WIDE), -1), roll_lanes(v, dz - WIDE)
        )
    return jnp.where(
        last, roll_lanes(v, dz - 2 * WIDE), roll_rows(roll_lanes(v, dz + WIDE), -1)
    )


def wrap(x):
    return jnp.where(x >= NX, x - NX, jnp.where(x < 0, x + NX, x))


def total(v):
    return jnp.sum(jnp.sum(v, axis=0, keepdims=True), axis=1, keepdims=True)


def region_kernel(
    own, a1, a2, a3, b1, b2, b3, basis_out, start_out, polar_out, info_out,
    chan, near, coef, moved, basis, inverse,
):
    gx = lax.axis_index("gx")
    gy = lax.axis_index("gy")
    gz = lax.axis_index("gz_0") * 4 + lax.axis_index("gz_1")
    lane = lane_iota()
    first, last = third_masks()
    along = lane - jnp.where(last, 2 * WIDE, jnp.where(first, 0, WIDE))
    is_low = (lane * 0 + gx) == 0

    def gather(x, carry):
        for group in range(GROUPS):
            blocks = [
                jnp.where(is_low, b3[x, group], a3[x, group]),
                jnp.where(is_low, b2[x, group], a2[x, group]),
                jnp.where(is_low, b1[x, group], a1[x, group]),
                own[x, group],
                jnp.where(is_low, a1[x, group], b1[x, group]),
                jnp.where(is_low, a2[x, group], b2[x, group]),
                jnp.where(is_low, a3[x, group], b3[x, group]),
            ]
            blocks = [pltpu.roll(v, 2 * gy, 0) for v in blocks]
            for member in range(PER):
                acc = roll_lanes(blocks[0], 6 * member)
                for k in range(1, 7):
                    acc = jnp.where(along >= 6 * k, roll_lanes(blocks[k], 6 * (member - k)), acc)
                if group * PER + member == 3:
                    acc = jnp.where(lane >= 3 * WIDE, 1.0, acc)
                    inverse[x] = 1.0 / acc
                chan[group * PER + member, x] = acc
        return carry

    lax.fori_loop(0, NX, gather, 0)

    def spread(x, carry):
        for c in range(4):
            v = chan[3 + c, x]
            for number, (dy, dz) in enumerate(PLANES):
                near[number, c, x] = shifted(v, dy, dz, first, last)
        return carry

    lax.fori_loop(0, NX, spread, 0)

    def pairs(x, carry):
        polar = chan[3, x]
        jit = [chan[4 + c, x] for c in range(3)]
        for number, d in enumerate(FORWARD):
            other = wrap(x + d[0])
            place = PLANES.index(d[1:])
            sep = [((near[place, 1 + c, other] - jit[c]) + float(d[c])) * SPACING for c in range(3)]
            dist_sq = sep[0] * sep[0] + sep[1] * sep[1] + sep[2] * sep[2]
            over = lax.rsqrt(dist_sq)
            cube = dist_sq * dist_sq * over
            over_sq = over * over
            over_cube = over_sq * over
            damping = THOLE * cube * lax.rsqrt(polar * near[place, 0, other])
            falloff = jnp.exp(-damping)
            iso = (1.0 - falloff) * over_cube
            radial = 3.0 * (1.0 - (1.0 + damping) * falloff) * over_cube * over_sq
            root = jnp.sqrt(radial)
            here = chan[7 + number, x] > 0.5
            values = [jnp.where(here, s * root, 0.0) for s in sep] + [jnp.where(here, iso, 0.0)]
            ahead = OFFSETS.index(d)
            behind = OFFSETS.index((-d[0], -d[1], -d[2]))
            for c in range(4):
                coef[ahead, c, x] = values[c]
                coef[behind, c, other] = shifted(values[c], -d[1], -d[2], first, last)
        return carry

    lax.fori_loop(0, NX, pairs, 0)

    def spread_vector(load):
        def one(x, carry):
            for c in range(3):
                v = load(c, x)
                by_y = {dy: shifted(v, dy, 0, first, last) for dy in range(-2, 3)}
                for number, (dy, dz) in enumerate(PLANES):
                    moved[number, c, x] = roll_lanes(by_y[dy], dz)
            return carry

        lax.fori_loop(0, NX, one, 0)

    def couple(x):
        acc = [jnp.zeros((8, 128), F32) for _ in range(3)]
        for number, d in enumerate(OFFSETS):
            other = wrap(x + d[0])
            place = PLANES.index(d[1:])
            v = [moved[place, c, other] for c in range(3)]
            s = [coef[number, c, x] for c in range(3)]
            iso = coef[number, 3, x]
            dot = s[0] * v[0] + s[1] * v[1] + s[2] * v[2]
            acc = [acc[c] + (s[c] * dot - iso * v[c]) for c in range(3)]
        polar = chan[3, x]
        return [polar * t for t in acc]

    zero = jnp.zeros((8, 128), F32)
    mine = (along >= 18) & (along < 24)

    spread_vector(lambda c, x: chan[3, x] * chan[c, x])

    def begin(x, carry):
        out = couple(x)
        for c in range(3):
            basis[0, c, x] = zero
            basis[1, c, x] = out[c]
            carry = carry + out[c] * out[c] * inverse[x]
        return carry

    norm = total(jnp.where(mine, lax.fori_loop(0, NX, begin, zero), 0.0))

    def extend(k, carry):
        info, norm, before, mixed = carry
        spread_vector(lambda c, x: basis[k + 1, c, x])

        def one(x, sums):
            out = couple(x)
            for c in range(3):
                basis[k + 2, c, x] = out[c]
                weighted = out[c] * inverse[x]
                sums = (
                    sums[0] + weighted * basis[k + 1, c, x],
                    sums[1] + weighted * basis[k, c, x],
                    sums[2] + weighted * out[c],
                )
            return sums

        sums = lax.fori_loop(0, NX, one, (zero, zero, zero))
        now, past, full = [total(jnp.where(mine, s, 0.0)) for s in sums]
        tiny = 1e-30
        al = jnp.where(norm > tiny, now / jnp.maximum(norm, tiny), 0.0)
        be = jnp.where(before > tiny, past / jnp.maximum(before, tiny), 0.0)
        rest = (
            full - 2.0 * al * now - 2.0 * be * past
            + al * al * norm + be * be * before + 2.0 * al * be * mixed
        )
        rest = jnp.maximum(rest, 1e-10 * full)
        good = (rest > tiny) & (norm > tiny)
        inv = jnp.where(good, jnp.sqrt(rest / jnp.maximum(norm, tiny)), 1.0)
        inv = jnp.minimum(jnp.maximum(inv, 1e-6), 1e3)
        sc = 1.0 / inv

        def scale(x, sums):
            for c in range(3):
                u = basis[k + 1, c, x]
                new = (basis[k + 2, c, x] - al * u - be * basis[k, c, x]) * sc
                basis[k + 2, c, x] = new
                weighted = new * inverse[x]
                sums = (sums[0] + weighted * new, sums[1] + weighted * u)
            return sums

        sums = lax.fori_loop(0, NX, scale, (zero, zero))
        after, mixed = [total(jnp.where(mine, s, 0.0)) for s in sums]
        info = jnp.where(lane == 45 + k, al, info)
        info = jnp.where(lane == 53 + k, be, info)
        info = jnp.where(lane == 61 + k, inv, info)
        return info, after, norm, mixed

    none = jnp.zeros((1, 1), F32)
    info, _, _, _ = lax.fori_loop(0, ITERS, extend, (zero, norm, none, none))

    number = 0
    for low, high in ((0, 3), (3, BASIS)):
        entries = [(i, j) for i in range(low, high) for j in range(i, BASIS)]

        def one(x, sums):
            sums = list(sums)
            for c in range(3):
                u = {j: basis[j + 1, c, x] for j in range(low, BASIS)}
                for i in range(low, high):
                    weighted = u[i] * inverse[x]
                    for n, (p, q) in enumerate(entries):
                        if p == i:
                            sums[n] = sums[n] + weighted * u[q]
            return tuple(sums)

        sums = lax.fori_loop(0, NX, one, (zero,) * len(entries))
        for n in range(len(entries)):
            info = jnp.where(lane == number, total(jnp.where(mine, sums[n], 0.0)), info)
            number += 1

    row = lax.broadcasted_iota(jnp.int32, (8, 128), 0)
    info_out[0:8, :] = jnp.where(row == gz, info, 0.0)
    info_out[8:16, :] = jnp.where(row + 8 == gz, info, 0.0)

    def keep(x, carry):
        far = x + EDGE * gx

        def front(v):
            return pltpu.roll(roll_lanes(v, 18), 8 - 2 * gy, 0)

        for c in range(3):
            for k in range(BASIS):
                basis_out[k, c, x] = front(basis[k + 1, c, far])
            start_out[c, x] = front(chan[3, far] * chan[c, far])
        polar_out[x] = front(inverse[far])
        return carry

    lax.fori_loop(0, EDGE, keep, 0)


def finish_kernel(basis, start, inverse, info, dip_out, res_out, len_out, table):
    gz = lax.axis_index("gz_0") * 4 + lax.axis_index("gz_1")
    wide = jnp.concatenate([info[...], jnp.zeros((112, 128), F32)], axis=0)
    table[...] = wide.T
    rows = {}
    number = 0
    for low, high in ((0, 3), (3, BASIS)):
        for i in range(low, high):
            for j in range(i, BASIS):
                rows[i, j] = rows[j, i] = table[number : number + 1, :]
                number += 1
    al = [table[45 + k : 46 + k, :] for k in range(ITERS)]
    be = [table[53 + k : 54 + k, :] for k in range(ITERS)]
    inv = [table[61 + k : 62 + k, :] for k in range(ITERS)]
    lane = lax.broadcasted_iota(jnp.int32, (1, 128), 1)
    zero = jnp.zeros((1, 128), F32)
    one = jnp.where(lane < 16, 1.0, 0.0)

    def summed(v):
        return jnp.sum(v, axis=1, keepdims=True)

    def form(left, right, size_left, size_right):
        acc = zero
        for i in range(size_left):
            inner = zero
            for j in range(size_right):
                inner = inner + rows[i, j] * right[j]
            acc = acc + left[i] * inner
        return summed(acc)

    search = [one] + [zero] * ITERS
    resid = [one] + [zero] * ITERS
    moves = [zero] * BASIS
    gamma = summed(rows[0, 0])
    lengths = jnp.zeros((8, 128), F32)
    lanes = lane_iota()
    for k in range(ITERS):
        image = list(search)
        for j in range(k + 1):
            image[j] = image[j] - al[j] * search[j]
            image[j + 1] = image[j + 1] - inv[j] * search[j]
            if j:
                image[j - 1] = image[j - 1] - be[j] * search[j]
        step = gamma / form(search, image, k + 1, k + 2)
        lengths = jnp.where(lanes == k, step, lengths)
        moves = [moves[j] + step * search[j] for j in range(BASIS)]
        resid = [resid[j] - step * image[j] for j in range(BASIS)]
        if k + 1 < ITERS:
            after = form(resid, resid, k + 2, k + 2)
            ratio = after / gamma
            search = [resid[j] + ratio * search[j] for j in range(BASIS)]
            gamma = after
    len_out[...] = lengths
    here = lane == gz
    moves = [summed(jnp.where(here, v, 0.0)) for v in moves]
    resid = [summed(jnp.where(here, v, 0.0)) for v in resid]
    for x in range(EDGE):
        for c in range(3):
            dip = start[c, x]
            res = jnp.zeros((8, 128), F32)
            for k in range(BASIS):
                u = basis[k, c, x]
                if k < ITERS:
                    dip = dip + moves[k] * u
                res = res + resid[k] * u
            dip_out[c, x] = dip
            res_out[c, x] = res * inverse[x]


def per_device(permanent_field, polar, jitter, neighbors):
    grid = lambda dim: lax.broadcasted_iota(jnp.int32, (EDGE, EDGE, EDGE, 1), dim)
    home = ((grid(0) + 2) * 10 + grid(1) + 2) * 10 + grid(2) + 2
    relative = neighbors - home
    codes = [d[0] * 100 + d[1] * 10 + d[2] for d in FORWARD]
    flags = jnp.stack(
        [jnp.max((relative == code).astype(F32), axis=-1) for code in codes], axis=-1
    )
    sites = jnp.concatenate([permanent_field, polar[..., None], jitter, flags], axis=-1)
    packed = sites.reshape(EDGE, 2, 3, EDGE, GROUPS, PER).transpose(0, 4, 1, 2, 5, 3)
    packed = packed.reshape(EDGE, GROUPS, 2, 126)
    packed = jnp.pad(packed, ((0, 0), (0, 0), (0, 0), (0, 2)))

    both = lax.all_gather(packed, "gx", axis=0, tiled=True)
    around = [both] + [
        lax.ppermute(both, "gy", [((i + k) % 4, i) for i in range(4)]) for k in (1, 2, 3)
    ]
    own = jnp.concatenate(around, axis=2)

    def fetch(k):
        pairs = [((i + k) % 16, i) for i in range(16)]
        pairs += [(16 + (i - k) % 16, 16 + i) for i in range(16)]
        return lax.ppermute(own, ("gx",) + GZ, pairs)

    direct = [fetch(k) for k in (1, 2, 3)]
    passed = [lax.ppermute(v, "gx", [(0, 1), (1, 0)]) for v in direct]

    vreg = (8, 128)
    basis, start, inverse, info = pl.pallas_call(
        region_kernel,
        out_shape=(
            jax.ShapeDtypeStruct((BASIS, 3, EDGE) + vreg, F32),
            jax.ShapeDtypeStruct((3, EDGE) + vreg, F32),
            jax.ShapeDtypeStruct((EDGE,) + vreg, F32),
            jax.ShapeDtypeStruct((16, 128), F32),
        ),
        scratch_shapes=[
            pltpu.VMEM((GROUPS * PER, NX) + vreg, F32),
            pltpu.VMEM((len(PLANES), 4, NX) + vreg, F32),
            pltpu.VMEM((len(OFFSETS), 4, NX) + vreg, F32),
            pltpu.VMEM((len(PLANES), 3, NX) + vreg, F32),
            pltpu.VMEM((BASIS + 1, 3, NX) + vreg, F32),
            pltpu.VMEM((NX,) + vreg, F32),
        ],
        compiler_params=pltpu.CompilerParams(vmem_limit_bytes=48 * 1024 * 1024),
        name="region",
    )(own, *direct, *passed)

    info = lax.psum(lax.psum(info, "gz_1"), "gz_0")

    dip, res, lengths = pl.pallas_call(
        finish_kernel,
        out_shape=(
            jax.ShapeDtypeStruct((3, EDGE) + vreg, F32),
            jax.ShapeDtypeStruct((3, EDGE) + vreg, F32),
            jax.ShapeDtypeStruct(vreg, F32),
        ),
        scratch_shapes=[pltpu.VMEM((128, 128), F32)],
        name="finish",
    )(basis, start, inverse, info)

    def unpack(v):
        v = v[:, :, :2, :126].reshape(3, EDGE, 2, 3, WIDE)[..., :EDGE]
        return v.reshape(3, EDGE, EDGE, EDGE).transpose(1, 2, 3, 0)

    return unpack(dip), unpack(res), lengths[0, :ITERS]


def solution(mesh):
    finer = Mesh(
        mesh.devices.reshape(mesh.shape["gx"], mesh.shape["gy"], 4, 4), ("gx", "gy", "gz_0", "gz_1")
    )
    return jax.shard_map(
        per_device,
        mesh=finer,
        in_specs=(
            P("gx", "gy", GZ, None),
            P("gx", "gy", GZ),
            P("gx", "gy", GZ, None),
            P("gx", "gy", GZ, None),
        ),
        out_specs=(P("gx", "gy", GZ, None), P("gx", "gy", GZ, None), P()),
        check_vma=False,
    )
```

```python
import jax
import jax.numpy as jnp
from jax import lax
from jax.experimental import pallas as pl
from jax.experimental.pallas import tpu as pltpu
from jax.sharding import Mesh
from jax.sharding import PartitionSpec as P

ITERS = 8
BASIS = ITERS + 1
THOLE = 0.39
SPACING = 3.5
EDGE = 6
NX = 12
WIDE = 42
GZ = ("gz_0", "gz_1")
F32 = jnp.float32

OFFSETS = [
    (a, b, c)
    for a in range(-2, 3)
    for b in range(-2, 3)
    for c in range(-2, 3)
    if 1 <= a * a + b * b + c * c <= 5
]
FORWARD = [d for d in OFFSETS if d > (0, 0, 0)]
PLANES = sorted({d[1:] for d in OFFSETS})
GROUPS, PER = 5, 7


def lane_iota():
    return lax.broadcasted_iota(jnp.int32, (8, 128), 1)


def third_masks():
    lane = lane_iota()
    return lane < WIDE, lane >= 2 * WIDE


def roll_lanes(v, ahead):
    ahead = ahead % 128
    return v if ahead == 0 else pltpu.roll(v, 128 - ahead, 1)


def roll_rows(v, ahead):
    return pltpu.roll(v, (-ahead) % 8, 0)


def shifted(v, dy, dz, first, last):
    if dy == 0:
        return roll_lanes(v, dz)
    if dy == 1:
        return jnp.where(
            last, roll_rows(roll_lanes(v, dz - 2 * WIDE), 1), roll_lanes(v, dz + WIDE)
        )
    if dy == 2:
        return jnp.where(
            first, roll_lanes(v, dz + 2 * WIDE), roll_rows(roll_lanes(v, dz - WIDE), 1)
        )
    if dy == -1:
        return jnp.where(
            first, roll_rows(roll_lanes(v, dz + 2 * WIDE), -1), roll_lanes(v, dz - WIDE)
        )
    return jnp.where(
        last, roll_lanes(v, dz - 2 * WIDE), roll_rows(roll_lanes(v, dz + WIDE), -1)
    )


def wrap(x):
    return jnp.where(x >= NX, x - NX, jnp.where(x < 0, x + NX, x))


def total(v):
    return jnp.sum(jnp.sum(v, axis=0, keepdims=True), axis=1, keepdims=True)


def unrolled(count, times, body, carry):
    def several(i, carry):
        for t in range(times):
            carry = body(i * times + t, carry)
        return carry

    return lax.fori_loop(0, count // times, several, carry)


def pack_kernel(field, polar, jitter, neighbors, out):
    lane = lax.broadcasted_iota(jnp.int32, (1, 128), 1)
    third = jnp.where(lane >= 2 * WIDE, 2, jnp.where(lane >= WIDE, 1, 0))
    inside = lane - third * WIDE
    member = inside // EDGE
    z = inside - member * EDGE
    wanted = []
    for group in range(1, GROUPS):
        code = jnp.full((1, 128), -5000, jnp.int32)
        for n in range(PER):
            d = FORWARD[(group - 1) * PER + n]
            code = jnp.where(member == n, d[0] * 100 + d[1] * 10 + d[2], code)
        wanted.append(jnp.where(lane < 3 * WIDE, code + third * 10 + z, -5000))
    row = lax.broadcasted_iota(jnp.int32, (EDGE, 128), 0)
    column = lax.broadcasted_iota(jnp.int32, (EDGE, 128), 1)
    pick = []
    for t in range(3):
        hit = column * 0 > 0
        for n in range(PER):
            hit = hit | (column == row + (t * WIDE + n * EDGE))
        pick.append(jnp.where(hit, 1.0, 0.0))

    def one(x, carry):
        for s in range(2):
            slots = jnp.zeros((56, 128), F32)
            values = jnp.zeros((1, 128), F32)
            for t in range(3):
                y = 3 * s + t
                slots = slots + lax.dot_general(
                    neighbors[x, y].astype(F32), pick[t], (((0,), (0,)), ((), ())),
                    precision=lax.Precision.HIGHEST, preferred_element_type=F32,
                )
                parts = [field[x, y, c : c + 1, :] for c in range(3)]
                parts += [polar[x, y : y + 1, :]]
                parts += [jitter[x, y, c : c + 1, :] for c in range(3)]
                for n in range(PER):
                    wide = jnp.concatenate([parts[n], jnp.zeros((1, 122), F32)], axis=1)
                    start = t * WIDE + n * EDGE
                    values = values + (pltpu.roll(wide, start, 1) if start else wide)
            out[x, 0, s : s + 1, :] = values
            home = (x + 2) * 100 + (2 + 3 * s) * 10 + 2
            for group in range(1, GROUPS):
                target = (wanted[group - 1] + home).astype(F32)
                flag = jnp.max(jnp.where(slots == target, 1.0, 0.0), axis=0, keepdims=True)
                out[x, group, s : s + 1, :] = flag
        return carry

    lax.fori_loop(0, EDGE, one, 0)


def region_kernel(
    own, a1, a2, a3, b1, b2, b3, kept_out, info_out,
    chan, near, coef, moved, basis,
):
    gx = lax.axis_index("gx")
    gy = lax.axis_index("gy")
    gz = lax.axis_index("gz_0") * 4 + lax.axis_index("gz_1")
    lane = lane_iota()
    first, last = third_masks()
    along = lane - jnp.where(last, 2 * WIDE, jnp.where(first, 0, WIDE))
    is_low = (lane * 0 + gx) == 0

    def gather(x, carry):
        for group in range(GROUPS):
            blocks = [
                jnp.where(is_low, b3[x, group], a3[x, group]),
                jnp.where(is_low, b2[x, group], a2[x, group]),
                jnp.where(is_low, b1[x, group], a1[x, group]),
                own[x, group],
                jnp.where(is_low, a1[x, group], b1[x, group]),
                jnp.where(is_low, a2[x, group], b2[x, group]),
                jnp.where(is_low, a3[x, group], b3[x, group]),
            ]
            blocks = [pltpu.roll(v, 2 * gy, 0) for v in blocks]
            for member in range(PER):
                acc = roll_lanes(blocks[0], 6 * member)
                for k in range(1, 7):
                    acc = jnp.where(along >= 6 * k, roll_lanes(blocks[k], 6 * (member - k)), acc)
                if group * PER + member == 3:
                    acc = jnp.where(lane >= 3 * WIDE, 1.0, acc)
                    chan[x, 35] = 1.0 / acc
                chan[x, group * PER + member] = acc
        return carry

    lax.fori_loop(0, NX, gather, 0)

    def spread(x, carry):
        for c in range(4):
            v = chan[x, 3 + c]
            for number, (dy, dz) in enumerate(PLANES):
                near[x, number * 4 + c] = shifted(v, dy, dz, first, last)
        return carry

    unrolled(NX, 3, spread, 0)

    def pairs(x, carry):
        polar = chan[x, 3]
        jit = [chan[x, 4 + c] for c in range(3)]
        for number, d in enumerate(FORWARD):
            other = wrap(x + d[0])
            place = PLANES.index(d[1:]) * 4
            sep = [((near[other, place + 1 + c] - jit[c]) + float(d[c])) * SPACING for c in range(3)]
            dist_sq = sep[0] * sep[0] + sep[1] * sep[1] + sep[2] * sep[2]
            over = lax.rsqrt(dist_sq)
            cube = dist_sq * dist_sq * over
            over_sq = over * over
            over_cube = over_sq * over
            damping = THOLE * cube * lax.rsqrt(polar * near[other, place])
            falloff = jnp.exp(-damping)
            iso = (1.0 - falloff) * over_cube
            radial = 3.0 * (1.0 - (1.0 + damping) * falloff) * over_cube * over_sq
            root = jnp.sqrt(radial)
            here = chan[x, 7 + number] > 0.5
            values = [jnp.where(here, s * root, 0.0) for s in sep] + [jnp.where(here, iso, 0.0)]
            ahead = OFFSETS.index(d) * 4
            behind = OFFSETS.index((-d[0], -d[1], -d[2])) * 4
            for c in range(4):
                coef[x, ahead + c] = values[c]
                coef[other, behind + c] = shifted(values[c], -d[1], -d[2], first, last)
        return carry

    lax.fori_loop(0, NX, pairs, 0)

    def move(x, c, v):
        by_y = {dy: shifted(v, dy, 0, first, last) for dy in range(-2, 3)}
        for number, (dy, dz) in enumerate(PLANES):
            moved[x, number * 3 + c] = roll_lanes(by_y[dy], dz)

    def couple(x):
        acc = [jnp.zeros((8, 128), F32) for _ in range(3)]
        for number, d in enumerate(OFFSETS):
            other = wrap(x + d[0])
            place = PLANES.index(d[1:]) * 3
            v = [moved[other, place + c] for c in range(3)]
            s = [coef[x, number * 4 + c] for c in range(3)]
            iso = coef[x, number * 4 + 3]
            dot = s[0] * v[0] + s[1] * v[1] + s[2] * v[2]
            acc = [acc[c] + (s[c] * dot - iso * v[c]) for c in range(3)]
        polar = chan[x, 3]
        return [polar * t for t in acc]

    zero = jnp.zeros((8, 128), F32)
    mine = (along >= 18) & (along < 24)

    def start(x, carry):
        for c in range(3):
            move(x, c, chan[x, 3] * chan[x, c])
        return carry

    unrolled(NX, 4, start, 0)

    def begin(x, carry):
        out = couple(x)
        for c in range(3):
            basis[0, x * 3 + c] = zero
            basis[1, x * 3 + c] = out[c]
        return carry

    lax.fori_loop(0, NX, begin, 0)

    def again(x, carry):
        for c in range(3):
            move(x, c, basis[1, x * 3 + c])
        return carry

    unrolled(NX, 4, again, 0)

    def extend(k, info):
        def one(x, sums):
            out = couple(x)
            over = chan[x, 35]
            sums = list(sums)
            for c in range(3):
                u = basis[k + 1, x * 3 + c]
                p = basis[k, x * 3 + c]
                basis[k + 2, x * 3 + c] = out[c]
                w = out[c] * over
                uw = u * over
                sums[0] = sums[0] + w * u
                sums[1] = sums[1] + w * p
                sums[2] = sums[2] + w * out[c]
                sums[3] = sums[3] + uw * u
                sums[4] = sums[4] + uw * p
                sums[5] = sums[5] + (p * over) * p
            return tuple(sums)

        sums = lax.fori_loop(0, NX, one, (zero,) * 6)
        now, past, full, norm, mixed, before = [total(jnp.where(mine, s, 0.0)) for s in sums]
        tiny = 1e-30
        al = jnp.where(norm > tiny, now / jnp.maximum(norm, tiny), 0.0)
        be = jnp.where(before > tiny, past / jnp.maximum(before, tiny), 0.0)
        rest = (
            full - 2.0 * al * now - 2.0 * be * past
            + al * al * norm + be * be * before + 2.0 * al * be * mixed
        )
        rest = jnp.maximum(rest, 1e-10 * full)
        good = (rest > tiny) & (norm > tiny)
        inv = jnp.where(good, jnp.sqrt(rest / jnp.maximum(norm, tiny)), 1.0)
        inv = jnp.minimum(jnp.maximum(inv, 1e-6), 1e3)
        sc = 1.0 / inv

        def scale(x, carry):
            for c in range(3):
                at = x * 3 + c
                new = (basis[k + 2, at] - al * basis[k + 1, at] - be * basis[k, at]) * sc
                basis[k + 2, at] = new
                move(x, c, new)
            return carry

        unrolled(NX, 4, scale, 0)
        info = jnp.where(lane == 45 + k, al, info)
        info = jnp.where(lane == 53 + k, be, info)
        return jnp.where(lane == 61 + k, inv, info)

    info = lax.fori_loop(0, ITERS, extend, zero)

    number = 0
    for low, high in ((0, 3), (3, BASIS)):
        entries = [(i, j) for i in range(low, high) for j in range(i, BASIS)]

        def one(x, sums):
            sums = list(sums)
            for c in range(3):
                u = {j: basis[j + 1, x * 3 + c] for j in range(low, BASIS)}
                for i in range(low, high):
                    weighted = u[i] * chan[x, 35]
                    for n, (p, q) in enumerate(entries):
                        if p == i:
                            sums[n] = sums[n] + weighted * u[q]
            return tuple(sums)

        sums = lax.fori_loop(0, NX, one, (zero,) * len(entries))
        for n in range(len(entries)):
            info = jnp.where(lane == number, total(jnp.where(mine, sums[n], 0.0)), info)
            number += 1

    row = lax.broadcasted_iota(jnp.int32, (8, 128), 0)
    info_out[0:8, :] = jnp.where(row == gz, info, 0.0)
    info_out[8:16, :] = jnp.where(row + 8 == gz, info, 0.0)

    def keep(x, carry):
        far = x + EDGE * gx

        def front(v):
            return pltpu.roll(roll_lanes(v, 18), 8 - 2 * gy, 0)

        for c in range(3):
            for k in range(BASIS):
                kept_out[x, k * 3 + c] = front(basis[k + 1, far * 3 + c])
            kept_out[x, 27 + c] = front(chan[far, 3] * chan[far, c])
        kept_out[x, 30] = front(chan[far, 35])
        return carry

    unrolled(EDGE, 2, keep, 0)


def finish_kernel(kept, info, dip_out, res_out, len_out, table):
    gz = lax.axis_index("gz_0") * 4 + lax.axis_index("gz_1")
    wide = jnp.concatenate([info[...], jnp.zeros((112, 128), F32)], axis=0)
    table[...] = wide.T
    rows = {}
    number = 0
    for low, high in ((0, 3), (3, BASIS)):
        for i in range(low, high):
            for j in range(i, BASIS):
                rows[i, j] = rows[j, i] = table[number : number + 1, :]
                number += 1
    al = [table[45 + k : 46 + k, :] for k in range(ITERS)]
    be = [table[53 + k : 54 + k, :] for k in range(ITERS)]
    inv = [table[61 + k : 62 + k, :] for k in range(ITERS)]
    lane = lax.broadcasted_iota(jnp.int32, (1, 128), 1)
    zero = jnp.zeros((1, 128), F32)
    one = jnp.where(lane < 16, 1.0, 0.0)

    def summed(v):
        return jnp.sum(v, axis=1, keepdims=True)

    def form(left, right, size_left, size_right):
        acc = zero
        for i in range(size_left):
            inner = zero
            for j in range(size_right):
                inner = inner + rows[i, j] * right[j]
            acc = acc + left[i] * inner
        return summed(acc)

    search = [one] + [zero] * ITERS
    resid = [one] + [zero] * ITERS
    moves = [zero] * BASIS
    gamma = summed(rows[0, 0])
    lengths = zero
    for k in range(ITERS):
        image = list(search)
        for j in range(k + 1):
            image[j] = image[j] - al[j] * search[j]
            image[j + 1] = image[j + 1] - inv[j] * search[j]
            if j:
                image[j - 1] = image[j - 1] - be[j] * search[j]
        step = gamma / form(search, image, k + 1, k + 2)
        lengths = jnp.where(lane == k, step, lengths)
        moves = [moves[j] + step * search[j] for j in range(BASIS)]
        resid = [resid[j] - step * image[j] for j in range(BASIS)]
        if k + 1 < ITERS:
            after = form(resid, resid, k + 2, k + 2)
            ratio = after / gamma
            search = [resid[j] + ratio * search[j] for j in range(BASIS)]
            gamma = after
    len_out[...] = lengths[:, :ITERS]
    here = lane == gz
    moves = [summed(jnp.where(here, v, 0.0)) for v in moves]
    resid = [summed(jnp.where(here, v, 0.0)) for v in resid]
    for x in range(EDGE):
        for c in range(3):
            dip = kept[x, 27 + c]
            res = jnp.zeros((8, 128), F32)
            for k in range(BASIS):
                u = kept[x, k * 3 + c]
                if k < ITERS:
                    dip = dip + moves[k] * u
                res = res + resid[k] * u
            res = res * kept[x, 30]
            for out, v in ((dip_out, dip), (res_out, res)):
                for t in range(3):
                    w = roll_lanes(v, t * WIDE)
                    for s in range(2):
                        out[x, 3 * s + t, c : c + 1, :] = w[s : s + 1, :EDGE]


def per_device(permanent_field, polar, jitter, neighbors):
    packed = pl.pallas_call(
        pack_kernel,
        out_shape=jax.ShapeDtypeStruct((EDGE, GROUPS, 2, 128), F32),
        name="pack",
    )(permanent_field.transpose(0, 1, 3, 2), polar, jitter.transpose(0, 1, 3, 2), neighbors)

    both = lax.all_gather(packed, "gx", axis=0, tiled=True)
    around = [both] + [
        lax.ppermute(both, "gy", [((i + k) % 4, i) for i in range(4)]) for k in (1, 2, 3)
    ]
    own = jnp.concatenate(around, axis=2)

    def fetch(k):
        pairs = [((i + k) % 16, i) for i in range(16)]
        pairs += [(16 + (i - k) % 16, 16 + i) for i in range(16)]
        return lax.ppermute(own, ("gx",) + GZ, pairs)

    direct = [fetch(k) for k in (1, 2, 3)]
    passed = [lax.ppermute(v, "gx", [(0, 1), (1, 0)]) for v in direct]

    vreg = (8, 128)
    kept, info = pl.pallas_call(
        region_kernel,
        out_shape=(
            jax.ShapeDtypeStruct((EDGE, 31) + vreg, F32),
            jax.ShapeDtypeStruct((16, 128), F32),
        ),
        scratch_shapes=[
            pltpu.VMEM((NX, 36) + vreg, F32),
            pltpu.VMEM((NX, 4 * len(PLANES)) + vreg, F32),
            pltpu.VMEM((NX, 4 * len(OFFSETS)) + vreg, F32),
            pltpu.VMEM((NX, 64) + vreg, F32),
            pltpu.VMEM((BASIS + 1, 3 * NX) + vreg, F32),
        ],
        compiler_params=pltpu.CompilerParams(vmem_limit_bytes=36 * 1024 * 1024),
        name="region",
    )(own, *direct, *passed)

    info = lax.psum(lax.psum(info, "gz_1"), "gz_0")

    dip, res, lengths = pl.pallas_call(
        finish_kernel,
        out_shape=(
            jax.ShapeDtypeStruct((EDGE, EDGE, 3, EDGE), F32),
            jax.ShapeDtypeStruct((EDGE, EDGE, 3, EDGE), F32),
            jax.ShapeDtypeStruct((1, ITERS), F32),
        ),
        scratch_shapes=[pltpu.VMEM((128, 128), F32)],
        compiler_params=pltpu.CompilerParams(vmem_limit_bytes=8 * 1024 * 1024),
        name="finish",
    )(kept, info)
    return dip.transpose(0, 1, 3, 2), res.transpose(0, 1, 3, 2), lengths.reshape(ITERS)


def solution(mesh):
    finer = Mesh(
        mesh.devices.reshape(mesh.shape["gx"], mesh.shape["gy"], 4, 4), ("gx", "gy", "gz_0", "gz_1")
    )
    return jax.shard_map(
        per_device,
        mesh=finer,
        in_specs=(
            P("gx", "gy", GZ, None),
            P("gx", "gy", GZ),
            P("gx", "gy", GZ, None),
            P("gx", "gy", GZ, None),
        ),
        out_specs=(P("gx", "gy", GZ, None), P("gx", "gy", GZ, None), P()),
        check_vma=False,
    )
```

```python
import jax
import jax.numpy as jnp
from jax import lax
from jax.experimental import pallas as pl
from jax.experimental.pallas import tpu as pltpu
from jax.sharding import Mesh
from jax.sharding import PartitionSpec as P

ITERS = 8
BASIS = ITERS + 1
THOLE = 0.39
SPACING = 3.5
EDGE = 6
NX = 12
WIDE = 42
GZ = ("gz_0", "gz_1")
F32 = jnp.float32

OFFSETS = [
    (a, b, c)
    for a in range(-2, 3)
    for b in range(-2, 3)
    for c in range(-2, 3)
    if 1 <= a * a + b * b + c * c <= 5
]
FORWARD = [d for d in OFFSETS if d > (0, 0, 0)]
GROUPS, PER = 5, 7


def lane_iota():
    return lax.broadcasted_iota(jnp.int32, (8, 128), 1)


def third_masks():
    lane = lane_iota()
    return lane < WIDE, lane >= 2 * WIDE


def roll_lanes(v, ahead):
    ahead = ahead % 128
    return v if ahead == 0 else pltpu.roll(v, 128 - ahead, 1)


def roll_rows(v, ahead):
    return pltpu.roll(v, (-ahead) % 8, 0)


def shifted(v, dy, dz, first, last):
    if dy == 0:
        return roll_lanes(v, dz)
    if dy == 1:
        return jnp.where(
            last, roll_rows(roll_lanes(v, dz - 2 * WIDE), 1), roll_lanes(v, dz + WIDE)
        )
    if dy == 2:
        return jnp.where(
            first, roll_lanes(v, dz + 2 * WIDE), roll_rows(roll_lanes(v, dz - WIDE), 1)
        )
    if dy == -1:
        return jnp.where(
            first, roll_rows(roll_lanes(v, dz + 2 * WIDE), -1), roll_lanes(v, dz - WIDE)
        )
    return jnp.where(
        last, roll_lanes(v, dz - 2 * WIDE), roll_rows(roll_lanes(v, dz + WIDE), -1)
    )


def wrap(x):
    return jnp.where(x >= NX, x - NX, jnp.where(x < 0, x + NX, x))


def total(v):
    return jnp.sum(jnp.sum(v, axis=0, keepdims=True), axis=1, keepdims=True)


def unrolled(count, times, body, carry):
    def several(i, carry):
        for t in range(times):
            carry = body(i * times + t, carry)
        return carry

    return lax.fori_loop(0, count // times, several, carry)


def pack_kernel(field, polar, jitter, neighbors, out):
    lane = lax.broadcasted_iota(jnp.int32, (1, 128), 1)
    third = jnp.where(lane >= 2 * WIDE, 2, jnp.where(lane >= WIDE, 1, 0))
    inside = lane - third * WIDE
    member = inside // EDGE
    z = inside - member * EDGE
    wanted = []
    for group in range(1, GROUPS):
        code = jnp.full((1, 128), -5000, jnp.int32)
        for n in range(PER):
            d = FORWARD[(group - 1) * PER + n]
            code = jnp.where(member == n, d[0] * 100 + d[1] * 10 + d[2], code)
        wanted.append(jnp.where(lane < 3 * WIDE, code + third * 10 + z, -5000))
    row = lax.broadcasted_iota(jnp.int32, (EDGE, 128), 0)
    column = lax.broadcasted_iota(jnp.int32, (EDGE, 128), 1)
    pick = []
    for t in range(3):
        hit = column * 0 > 0
        for n in range(PER):
            hit = hit | (column == row + (t * WIDE + n * EDGE))
        pick.append(jnp.where(hit, 1.0, 0.0))

    def one(x, carry):
        for s in range(2):
            slots = jnp.zeros((56, 128), F32)
            values = jnp.zeros((1, 128), F32)
            for t in range(3):
                y = 3 * s + t
                slots = slots + lax.dot_general(
                    neighbors[x, y].astype(F32), pick[t], (((0,), (0,)), ((), ())),
                    precision=lax.Precision.HIGHEST, preferred_element_type=F32,
                )
                parts = [field[x, y, c : c + 1, :] for c in range(3)]
                parts += [polar[x, y : y + 1, :]]
                parts += [jitter[x, y, c : c + 1, :] for c in range(3)]
                for n in range(PER):
                    wide = jnp.concatenate([parts[n], jnp.zeros((1, 122), F32)], axis=1)
                    start = t * WIDE + n * EDGE
                    values = values + (pltpu.roll(wide, start, 1) if start else wide)
            out[x, 0, s : s + 1, :] = values
            home = (x + 2) * 100 + (2 + 3 * s) * 10 + 2
            for group in range(1, GROUPS):
                target = (wanted[group - 1] + home).astype(F32)
                flag = jnp.max(jnp.where(slots == target, 1.0, 0.0), axis=0, keepdims=True)
                out[x, group, s : s + 1, :] = flag
        return carry

    lax.fori_loop(0, EDGE, one, 0)


def region_kernel(
    own, a1, a2, a3, b1, b2, b3, kept_out, info_out,
    chan, near, coef, moved, basis,
):
    gx = lax.axis_index("gx")
    gy = lax.axis_index("gy")
    gz = lax.axis_index("gz_0") * 4 + lax.axis_index("gz_1")
    lane = lane_iota()
    first, last = third_masks()
    along = lane - jnp.where(last, 2 * WIDE, jnp.where(first, 0, WIDE))
    is_low = (lane * 0 + gx) == 0

    def gather(x, carry):
        for group in range(GROUPS):
            blocks = [
                jnp.where(is_low, b3[x, group], a3[x, group]),
                jnp.where(is_low, b2[x, group], a2[x, group]),
                jnp.where(is_low, b1[x, group], a1[x, group]),
                own[x, group],
                jnp.where(is_low, a1[x, group], b1[x, group]),
                jnp.where(is_low, a2[x, group], b2[x, group]),
                jnp.where(is_low, a3[x, group], b3[x, group]),
            ]
            outs = [None] * PER
            for gap in range(-6, 7):
                members = [m for m in range(PER) if 0 <= m + gap < PER]
                mixed = blocks[members[0] + gap]
                for m in members[1:]:
                    mixed = jnp.where(along >= 6 * m, blocks[m + gap], mixed)
                mixed = roll_lanes(mixed, -6 * gap)
                for m in members:
                    outs[m] = (
                        mixed if outs[m] is None
                        else jnp.where(along >= 6 * (m + gap), mixed, outs[m])
                    )
            for member in range(PER):
                acc = pltpu.roll(outs[member], 2 * gy, 0)
                if group * PER + member == 3:
                    acc = jnp.where(lane >= 3 * WIDE, 1.0, acc)
                    chan[x, 35] = 1.0 / acc
                chan[x, group * PER + member] = acc
        return carry

    lax.fori_loop(0, NX, gather, 0)

    def spread(x, carry):
        for c in range(4):
            v = chan[x, 3 + c]
            for dy in range(-2, 3):
                near[x, (dy + 2) * 4 + c] = shifted(v, dy, 0, first, last)
        return carry

    unrolled(NX, 3, spread, 0)

    def pairs(x, carry):
        home = {dz: [roll_lanes(chan[x, 3 + c], -dz) for c in range(4)] for dz in range(-2, 3)}
        for number, d in enumerate(FORWARD):
            other = wrap(x + d[0])
            place = (d[1] + 2) * 4
            polar, *jit = home[d[2]]
            sep = [((near[other, place + 1 + c] - jit[c]) + float(d[c])) * SPACING for c in range(3)]
            dist_sq = sep[0] * sep[0] + sep[1] * sep[1] + sep[2] * sep[2]
            over = lax.rsqrt(dist_sq)
            cube = dist_sq * dist_sq * over
            over_sq = over * over
            over_cube = over_sq * over
            damping = THOLE * cube * lax.rsqrt(polar * near[other, place])
            falloff = jnp.exp(-damping)
            iso = (1.0 - falloff) * over_cube
            radial = 3.0 * (1.0 - (1.0 + damping) * falloff) * over_cube * over_sq
            root = jnp.sqrt(radial)
            here = roll_lanes(chan[x, 7 + number], -d[2]) > 0.5
            values = [jnp.where(here, s * root, 0.0) for s in sep] + [jnp.where(here, iso, 0.0)]
            ahead = OFFSETS.index(d) * 4
            behind = OFFSETS.index((-d[0], -d[1], -d[2])) * 4
            for c in range(4):
                coef[x, ahead + c] = values[c]
                coef[other, behind + c] = shifted(values[c], -d[1], d[2], first, last)
        return carry

    lax.fori_loop(0, NX, pairs, 0)

    def move(x, c, v):
        for dy in range(-2, 3):
            moved[x, (dy + 2) * 3 + c] = shifted(v, dy, 0, first, last)

    def couple(x):
        total_of = [None] * 3
        for dz in (0, 1, -1, 2, -2):
            acc = [None] * 3
            for number, d in enumerate(OFFSETS):
                if d[2] != dz:
                    continue
                other = wrap(x + d[0])
                place = (d[1] + 2) * 3
                v = [moved[other, place + c] for c in range(3)]
                s = [coef[x, number * 4 + c] for c in range(3)]
                iso = coef[x, number * 4 + 3]
                dot = s[0] * v[0] + s[1] * v[1] + s[2] * v[2]
                new = [s[c] * dot - iso * v[c] for c in range(3)]
                acc = [new[c] if acc[c] is None else acc[c] + new[c] for c in range(3)]
            acc = [roll_lanes(t, dz) for t in acc]
            total_of = [acc[c] if total_of[c] is None else total_of[c] + acc[c] for c in range(3)]
        polar = chan[x, 3]
        return [polar * t for t in total_of]

    zero = jnp.zeros((8, 128), F32)
    mine = (along >= 18) & (along < 24)

    def start(x, carry):
        for c in range(3):
            move(x, c, chan[x, 3] * chan[x, c])
        return carry

    unrolled(NX, 4, start, 0)

    def begin(x, carry):
        out = couple(x)
        for c in range(3):
            basis[0, x * 3 + c] = zero
            basis[1, x * 3 + c] = out[c]
        return carry

    lax.fori_loop(0, NX, begin, 0)

    def again(x, carry):
        for c in range(3):
            move(x, c, basis[1, x * 3 + c])
        return carry

    unrolled(NX, 4, again, 0)

    def extend(k, info):
        def one(x, sums):
            out = couple(x)
            over = chan[x, 35]
            sums = list(sums)
            for c in range(3):
                u = basis[k + 1, x * 3 + c]
                p = basis[k, x * 3 + c]
                basis[k + 2, x * 3 + c] = out[c]
                w = out[c] * over
                uw = u * over
                sums[0] = sums[0] + w * u
                sums[1] = sums[1] + w * p
                sums[2] = sums[2] + w * out[c]
                sums[3] = sums[3] + uw * u
                sums[4] = sums[4] + uw * p
                sums[5] = sums[5] + (p * over) * p
            return tuple(sums)

        sums = lax.fori_loop(0, NX, one, (zero,) * 6)
        now, past, full, norm, mixed, before = [total(jnp.where(mine, s, 0.0)) for s in sums]
        tiny = 1e-30
        al = jnp.where(norm > tiny, now / jnp.maximum(norm, tiny), 0.0)
        be = jnp.where(before > tiny, past / jnp.maximum(before, tiny), 0.0)
        rest = (
            full - 2.0 * al * now - 2.0 * be * past
            + al * al * norm + be * be * before + 2.0 * al * be * mixed
        )
        rest = jnp.maximum(rest, 1e-10 * full)
        good = (rest > tiny) & (norm > tiny)
        inv = jnp.where(good, jnp.sqrt(rest / jnp.maximum(norm, tiny)), 1.0)
        inv = jnp.minimum(jnp.maximum(inv, 1e-6), 1e3)
        sc = 1.0 / inv

        def scale(x, carry):
            for c in range(3):
                at = x * 3 + c
                new = (basis[k + 2, at] - al * basis[k + 1, at] - be * basis[k, at]) * sc
                basis[k + 2, at] = new
                move(x, c, new)
            return carry

        unrolled(NX, 4, scale, 0)
        info = jnp.where(lane == 45 + k, al, info)
        info = jnp.where(lane == 53 + k, be, info)
        return jnp.where(lane == 61 + k, inv, info)

    info = lax.fori_loop(0, ITERS, extend, zero)

    number = 0
    for low, high in ((0, 3), (3, BASIS)):
        entries = [(i, j) for i in range(low, high) for j in range(i, BASIS)]

        def one(x, sums):
            sums = list(sums)
            for c in range(3):
                u = {j: basis[j + 1, x * 3 + c] for j in range(low, BASIS)}
                for i in range(low, high):
                    weighted = u[i] * chan[x, 35]
                    for n, (p, q) in enumerate(entries):
                        if p == i:
                            sums[n] = sums[n] + weighted * u[q]
            return tuple(sums)

        sums = lax.fori_loop(0, NX, one, (zero,) * len(entries))
        for n in range(len(entries)):
            info = jnp.where(lane == number, total(jnp.where(mine, sums[n], 0.0)), info)
            number += 1

    row = lax.broadcasted_iota(jnp.int32, (8, 128), 0)
    info_out[0:8, :] = jnp.where(row == gz, info, 0.0)
    info_out[8:16, :] = jnp.where(row + 8 == gz, info, 0.0)

    def keep(x, carry):
        far = x + EDGE * gx

        def front(v):
            return pltpu.roll(v, 8 - 2 * gy, 0)

        for c in range(3):
            for k in range(BASIS):
                kept_out[x, k * 3 + c] = front(basis[k + 1, far * 3 + c])
            kept_out[x, 27 + c] = front(chan[far, 3] * chan[far, c])
        kept_out[x, 30] = front(chan[far, 35])
        return carry

    unrolled(EDGE, 2, keep, 0)


def finish_kernel(kept, info, dip_out, res_out, len_out, table):
    gz = lax.axis_index("gz_0") * 4 + lax.axis_index("gz_1")
    wide = jnp.concatenate([info[...], jnp.zeros((112, 128), F32)], axis=0)
    table[...] = wide.T
    rows = {}
    number = 0
    for low, high in ((0, 3), (3, BASIS)):
        for i in range(low, high):
            for j in range(i, BASIS):
                rows[i, j] = rows[j, i] = table[number : number + 1, :]
                number += 1
    al = [table[45 + k : 46 + k, :] for k in range(ITERS)]
    be = [table[53 + k : 54 + k, :] for k in range(ITERS)]
    inv = [table[61 + k : 62 + k, :] for k in range(ITERS)]
    lane = lax.broadcasted_iota(jnp.int32, (1, 128), 1)
    zero = jnp.zeros((1, 128), F32)
    one = jnp.where(lane < 16, 1.0, 0.0)

    def summed(v):
        return jnp.sum(v, axis=1, keepdims=True)

    def form(left, right, size_left, size_right):
        acc = zero
        for i in range(size_left):
            inner = zero
            for j in range(size_right):
                inner = inner + rows[i, j] * right[j]
            acc = acc + left[i] * inner
        return summed(acc)

    search = [one] + [zero] * ITERS
    resid = [one] + [zero] * ITERS
    moves = [zero] * BASIS
    gamma = summed(rows[0, 0])
    lengths = zero
    for k in range(ITERS):
        image = list(search)
        for j in range(k + 1):
            image[j] = image[j] - al[j] * search[j]
            image[j + 1] = image[j + 1] - inv[j] * search[j]
            if j:
                image[j - 1] = image[j - 1] - be[j] * search[j]
        step = gamma / form(search, image, k + 1, k + 2)
        lengths = jnp.where(lane == k, step, lengths)
        moves = [moves[j] + step * search[j] for j in range(BASIS)]
        resid = [resid[j] - step * image[j] for j in range(BASIS)]
        if k + 1 < ITERS:
            after = form(resid, resid, k + 2, k + 2)
            ratio = after / gamma
            search = [resid[j] + ratio * search[j] for j in range(BASIS)]
            gamma = after
    len_out[...] = lengths[:, :ITERS]
    here = lane == gz
    moves = [summed(jnp.where(here, v, 0.0)) for v in moves]
    resid = [summed(jnp.where(here, v, 0.0)) for v in resid]
    for x in range(EDGE):
        for c in range(3):
            dip = kept[x, 27 + c]
            res = jnp.zeros((8, 128), F32)
            for k in range(BASIS):
                u = kept[x, k * 3 + c]
                if k < ITERS:
                    dip = dip + moves[k] * u
                res = res + resid[k] * u
            res = res * kept[x, 30]
            for out, v in ((dip_out, dip), (res_out, res)):
                for t in range(3):
                    w = roll_lanes(v, t * WIDE + 18)
                    for s in range(2):
                        out[x, 3 * s + t, c : c + 1, :] = w[s : s + 1, :EDGE]


def per_device(permanent_field, polar, jitter, neighbors):
    packed = pl.pallas_call(
        pack_kernel,
        out_shape=jax.ShapeDtypeStruct((EDGE, GROUPS, 2, 128), F32),
        name="pack",
    )(permanent_field.transpose(0, 1, 3, 2), polar, jitter.transpose(0, 1, 3, 2), neighbors)

    both = lax.all_gather(packed, "gx", axis=0, tiled=True)
    around = [both] + [
        lax.ppermute(both, "gy", [((i + k) % 4, i) for i in range(4)]) for k in (1, 2, 3)
    ]
    own = jnp.concatenate(around, axis=2)

    def fetch(k):
        pairs = [((i + k) % 16, i) for i in range(16)]
        pairs += [(16 + (i - k) % 16, 16 + i) for i in range(16)]
        return lax.ppermute(own, ("gx",) + GZ, pairs)

    direct = [fetch(k) for k in (1, 2, 3)]
    passed = [lax.ppermute(v, "gx", [(0, 1), (1, 0)]) for v in direct]

    vreg = (8, 128)
    kept, info = pl.pallas_call(
        region_kernel,
        out_shape=(
            jax.ShapeDtypeStruct((EDGE, 31) + vreg, F32),
            jax.ShapeDtypeStruct((16, 128), F32),
        ),
        scratch_shapes=[
            pltpu.VMEM((NX, 36) + vreg, F32),
            pltpu.VMEM((NX, 20) + vreg, F32),
            pltpu.VMEM((NX, 4 * len(OFFSETS)) + vreg, F32),
            pltpu.VMEM((NX, 16) + vreg, F32),
            pltpu.VMEM((BASIS + 1, 3 * NX) + vreg, F32),
        ],
        compiler_params=pltpu.CompilerParams(vmem_limit_bytes=36 * 1024 * 1024),
        name="region",
    )(own, *direct, *passed)

    info = lax.psum(lax.psum(info, "gz_1"), "gz_0")

    dip, res, lengths = pl.pallas_call(
        finish_kernel,
        out_shape=(
            jax.ShapeDtypeStruct((EDGE, EDGE, 3, EDGE), F32),
            jax.ShapeDtypeStruct((EDGE, EDGE, 3, EDGE), F32),
            jax.ShapeDtypeStruct((1, ITERS), F32),
        ),
        scratch_shapes=[pltpu.VMEM((128, 128), F32)],
        compiler_params=pltpu.CompilerParams(vmem_limit_bytes=8 * 1024 * 1024),
        name="finish",
    )(kept, info)
    return dip.transpose(0, 1, 3, 2), res.transpose(0, 1, 3, 2), lengths.reshape(ITERS)


def solution(mesh):
    finer = Mesh(
        mesh.devices.reshape(mesh.shape["gx"], mesh.shape["gy"], 4, 4), ("gx", "gy", "gz_0", "gz_1")
    )
    return jax.shard_map(
        per_device,
        mesh=finer,
        in_specs=(
            P("gx", "gy", GZ, None),
            P("gx", "gy", GZ),
            P("gx", "gy", GZ, None),
            P("gx", "gy", GZ, None),
        ),
        out_specs=(P("gx", "gy", GZ, None), P("gx", "gy", GZ, None), P()),
        check_vma=False,
    )
```

```python
import jax
import jax.numpy as jnp
from jax import lax
from jax.experimental import pallas as pl
from jax.experimental.pallas import tpu as pltpu
from jax.sharding import Mesh
from jax.sharding import PartitionSpec as P

ITERS = 8
BASIS = ITERS + 1
THOLE = 0.39
SPACING = 3.5
EDGE = 6
NX = 12
WIDE = 42
GZ = ("gz_0", "gz_1")
F32 = jnp.float32

OFFSETS = [
    (a, b, c)
    for a in range(-2, 3)
    for b in range(-2, 3)
    for c in range(-2, 3)
    if 1 <= a * a + b * b + c * c <= 5
]
FORWARD = [d for d in OFFSETS if d > (0, 0, 0)]
GROUPS, PER = 5, 7


def lane_iota():
    return lax.broadcasted_iota(jnp.int32, (8, 128), 1)


def third_masks():
    lane = lane_iota()
    return lane < WIDE, lane >= 2 * WIDE


def roll_lanes(v, ahead):
    ahead = ahead % 128
    return v if ahead == 0 else pltpu.roll(v, 128 - ahead, 1)


def roll_rows(v, ahead):
    return pltpu.roll(v, (-ahead) % 8, 0)


def shifted(v, dy, dz, first, last):
    if dy == 0:
        return roll_lanes(v, dz)
    if dy == 1:
        return jnp.where(
            last, roll_rows(roll_lanes(v, dz - 2 * WIDE), 1), roll_lanes(v, dz + WIDE)
        )
    if dy == 2:
        return jnp.where(
            first, roll_lanes(v, dz + 2 * WIDE), roll_rows(roll_lanes(v, dz - WIDE), 1)
        )
    if dy == -1:
        return jnp.where(
            first, roll_rows(roll_lanes(v, dz + 2 * WIDE), -1), roll_lanes(v, dz - WIDE)
        )
    return jnp.where(
        last, roll_lanes(v, dz - 2 * WIDE), roll_rows(roll_lanes(v, dz + WIDE), -1)
    )


def wrap(x):
    return jnp.where(x >= NX, x - NX, jnp.where(x < 0, x + NX, x))


def total(v):
    return jnp.sum(jnp.sum(v, axis=0, keepdims=True), axis=1, keepdims=True)


def unrolled(count, times, body, carry):
    def several(i, carry):
        for t in range(times):
            carry = body(i * times + t, carry)
        return carry

    return lax.fori_loop(0, count // times, several, carry)


def pack_kernel(field, polar, jitter, neighbors, out):
    lane = lax.broadcasted_iota(jnp.int32, (1, 128), 1)
    third = jnp.where(lane >= 2 * WIDE, 2, jnp.where(lane >= WIDE, 1, 0))
    inside = lane - third * WIDE
    member = inside // EDGE
    z = inside - member * EDGE
    wanted = []
    for group in range(1, GROUPS):
        code = jnp.full((1, 128), -5000, jnp.int32)
        for n in range(PER):
            d = FORWARD[(group - 1) * PER + n]
            code = jnp.where(member == n, d[0] * 100 + d[1] * 10 + d[2], code)
        wanted.append(jnp.where(lane < 3 * WIDE, code + third * 10 + z, -5000))
    row = lax.broadcasted_iota(jnp.int32, (EDGE, 128), 0)
    column = lax.broadcasted_iota(jnp.int32, (EDGE, 128), 1)
    pick = []
    for t in range(3):
        hit = column * 0 > 0
        for n in range(PER):
            hit = hit | (column == row + (t * WIDE + n * EDGE))
        pick.append(jnp.where(hit, 1.0, 0.0))

    def one(x, carry):
        for s in range(2):
            slots = jnp.zeros((56, 128), F32)
            values = jnp.zeros((1, 128), F32)
            for t in range(3):
                y = 3 * s + t
                slots = slots + lax.dot_general(
                    neighbors[x, y].astype(F32), pick[t], (((0,), (0,)), ((), ())),
                    precision=lax.Precision.HIGHEST, preferred_element_type=F32,
                )
                parts = [field[x, y, c : c + 1, :] for c in range(3)]
                parts += [polar[x, y : y + 1, :]]
                parts += [jitter[x, y, c : c + 1, :] for c in range(3)]
                for n in range(PER):
                    wide = jnp.concatenate([parts[n], jnp.zeros((1, 122), F32)], axis=1)
                    start = t * WIDE + n * EDGE
                    values = values + (pltpu.roll(wide, start, 1) if start else wide)
            out[x, 0, s : s + 1, :] = values
            home = (x + 2) * 100 + (2 + 3 * s) * 10 + 2
            for group in range(1, GROUPS):
                target = (wanted[group - 1] + home).astype(F32)
                flag = jnp.max(jnp.where(slots == target, 1.0, 0.0), axis=0, keepdims=True)
                out[x, group, s : s + 1, :] = flag
        return carry

    lax.fori_loop(0, EDGE, one, 0)


def region_kernel(
    own, a1, a2, a3, b1, b2, b3, kept_out, info_out,
    chan, near, coef, moved, basis,
):
    gx = lax.axis_index("gx")
    gy = lax.axis_index("gy")
    lane = lane_iota()
    first, last = third_masks()
    along = lane - jnp.where(last, 2 * WIDE, jnp.where(first, 0, WIDE))
    is_low = (lane * 0 + gx) == 0

    def gather(x, carry):
        for group in range(GROUPS):
            blocks = [
                jnp.where(is_low, b3[x, group], a3[x, group]),
                jnp.where(is_low, b2[x, group], a2[x, group]),
                jnp.where(is_low, b1[x, group], a1[x, group]),
                own[x, group],
                jnp.where(is_low, a1[x, group], b1[x, group]),
                jnp.where(is_low, a2[x, group], b2[x, group]),
                jnp.where(is_low, a3[x, group], b3[x, group]),
            ]
            outs = [None] * PER
            for gap in range(-6, 7):
                members = [m for m in range(PER) if 0 <= m + gap < PER]
                mixed = blocks[members[0] + gap]
                for m in members[1:]:
                    mixed = jnp.where(along >= 6 * m, blocks[m + gap], mixed)
                mixed = roll_lanes(mixed, -6 * gap)
                for m in members:
                    outs[m] = (
                        mixed if outs[m] is None
                        else jnp.where(along >= 6 * (m + gap), mixed, outs[m])
                    )
            for member in range(PER):
                acc = outs[member]
                if group * PER + member == 3:
                    acc = jnp.where(lane >= 3 * WIDE, 1.0, acc)
                    chan[x, 35] = 1.0 / acc
                chan[x, group * PER + member] = acc
        return carry

    lax.fori_loop(0, NX, gather, 0)

    def spread(x, carry):
        for c in range(4):
            v = chan[x, 3 + c]
            for dy in range(-2, 3):
                near[x, (dy + 2) * 4 + c] = shifted(v, dy, 0, first, last)
        return carry

    unrolled(NX, 3, spread, 0)

    def pairs(x, carry):
        home = {dz: [roll_lanes(chan[x, 3 + c], -dz) for c in range(4)] for dz in range(-2, 3)}
        for number, d in enumerate(FORWARD):
            other = wrap(x + d[0])
            place = (d[1] + 2) * 4
            polar, *jit = home[d[2]]
            sep = [((near[other, place + 1 + c] - jit[c]) + float(d[c])) * SPACING for c in range(3)]
            dist_sq = sep[0] * sep[0] + sep[1] * sep[1] + sep[2] * sep[2]
            over = lax.rsqrt(dist_sq)
            cube = dist_sq * dist_sq * over
            over_sq = over * over
            over_cube = over_sq * over
            damping = THOLE * cube * lax.rsqrt(polar * near[other, place])
            falloff = jnp.exp(-damping)
            iso = (1.0 - falloff) * over_cube
            radial = 3.0 * (1.0 - (1.0 + damping) * falloff) * over_cube * over_sq
            root = jnp.sqrt(radial)
            here = roll_lanes(chan[x, 7 + number], -d[2]) > 0.5
            values = [jnp.where(here, s * root, 0.0) for s in sep] + [jnp.where(here, iso, 0.0)]
            ahead = OFFSETS.index(d) * 4
            behind = OFFSETS.index((-d[0], -d[1], -d[2])) * 4
            for c in range(4):
                coef[x, ahead + c] = values[c]
                coef[other, behind + c] = shifted(values[c], -d[1], d[2], first, last)
        return carry

    lax.fori_loop(0, NX, pairs, 0)

    def move(x, c, v):
        for dy in range(-2, 3):
            moved[x, (dy + 2) * 3 + c] = shifted(v, dy, 0, first, last)

    def couple(x):
        total_of = [None] * 3
        for dz in (0, 1, -1, 2, -2):
            acc = [None] * 3
            for number, d in enumerate(OFFSETS):
                if d[2] != dz:
                    continue
                other = wrap(x + d[0])
                place = (d[1] + 2) * 3
                v = [moved[other, place + c] for c in range(3)]
                s = [coef[x, number * 4 + c] for c in range(3)]
                iso = coef[x, number * 4 + 3]
                dot = s[0] * v[0] + s[1] * v[1] + s[2] * v[2]
                new = [s[c] * dot - iso * v[c] for c in range(3)]
                acc = [new[c] if acc[c] is None else acc[c] + new[c] for c in range(3)]
            acc = [roll_lanes(t, dz) for t in acc]
            total_of = [acc[c] if total_of[c] is None else total_of[c] + acc[c] for c in range(3)]
        polar = chan[x, 3]
        return [polar * t for t in total_of]

    zero = jnp.zeros((8, 128), F32)
    mine = (along >= 18) & (along < 24)

    def start(x, carry):
        for c in range(3):
            move(x, c, chan[x, 3] * chan[x, c])
        return carry

    unrolled(NX, 4, start, 0)

    def begin(x, carry):
        out = couple(x)
        for c in range(3):
            basis[0, x * 3 + c] = zero
            basis[1, x * 3 + c] = out[c]
        return carry

    lax.fori_loop(0, NX, begin, 0)

    def again(x, carry):
        for c in range(3):
            move(x, c, basis[1, x * 3 + c])
        return carry

    unrolled(NX, 4, again, 0)

    def extend(k, info):
        def one(x, sums):
            out = couple(x)
            over = chan[x, 35]
            sums = list(sums)
            for c in range(3):
                u = basis[k + 1, x * 3 + c]
                p = basis[k, x * 3 + c]
                basis[k + 2, x * 3 + c] = out[c]
                w = out[c] * over
                uw = u * over
                sums[0] = sums[0] + w * u
                sums[1] = sums[1] + w * p
                sums[2] = sums[2] + w * out[c]
                sums[3] = sums[3] + uw * u
                sums[4] = sums[4] + uw * p
                sums[5] = sums[5] + (p * over) * p
            return tuple(sums)

        sums = lax.fori_loop(0, NX, one, (zero,) * 6)
        now, past, full, norm, mixed, before = [total(jnp.where(mine, s, 0.0)) for s in sums]
        tiny = 1e-30
        al = jnp.where(norm > tiny, now / jnp.maximum(norm, tiny), 0.0)
        be = jnp.where(before > tiny, past / jnp.maximum(before, tiny), 0.0)
        rest = (
            full - 2.0 * al * now - 2.0 * be * past
            + al * al * norm + be * be * before + 2.0 * al * be * mixed
        )
        rest = jnp.maximum(rest, 1e-10 * full)
        good = (rest > tiny) & (norm > tiny)
        inv = jnp.where(good, jnp.sqrt(rest / jnp.maximum(norm, tiny)), 1.0)
        inv = jnp.minimum(jnp.maximum(inv, 1e-6), 1e3)
        sc = 1.0 / inv

        def scale(x, carry):
            for c in range(3):
                at = x * 3 + c
                new = (basis[k + 2, at] - al * basis[k + 1, at] - be * basis[k, at]) * sc
                basis[k + 2, at] = new
                move(x, c, new)
            return carry

        unrolled(NX, 4, scale, 0)
        info = jnp.where(lane == 45 + k, al, info)
        info = jnp.where(lane == 53 + k, be, info)
        return jnp.where(lane == 61 + k, inv, info)

    info = lax.fori_loop(0, ITERS, extend, zero)

    number = 0
    for low, high in ((0, 3), (3, BASIS)):
        entries = [(i, j) for i in range(low, high) for j in range(i, BASIS)]

        def one(x, sums):
            sums = list(sums)
            for c in range(3):
                u = {j: basis[j + 1, x * 3 + c] for j in range(low, BASIS)}
                for i in range(low, high):
                    weighted = u[i] * chan[x, 35]
                    for n, (p, q) in enumerate(entries):
                        if p == i:
                            sums[n] = sums[n] + weighted * u[q]
            return tuple(sums)

        sums = lax.fori_loop(0, NX, one, (zero,) * len(entries))
        for n in range(len(entries)):
            info = jnp.where(lane == number, total(jnp.where(mine, sums[n], 0.0)), info)
            number += 1

    for e in range(16):
        info_out[e] = info

    def keep(x, carry):
        far = x + EDGE * gx

        def front(v):
            return pltpu.roll(v, 8 - 2 * gy, 0)

        for c in range(3):
            for k in range(BASIS):
                kept_out[x, k * 3 + c] = front(basis[k + 1, far * 3 + c])
            kept_out[x, 27 + c] = front(chan[far, 3] * chan[far, c])
        kept_out[x, 30] = front(chan[far, 35])
        return carry

    unrolled(EDGE, 2, keep, 0)


def finish_kernel(kept, info, dip_out, res_out, len_out, table):
    gz = lax.axis_index("gz_0") * 4 + lax.axis_index("gz_1")
    wide = jnp.concatenate([info[e, 0:1, :] for e in range(16)] + [jnp.zeros((112, 128), F32)], axis=0)
    table[...] = wide.T
    rows = {}
    number = 0
    for low, high in ((0, 3), (3, BASIS)):
        for i in range(low, high):
            for j in range(i, BASIS):
                rows[i, j] = rows[j, i] = table[number : number + 1, :]
                number += 1
    al = [table[45 + k : 46 + k, :] for k in range(ITERS)]
    be = [table[53 + k : 54 + k, :] for k in range(ITERS)]
    inv = [table[61 + k : 62 + k, :] for k in range(ITERS)]
    lane = lax.broadcasted_iota(jnp.int32, (1, 128), 1)
    zero = jnp.zeros((1, 128), F32)
    one = jnp.where(lane < 16, 1.0, 0.0)

    def summed(v):
        return jnp.sum(v, axis=1, keepdims=True)

    def form(left, right, size_left, size_right):
        acc = zero
        for i in range(size_left):
            inner = zero
            for j in range(size_right):
                inner = inner + rows[i, j] * right[j]
            acc = acc + left[i] * inner
        return summed(acc)

    search = [one] + [zero] * ITERS
    resid = [one] + [zero] * ITERS
    moves = [zero] * BASIS
    gamma = summed(rows[0, 0])
    lengths = zero
    for k in range(ITERS):
        image = list(search)
        for j in range(k + 1):
            image[j] = image[j] - al[j] * search[j]
            image[j + 1] = image[j + 1] - inv[j] * search[j]
            if j:
                image[j - 1] = image[j - 1] - be[j] * search[j]
        step = gamma / form(search, image, k + 1, k + 2)
        lengths = jnp.where(lane == k, step, lengths)
        moves = [moves[j] + step * search[j] for j in range(BASIS)]
        resid = [resid[j] - step * image[j] for j in range(BASIS)]
        if k + 1 < ITERS:
            after = form(resid, resid, k + 2, k + 2)
            ratio = after / gamma
            search = [resid[j] + ratio * search[j] for j in range(BASIS)]
            gamma = after
    len_out[...] = lengths[:, :ITERS]
    here = lane == gz
    moves = [summed(jnp.where(here, v, 0.0)) for v in moves]
    resid = [summed(jnp.where(here, v, 0.0)) for v in resid]
    for x in range(EDGE):
        for c in range(3):
            dip = kept[x, 27 + c]
            res = jnp.zeros((8, 128), F32)
            for k in range(BASIS):
                u = kept[x, k * 3 + c]
                if k < ITERS:
                    dip = dip + moves[k] * u
                res = res + resid[k] * u
            res = res * kept[x, 30]
            for out, v in ((dip_out, dip), (res_out, res)):
                for t in range(3):
                    w = roll_lanes(v, t * WIDE + 18)
                    for s in range(2):
                        out[x, 3 * s + t, c : c + 1, :] = w[s : s + 1, :EDGE]


def per_device(permanent_field, polar, jitter, neighbors):
    packed = pl.pallas_call(
        pack_kernel,
        out_shape=jax.ShapeDtypeStruct((EDGE, GROUPS, 2, 128), F32),
        name="pack",
    )(permanent_field.transpose(0, 1, 3, 2), polar, jitter.transpose(0, 1, 3, 2), neighbors)

    copies = jnp.broadcast_to(packed[None], (8,) + packed.shape)
    plane = lax.all_to_all(copies, ("gx", "gy"), 0, 0, tiled=True)
    plane = plane.reshape(2, 4, EDGE, GROUPS, 2, 128).transpose(0, 2, 3, 1, 4, 5)
    own = plane.reshape(NX, GROUPS, 8, 128)

    def fetch(k):
        pairs = [((i + k) % 16, i) for i in range(16)]
        pairs += [(16 + (i - k) % 16, 16 + i) for i in range(16)]
        return lax.ppermute(own, ("gx",) + GZ, pairs)

    direct = [fetch(k) for k in (1, 2, 3)]
    passed = [lax.ppermute(v, "gx", [(0, 1), (1, 0)]) for v in direct]

    vreg = (8, 128)
    kept, info = pl.pallas_call(
        region_kernel,
        out_shape=(
            jax.ShapeDtypeStruct((EDGE, 31) + vreg, F32),
            jax.ShapeDtypeStruct((16,) + vreg, F32),
        ),
        scratch_shapes=[
            pltpu.VMEM((NX, 36) + vreg, F32),
            pltpu.VMEM((NX, 20) + vreg, F32),
            pltpu.VMEM((NX, 4 * len(OFFSETS)) + vreg, F32),
            pltpu.VMEM((NX, 16) + vreg, F32),
            pltpu.VMEM((BASIS + 1, 3 * NX) + vreg, F32),
        ],
        compiler_params=pltpu.CompilerParams(vmem_limit_bytes=36 * 1024 * 1024),
        name="region",
    )(own, *direct, *passed)

    info = lax.all_to_all(info, GZ, 0, 0, tiled=True)

    dip, res, lengths = pl.pallas_call(
        finish_kernel,
        out_shape=(
            jax.ShapeDtypeStruct((EDGE, EDGE, 3, EDGE), F32),
            jax.ShapeDtypeStruct((EDGE, EDGE, 3, EDGE), F32),
            jax.ShapeDtypeStruct((1, ITERS), F32),
        ),
        scratch_shapes=[pltpu.VMEM((128, 128), F32)],
        compiler_params=pltpu.CompilerParams(vmem_limit_bytes=8 * 1024 * 1024),
        name="finish",
    )(kept, info)
    return dip.transpose(0, 1, 3, 2), res.transpose(0, 1, 3, 2), lengths.reshape(ITERS)


def solution(mesh):
    finer = Mesh(
        mesh.devices.reshape(mesh.shape["gx"], mesh.shape["gy"], 4, 4), ("gx", "gy", "gz_0", "gz_1")
    )
    return jax.shard_map(
        per_device,
        mesh=finer,
        in_specs=(
            P("gx", "gy", GZ, None),
            P("gx", "gy", GZ),
            P("gx", "gy", GZ, None),
            P("gx", "gy", GZ, None),
        ),
        out_specs=(P("gx", "gy", GZ, None), P("gx", "gy", GZ, None), P()),
        check_vma=False,
    )
```

```python
import jax
import jax.numpy as jnp
from jax import lax
from jax.experimental import pallas as pl
from jax.experimental.pallas import tpu as pltpu
from jax.sharding import Mesh
from jax.sharding import PartitionSpec as P

ITERS = 8
BASIS = ITERS + 1
THOLE = 0.39
SPACING = 3.5
EDGE = 6
NX = 12
WIDE = 42
GZ = ("gz_0", "gz_1")
F32 = jnp.float32

OFFSETS = [
    (a, b, c)
    for a in range(-2, 3)
    for b in range(-2, 3)
    for c in range(-2, 3)
    if 1 <= a * a + b * b + c * c <= 5
]
FORWARD = [d for d in OFFSETS if d > (0, 0, 0)]
GROUPS, PER = 5, 7


def lane_iota():
    return lax.broadcasted_iota(jnp.int32, (8, 128), 1)


def third_masks():
    lane = lane_iota()
    return lane < WIDE, lane >= 2 * WIDE


def roll_lanes(v, ahead):
    ahead = ahead % 128
    return v if ahead == 0 else pltpu.roll(v, 128 - ahead, 1)


def roll_rows(v, ahead):
    return pltpu.roll(v, (-ahead) % 8, 0)


def shifted(v, dy, dz, first, last):
    if dy == 0:
        return roll_lanes(v, dz)
    if dy == 1:
        return jnp.where(
            last, roll_rows(roll_lanes(v, dz - 2 * WIDE), 1), roll_lanes(v, dz + WIDE)
        )
    if dy == 2:
        return jnp.where(
            first, roll_lanes(v, dz + 2 * WIDE), roll_rows(roll_lanes(v, dz - WIDE), 1)
        )
    if dy == -1:
        return jnp.where(
            first, roll_rows(roll_lanes(v, dz + 2 * WIDE), -1), roll_lanes(v, dz - WIDE)
        )
    return jnp.where(
        last, roll_lanes(v, dz - 2 * WIDE), roll_rows(roll_lanes(v, dz + WIDE), -1)
    )


def wrap(x):
    return jnp.where(x >= NX, x - NX, jnp.where(x < 0, x + NX, x))


def total(v):
    return jnp.sum(jnp.sum(v, axis=0, keepdims=True), axis=1, keepdims=True)


def unrolled(count, times, body, carry):
    def several(i, carry):
        for t in range(times):
            carry = body(i * times + t, carry)
        return carry

    return lax.fori_loop(0, count // times, several, carry)


def pack_kernel(field, polar, jitter, neighbors, out):
    lane = lax.broadcasted_iota(jnp.int32, (1, 128), 1)
    third = jnp.where(lane >= 2 * WIDE, 2, jnp.where(lane >= WIDE, 1, 0))
    inside = lane - third * WIDE
    member = inside // EDGE
    z = inside - member * EDGE
    wanted = []
    for group in range(1, GROUPS):
        code = jnp.full((1, 128), -5000, jnp.int32)
        for n in range(PER):
            d = FORWARD[(group - 1) * PER + n]
            code = jnp.where(member == n, d[0] * 100 + d[1] * 10 + d[2], code)
        wanted.append(jnp.where(lane < 3 * WIDE, code + third * 10 + z, -5000))
    row = lax.broadcasted_iota(jnp.int32, (EDGE, 128), 0)
    column = lax.broadcasted_iota(jnp.int32, (EDGE, 128), 1)
    pick = []
    for t in range(3):
        hit = column * 0 > 0
        for n in range(PER):
            hit = hit | (column == row + (t * WIDE + n * EDGE))
        pick.append((jnp.where(hit, 32.0, 0.0).astype(jnp.bfloat16), jnp.where(hit, 1.0, 0.0).astype(jnp.bfloat16)))

    def one(x, carry):
        for s in range(2):
            slots = jnp.zeros((56, 128), F32)
            values = jnp.zeros((1, 128), F32)
            for t in range(3):
                y = 3 * s + t
                entry = neighbors[x, y]
                high = lax.shift_right_arithmetic(entry, 5)
                low = entry & 31
                for part, chosen in zip((high, low), pick[t]):
                    slots = slots + lax.dot_general(
                        part.astype(F32).astype(jnp.bfloat16), chosen, (((0,), (0,)), ((), ())),
                        preferred_element_type=F32,
                    )
                parts = [field[x, y, c : c + 1, :] for c in range(3)]
                parts += [polar[x, y : y + 1, :]]
                parts += [jitter[x, y, c : c + 1, :] for c in range(3)]
                for n in range(PER):
                    wide = jnp.concatenate([parts[n], jnp.zeros((1, 122), F32)], axis=1)
                    start = t * WIDE + n * EDGE
                    values = values + (pltpu.roll(wide, start, 1) if start else wide)
            out[x, 0, s : s + 1, :] = values
            home = (x + 2) * 100 + (2 + 3 * s) * 10 + 2
            for group in range(1, GROUPS):
                target = (wanted[group - 1] + home).astype(F32)
                flag = jnp.max(jnp.where(slots == target, 1.0, 0.0), axis=0, keepdims=True)
                out[x, group, s : s + 1, :] = flag
        return carry

    unrolled(EDGE, 2, one, 0)


def region_kernel(*refs):
    mine, theirs = refs[:7], refs[7:14]
    kept_out, info_out, chan, near, coef, moved, basis = refs[14:]
    gx = lax.axis_index("gx")
    gy = lax.axis_index("gy")
    lane = lane_iota()
    first, last = third_masks()
    along = lane - jnp.where(last, 2 * WIDE, jnp.where(first, 0, WIDE))

    def gather(step, carry):
        half = step // EDGE
        at = step - half * EDGE
        x = step
        is_mine = (lane * 0 + gx) == half
        for group in range(GROUPS):
            blocks = [jnp.where(is_mine, m[at, group], t[at, group]) for m, t in zip(mine, theirs)]
            outs = [None] * PER
            for gap in range(-6, 7):
                members = [m for m in range(PER) if 0 <= m + gap < PER]
                mixed = blocks[members[0] + gap]
                for m in members[1:]:
                    mixed = jnp.where(along >= 6 * m, blocks[m + gap], mixed)
                mixed = roll_lanes(mixed, -6 * gap)
                for m in members:
                    outs[m] = (
                        mixed if outs[m] is None
                        else jnp.where(along >= 6 * (m + gap), mixed, outs[m])
                    )
            for member in range(PER):
                acc = pltpu.roll(outs[member], 2 * gy, 0)
                if group * PER + member == 3:
                    acc = jnp.where(lane >= 3 * WIDE, 1.0, acc)
                    chan[x, 35] = 1.0 / acc
                chan[x, group * PER + member] = acc
        return carry

    lax.fori_loop(0, NX, gather, 0)

    def spread(x, carry):
        for c in range(4):
            v = chan[x, 3 + c]
            for dy in range(-2, 3):
                near[x, (dy + 2) * 4 + c] = shifted(v, dy, 0, first, last)
        return carry

    unrolled(NX, 3, spread, 0)

    def pairs(x, carry):
        home = {dz: [roll_lanes(chan[x, 3 + c], -dz) for c in range(4)] for dz in range(-2, 3)}
        for number, d in enumerate(FORWARD):
            other = wrap(x + d[0])
            place = (d[1] + 2) * 4
            polar, *jit = home[d[2]]
            sep = [((near[other, place + 1 + c] - jit[c]) + float(d[c])) * SPACING for c in range(3)]
            dist_sq = sep[0] * sep[0] + sep[1] * sep[1] + sep[2] * sep[2]
            over = lax.rsqrt(dist_sq)
            cube = dist_sq * dist_sq * over
            over_sq = over * over
            over_cube = over_sq * over
            damping = THOLE * cube * lax.rsqrt(polar * near[other, place])
            falloff = jnp.exp(-damping)
            iso = (1.0 - falloff) * over_cube
            radial = 3.0 * (1.0 - (1.0 + damping) * falloff) * over_cube * over_sq
            root = jnp.sqrt(radial)
            here = roll_lanes(chan[x, 7 + number], -d[2]) > 0.5
            values = [jnp.where(here, s * root, 0.0) for s in sep] + [jnp.where(here, iso, 0.0)]
            ahead = OFFSETS.index(d) * 4
            behind = OFFSETS.index((-d[0], -d[1], -d[2])) * 4
            for c in range(4):
                coef[x, ahead + c] = values[c]
                coef[other, behind + c] = shifted(values[c], -d[1], d[2], first, last)
        return carry

    lax.fori_loop(0, NX, pairs, 0)

    def move(x, c, v):
        for dy in range(-2, 3):
            moved[x, (dy + 2) * 3 + c] = shifted(v, dy, 0, first, last)

    def couple(x):
        acc = {dz: [None] * 3 for dz in range(-2, 3)}
        for dx in range(-2, 3):
            other = wrap(x + dx)
            for dy in range(-2, 3):
                v = [moved[other, (dy + 2) * 3 + c] for c in range(3)]
                for dz in range(-2, 3):
                    if (dx, dy, dz) not in OFFSETS:
                        continue
                    number = OFFSETS.index((dx, dy, dz)) * 4
                    s = [coef[x, number + c] for c in range(3)]
                    iso = coef[x, number + 3]
                    dot = s[0] * v[0] + s[1] * v[1] + s[2] * v[2]
                    new = [s[c] * dot - iso * v[c] for c in range(3)]
                    acc[dz] = [n if t is None else t + n for t, n in zip(acc[dz], new)]
        out = acc[0]
        for dz in (1, -1, 2, -2):
            out = [o + roll_lanes(t, dz) for o, t in zip(out, acc[dz])]
        return out

    zero = jnp.zeros((8, 128), F32)
    slab = (along >= 18) & (along < 24)

    def start(x, carry):
        for c in range(3):
            move(x, c, chan[x, 3] * chan[x, c])
        return carry

    unrolled(NX, 4, start, 0)

    def begin(x, carry):
        out = couple(x)
        polar = chan[x, 3]
        for c in range(3):
            basis[0, x * 3 + c] = zero
            basis[1, x * 3 + c] = polar * out[c]
        return carry

    unrolled(NX, 3, begin, 0)

    def again(x, carry):
        for c in range(3):
            move(x, c, basis[1, x * 3 + c])
        return carry

    unrolled(NX, 4, again, 0)

    def extend(k, carry):
        info, before = carry

        def one(x, sums):
            out = couple(x)
            polar = chan[x, 3]
            over = chan[x, 35]
            sums = list(sums)
            for c in range(3):
                u = basis[k + 1, x * 3 + c]
                w = polar * out[c]
                basis[k + 2, x * 3 + c] = w
                sums[0] = sums[0] + out[c] * u
                sums[1] = sums[1] + out[c] * basis[k, x * 3 + c]
                sums[2] = sums[2] + out[c] * w
                sums[3] = sums[3] + (u * over) * u
            return tuple(sums)

        sums = unrolled(NX, 3, one, (zero,) * 4)
        now, past, full, norm = [total(jnp.where(slab, s, 0.0)) for s in sums]
        tiny = 1e-36
        al = jnp.where(norm > tiny, now / jnp.maximum(norm, tiny), 0.0)
        be = jnp.where(before > tiny, past / jnp.maximum(before, tiny), 0.0)
        rest = full - al * now - be * past
        rest = jnp.maximum(rest, 1e-10 * full)
        good = (rest > tiny) & (norm > tiny)
        inv = jnp.where(good, jnp.sqrt(rest / jnp.maximum(norm, tiny)), 1.0)
        inv = jnp.minimum(jnp.maximum(inv, 1e-6), 1e3)
        sc = 1.0 / inv

        def scale(x, carry):
            for c in range(3):
                at = x * 3 + c
                new = (basis[k + 2, at] - al * basis[k + 1, at] - be * basis[k, at]) * sc
                basis[k + 2, at] = new
                move(x, c, new)
            return carry

        unrolled(NX, 4, scale, 0)
        info = jnp.where(lane == 45 + k, al, info)
        info = jnp.where(lane == 53 + k, be, info)
        return jnp.where(lane == 61 + k, inv, info), norm

    info, _ = lax.fori_loop(0, ITERS, extend, (zero, jnp.zeros((1, 1), F32)))

    number = 0
    for low, high in ((0, 3), (3, BASIS)):
        entries = [(i, j) for i in range(low, high) for j in range(i, BASIS)]

        def one(x, sums):
            sums = list(sums)
            for c in range(3):
                u = {j: basis[j + 1, x * 3 + c] for j in range(low, BASIS)}
                for i in range(low, high):
                    weighted = u[i] * chan[x, 35]
                    for n, (p, q) in enumerate(entries):
                        if p == i:
                            sums[n] = sums[n] + weighted * u[q]
            return tuple(sums)

        sums = unrolled(NX, 2, one, (zero,) * len(entries))
        for n in range(len(entries)):
            info = jnp.where(lane == number, total(jnp.where(slab, sums[n], 0.0)), info)
            number += 1

    for e in range(16):
        info_out[e] = info

    def keep(x, carry):
        far = x + EDGE * gx

        def front(v):
            return pltpu.roll(v, 8 - 2 * gy, 0)

        for c in range(3):
            for k in range(BASIS):
                kept_out[x, k * 3 + c] = front(basis[k + 1, far * 3 + c])
            kept_out[x, 27 + c] = front(chan[far, 3] * chan[far, c])
        kept_out[x, 30] = front(chan[far, 35])
        return carry

    unrolled(EDGE, 2, keep, 0)


def finish_kernel(kept, info, dip_out, res_out, len_out, table):
    gz = lax.axis_index("gz_0") * 4 + lax.axis_index("gz_1")
    wide = jnp.concatenate([info[e, 0:1, :] for e in range(16)] + [jnp.zeros((112, 128), F32)], axis=0)
    table[...] = wide.T
    rows = {}
    number = 0
    for low, high in ((0, 3), (3, BASIS)):
        for i in range(low, high):
            for j in range(i, BASIS):
                rows[i, j] = rows[j, i] = table[number : number + 1, :]
                number += 1
    al = [table[45 + k : 46 + k, :] for k in range(ITERS)]
    be = [table[53 + k : 54 + k, :] for k in range(ITERS)]
    inv = [table[61 + k : 62 + k, :] for k in range(ITERS)]
    lane = lax.broadcasted_iota(jnp.int32, (1, 128), 1)
    zero = jnp.zeros((1, 128), F32)
    one = jnp.where(lane < 16, 1.0, 0.0)

    def summed(v):
        return jnp.sum(v, axis=1, keepdims=True)

    def form(left, right, size_left, size_right):
        acc = zero
        for i in range(size_left):
            inner = zero
            for j in range(size_right):
                inner = inner + rows[i, j] * right[j]
            acc = acc + left[i] * inner
        return summed(acc)

    search = [one] + [zero] * ITERS
    resid = [one] + [zero] * ITERS
    moves = [zero] * BASIS
    gamma = summed(rows[0, 0])
    lengths = zero
    for k in range(ITERS):
        image = list(search)
        for j in range(k + 1):
            image[j] = image[j] - al[j] * search[j]
            image[j + 1] = image[j + 1] - inv[j] * search[j]
            if j:
                image[j - 1] = image[j - 1] - be[j] * search[j]
        step = gamma / form(search, image, k + 1, k + 2)
        lengths = jnp.where(lane == k, step, lengths)
        moves = [moves[j] + step * search[j] for j in range(BASIS)]
        resid = [resid[j] - step * image[j] for j in range(BASIS)]
        if k + 1 < ITERS:
            after = form(resid, resid, k + 2, k + 2)
            ratio = after / gamma
            search = [resid[j] + ratio * search[j] for j in range(BASIS)]
            gamma = after
    len_out[...] = lengths[:, :ITERS]
    here = lane == gz
    moves = [summed(jnp.where(here, v, 0.0)) for v in moves]
    resid = [summed(jnp.where(here, v, 0.0)) for v in resid]
    for x in range(EDGE):
        for c in range(3):
            dip = kept[x, 27 + c]
            res = jnp.zeros((8, 128), F32)
            for k in range(BASIS):
                u = kept[x, k * 3 + c]
                if k < ITERS:
                    dip = dip + moves[k] * u
                res = res + resid[k] * u
            res = res * kept[x, 30]
            for out, v in ((dip_out, dip), (res_out, res)):
                for t in range(3):
                    w = roll_lanes(v, t * WIDE + 18)
                    for s in range(2):
                        out[x, 3 * s + t, c : c + 1, :] = w[s : s + 1, :EDGE]


REGION_IN = 14


def per_device(permanent_field, polar, jitter, neighbors):
    packed = pl.pallas_call(
        pack_kernel,
        out_shape=jax.ShapeDtypeStruct((EDGE, GROUPS, 2, 128), F32),
        compiler_params=pltpu.CompilerParams(vmem_limit_bytes=8 * 1024 * 1024),
        name="pack",
    )(permanent_field.transpose(0, 1, 3, 2), polar, jitter.transpose(0, 1, 3, 2), neighbors)

    around = [packed] + [
        lax.ppermute(packed, "gy", [((i + k) % 4, i) for i in range(4)]) for k in (1, 2, 3)
    ]
    own = jnp.concatenate(around, axis=2)

    def swap(v):
        return lax.ppermute(v, "gx", [(0, 1), (1, 0)])

    far = {k: lax.ppermute(own, GZ, [((i + k) % 16, i) for i in range(16)]) for k in (3, -3, 2, -2, 1, -1)}
    far[0] = own
    mine = [far[k] for k in range(-3, 4)]
    theirs = [swap(v) for v in mine]

    vreg = (8, 128)
    kept, info = pl.pallas_call(
        region_kernel,
        out_shape=(
            jax.ShapeDtypeStruct((EDGE, 31) + vreg, F32),
            jax.ShapeDtypeStruct((16,) + vreg, F32),
        ),
        scratch_shapes=[
            pltpu.VMEM((NX, 36) + vreg, F32),
            pltpu.VMEM((NX, 20) + vreg, F32),
            pltpu.VMEM((NX, 4 * len(OFFSETS)) + vreg, F32),
            pltpu.VMEM((NX, 16) + vreg, F32),
            pltpu.VMEM((BASIS + 1, 3 * NX) + vreg, F32),
        ],
        compiler_params=pltpu.CompilerParams(vmem_limit_bytes=36 * 1024 * 1024),
        name="region",
    )(*mine, *theirs)

    info = lax.all_to_all(info, GZ, 0, 0, tiled=True)

    dip, res, lengths = pl.pallas_call(
        finish_kernel,
        out_shape=(
            jax.ShapeDtypeStruct((EDGE, EDGE, 3, EDGE), F32),
            jax.ShapeDtypeStruct((EDGE, EDGE, 3, EDGE), F32),
            jax.ShapeDtypeStruct((1, ITERS), F32),
        ),
        scratch_shapes=[pltpu.VMEM((128, 128), F32)],
        compiler_params=pltpu.CompilerParams(vmem_limit_bytes=8 * 1024 * 1024),
        name="finish",
    )(kept, info)
    return dip.transpose(0, 1, 3, 2), res.transpose(0, 1, 3, 2), lengths.reshape(ITERS)


def solution(mesh):
    finer = Mesh(
        mesh.devices.reshape(mesh.shape["gx"], mesh.shape["gy"], 4, 4), ("gx", "gy", "gz_0", "gz_1")
    )
    return jax.shard_map(
        per_device,
        mesh=finer,
        in_specs=(
            P("gx", "gy", GZ, None),
            P("gx", "gy", GZ),
            P("gx", "gy", GZ, None),
            P("gx", "gy", GZ, None),
        ),
        out_specs=(P("gx", "gy", GZ, None), P("gx", "gy", GZ, None), P()),
        check_vma=False,
    )
```

```python
import jax
import jax.numpy as jnp
from jax import lax
from jax.experimental import pallas as pl
from jax.experimental.pallas import tpu as pltpu
from jax.sharding import Mesh
from jax.sharding import PartitionSpec as P

ITERS = 8
BASIS = ITERS + 1
THOLE = 0.39
SPACING = 3.5
EDGE = 6
NX = 12
WIDE = 42
GZ = ("gz_0", "gz_1")
F32 = jnp.float32

OFFSETS = [
    (a, b, c)
    for a in range(-2, 3)
    for b in range(-2, 3)
    for c in range(-2, 3)
    if 1 <= a * a + b * b + c * c <= 5
]
FORWARD = [d for d in OFFSETS if d > (0, 0, 0)]
GROUPS, PER = 5, 7


def lane_iota():
    return lax.broadcasted_iota(jnp.int32, (8, 128), 1)


def third_masks():
    lane = lane_iota()
    return lane < WIDE, lane >= 2 * WIDE


def roll_lanes(v, ahead):
    ahead = ahead % 128
    return v if ahead == 0 else pltpu.roll(v, 128 - ahead, 1)


def roll_rows(v, ahead):
    return pltpu.roll(v, (-ahead) % 8, 0)


def shifted(v, dy, dz, first, last):
    if dy == 0:
        return roll_lanes(v, dz)
    if dy == 1:
        return jnp.where(
            last, roll_rows(roll_lanes(v, dz - 2 * WIDE), 1), roll_lanes(v, dz + WIDE)
        )
    if dy == 2:
        return jnp.where(
            first, roll_lanes(v, dz + 2 * WIDE), roll_rows(roll_lanes(v, dz - WIDE), 1)
        )
    if dy == -1:
        return jnp.where(
            first, roll_rows(roll_lanes(v, dz + 2 * WIDE), -1), roll_lanes(v, dz - WIDE)
        )
    return jnp.where(
        last, roll_lanes(v, dz - 2 * WIDE), roll_rows(roll_lanes(v, dz + WIDE), -1)
    )


def wrap(x):
    return jnp.where(x >= NX, x - NX, jnp.where(x < 0, x + NX, x))


def total(v):
    return jnp.sum(jnp.sum(v, axis=0, keepdims=True), axis=1, keepdims=True)


def unrolled(count, times, body, carry):
    def several(i, carry):
        for t in range(times):
            carry = body(i * times + t, carry)
        return carry

    return lax.fori_loop(0, count // times, several, carry)


def pack_kernel(
    field_in, polar_in, jitter_in, neighbors_in, out, field, polar, jitter, neighbors, arrived
):
    given = (neighbors_in, field_in, jitter_in, polar_in)
    kept = (neighbors, field, jitter, polar)
    copies = [pltpu.make_async_copy(g, k, arrived.at[n]) for n, (g, k) in enumerate(zip(given, kept))]
    for copy in copies:
        copy.start()
    lane = lax.broadcasted_iota(jnp.int32, (1, 128), 1)
    third = jnp.where(lane >= 2 * WIDE, 2, jnp.where(lane >= WIDE, 1, 0))
    inside = lane - third * WIDE
    member = inside // EDGE
    z = inside - member * EDGE
    wanted = []
    for group in range(1, GROUPS):
        code = jnp.full((1, 128), -5000, jnp.int32)
        for n in range(PER):
            d = FORWARD[(group - 1) * PER + n]
            code = jnp.where(member == n, d[0] * 100 + d[1] * 10 + d[2], code)
        wanted.append(jnp.where(lane < 3 * WIDE, code + third * 10 + z, -5000))
    row = lax.broadcasted_iota(jnp.int32, (EDGE, 128), 0)
    column = lax.broadcasted_iota(jnp.int32, (EDGE, 128), 1)
    pick = []
    for t in range(3):
        hit = column * 0 > 0
        for n in range(PER):
            hit = hit | (column == row + (t * WIDE + n * EDGE))
        pick.append((jnp.where(hit, 32.0, 0.0).astype(jnp.bfloat16), jnp.where(hit, 1.0, 0.0).astype(jnp.bfloat16)))

    for copy in copies:
        copy.wait()

    def one(x, carry):
        for s in range(2):
            slots = jnp.zeros((56, 128), F32)
            values = jnp.zeros((1, 128), F32)
            for t in range(3):
                y = 3 * s + t
                entry = neighbors[x, y]
                high = lax.shift_right_arithmetic(entry, 5)
                low = entry & 31
                for part, chosen in zip((high, low), pick[t]):
                    slots = slots + lax.dot_general(
                        part.astype(F32).astype(jnp.bfloat16), chosen, (((0,), (0,)), ((), ())),
                        preferred_element_type=F32,
                    )
                parts = [field[x, y, c : c + 1, :] for c in range(3)]
                parts += [polar[x, y : y + 1, :]]
                parts += [jitter[x, y, c : c + 1, :] for c in range(3)]
                for n in range(PER):
                    wide = jnp.concatenate([parts[n], jnp.zeros((1, 122), F32)], axis=1)
                    start = t * WIDE + n * EDGE
                    values = values + (pltpu.roll(wide, start, 1) if start else wide)
            out[x, 0, s : s + 1, :] = values
            home = (x + 2) * 100 + (2 + 3 * s) * 10 + 2
            for group in range(1, GROUPS):
                target = (wanted[group - 1] + home).astype(F32)
                flag = jnp.max(jnp.where(slots == target, 1.0, 0.0), axis=0, keepdims=True)
                out[x, group, s : s + 1, :] = flag
        return carry

    unrolled(EDGE, 2, one, 0)


def region_kernel(
    own, a1, a2, a3, b1, b2, b3, kept_out, info_out, chan, near, coef, moved, basis,
):
    gx = lax.axis_index("gx")
    gy = lax.axis_index("gy")
    lane = lane_iota()
    first, last = third_masks()
    along = lane - jnp.where(last, 2 * WIDE, jnp.where(first, 0, WIDE))
    is_low = (lane * 0 + gx) == 0

    def gather(x, carry):
        half = x // EDGE
        within = x - half * EDGE
        here = within + jnp.where(half == gx, 0, EDGE)
        there = within + jnp.where(half == gx, EDGE, 0)
        for group in range(GROUPS):
            ahead = [jnp.where(is_low, a[here, group], b[there, group]) for a, b in ((a1, b1), (a2, b2), (a3, b3))]
            back = [jnp.where(is_low, b[there, group], a[here, group]) for a, b in ((a3, b3), (a2, b2), (a1, b1))]
            blocks = back + [own[here, group]] + ahead
            outs = [None] * PER
            for gap in range(-6, 7):
                members = [m for m in range(PER) if 0 <= m + gap < PER]
                mixed = blocks[members[0] + gap]
                for m in members[1:]:
                    mixed = jnp.where(along >= 6 * m, blocks[m + gap], mixed)
                mixed = roll_lanes(mixed, -6 * gap)
                for m in members:
                    outs[m] = (
                        mixed if outs[m] is None
                        else jnp.where(along >= 6 * (m + gap), mixed, outs[m])
                    )
            for member in range(PER):
                acc = pltpu.roll(outs[member], 2 * gy, 0)
                if group * PER + member == 3:
                    acc = jnp.where(lane >= 3 * WIDE, 1.0, acc)
                    chan[x, 35] = 1.0 / acc
                chan[x, group * PER + member] = acc
        return carry

    lax.fori_loop(0, NX, gather, 0)

    def spread(x, carry):
        for c in range(4):
            v = chan[x, 3 + c]
            for dy in range(-2, 3):
                near[x, (dy + 2) * 4 + c] = shifted(v, dy, 0, first, last)
        return carry

    unrolled(NX, 3, spread, 0)

    def pairs(x, carry):
        home = {dz: [roll_lanes(chan[x, 3 + c], -dz) for c in range(4)] for dz in range(-2, 3)}
        for number, d in enumerate(FORWARD):
            other = wrap(x + d[0])
            place = (d[1] + 2) * 4
            polar, *jit = home[d[2]]
            sep = [((near[other, place + 1 + c] - jit[c]) + float(d[c])) * SPACING for c in range(3)]
            dist_sq = sep[0] * sep[0] + sep[1] * sep[1] + sep[2] * sep[2]
            over = lax.rsqrt(dist_sq)
            cube = dist_sq * dist_sq * over
            over_sq = over * over
            over_cube = over_sq * over
            damping = THOLE * cube * lax.rsqrt(polar * near[other, place])
            falloff = jnp.exp(-damping)
            iso = (1.0 - falloff) * over_cube
            radial = 3.0 * (1.0 - (1.0 + damping) * falloff) * over_cube * over_sq
            root = jnp.sqrt(radial)
            here = roll_lanes(chan[x, 7 + number], -d[2]) > 0.5
            values = [jnp.where(here, s * root, 0.0) for s in sep] + [jnp.where(here, iso, 0.0)]
            ahead = OFFSETS.index(d) * 4
            behind = OFFSETS.index((-d[0], -d[1], -d[2])) * 4
            for c in range(4):
                coef[x, ahead + c] = values[c]
                coef[other, behind + c] = shifted(values[c], -d[1], d[2], first, last)
        return carry

    lax.fori_loop(0, NX, pairs, 0)

    def move(x, c, v):
        for dy in range(-2, 3):
            moved[x, (dy + 2) * 3 + c] = shifted(v, dy, 0, first, last)

    def couple(x):
        acc = {dz: [None] * 3 for dz in range(-2, 3)}
        for dx in range(-2, 3):
            other = wrap(x + dx)
            for dy in range(-2, 3):
                v = [moved[other, (dy + 2) * 3 + c] for c in range(3)]
                for dz in range(-2, 3):
                    if (dx, dy, dz) not in OFFSETS:
                        continue
                    number = OFFSETS.index((dx, dy, dz)) * 4
                    s = [coef[x, number + c] for c in range(3)]
                    iso = coef[x, number + 3]
                    dot = s[0] * v[0] + s[1] * v[1] + s[2] * v[2]
                    new = [s[c] * dot - iso * v[c] for c in range(3)]
                    acc[dz] = [n if t is None else t + n for t, n in zip(acc[dz], new)]
        out = acc[0]
        for dz in (1, -1, 2, -2):
            out = [o + roll_lanes(t, dz) for o, t in zip(out, acc[dz])]
        return out

    zero = jnp.zeros((8, 128), F32)
    slab = (along >= 18) & (along < 24)

    def start(x, carry):
        for c in range(3):
            move(x, c, chan[x, 3] * chan[x, c])
        return carry

    unrolled(NX, 4, start, 0)

    def begin(x, carry):
        out = couple(x)
        polar = chan[x, 3]
        for c in range(3):
            basis[0, x * 3 + c] = zero
            basis[1, x * 3 + c] = polar * out[c]
        return carry

    unrolled(NX, 3, begin, 0)

    def again(x, carry):
        for c in range(3):
            move(x, c, basis[1, x * 3 + c])
        return carry

    unrolled(NX, 4, again, 0)

    def extend(k, carry):
        info, before = carry

        def one(x, sums):
            out = couple(x)
            polar = chan[x, 3]
            over = chan[x, 35]
            sums = list(sums)
            for c in range(3):
                u = basis[k + 1, x * 3 + c]
                w = polar * out[c]
                basis[k + 2, x * 3 + c] = w
                sums[0] = sums[0] + out[c] * u
                sums[1] = sums[1] + out[c] * basis[k, x * 3 + c]
                sums[2] = sums[2] + out[c] * w
                sums[3] = sums[3] + (u * over) * u
            return tuple(sums)

        sums = unrolled(NX, 3, one, (zero,) * 4)
        now, past, full, norm = [total(jnp.where(slab, s, 0.0)) for s in sums]
        tiny = 1e-36
        al = jnp.where(norm > tiny, now / jnp.maximum(norm, tiny), 0.0)
        be = jnp.where(before > tiny, past / jnp.maximum(before, tiny), 0.0)
        rest = full - al * now - be * past
        rest = jnp.maximum(rest, 1e-10 * full)
        good = (rest > tiny) & (norm > tiny)
        inv = jnp.where(good, jnp.sqrt(rest / jnp.maximum(norm, tiny)), 1.0)
        inv = jnp.minimum(jnp.maximum(inv, 1e-6), 1e3)
        sc = 1.0 / inv

        def scale(x, carry):
            for c in range(3):
                at = x * 3 + c
                new = (basis[k + 2, at] - al * basis[k + 1, at] - be * basis[k, at]) * sc
                basis[k + 2, at] = new
                move(x, c, new)
            return carry

        unrolled(NX, 4, scale, 0)
        info = jnp.where(lane == 45 + k, al, info)
        info = jnp.where(lane == 53 + k, be, info)
        return jnp.where(lane == 61 + k, inv, info), norm

    info, _ = lax.fori_loop(0, ITERS, extend, (zero, jnp.zeros((1, 1), F32)))

    number = 0
    for low, high in ((0, 3), (3, BASIS)):
        entries = [(i, j) for i in range(low, high) for j in range(i, BASIS)]

        def one(x, sums):
            sums = list(sums)
            for c in range(3):
                u = {j: basis[j + 1, x * 3 + c] for j in range(low, BASIS)}
                for i in range(low, high):
                    weighted = u[i] * chan[x, 35]
                    for n, (p, q) in enumerate(entries):
                        if p == i:
                            sums[n] = sums[n] + weighted * u[q]
            return tuple(sums)

        sums = unrolled(NX, 2, one, (zero,) * len(entries))
        for n in range(len(entries)):
            info = jnp.where(lane == number, total(jnp.where(slab, sums[n], 0.0)), info)
            number += 1

    for e in range(16):
        info_out[e] = info

    def keep(x, carry):
        far = x + EDGE * gx

        def front(v):
            return pltpu.roll(v, 8 - 2 * gy, 0)

        for c in range(3):
            for k in range(BASIS):
                kept_out[x, k * 3 + c] = front(basis[k + 1, far * 3 + c])
            kept_out[x, 27 + c] = front(chan[far, 3] * chan[far, c])
        kept_out[x, 30] = front(chan[far, 35])
        return carry

    unrolled(EDGE, 2, keep, 0)


def finish_kernel(kept, info, dip_out, res_out, len_out, table):
    gz = lax.axis_index("gz_0") * 4 + lax.axis_index("gz_1")
    wide = jnp.concatenate([info[e, 0:1, :] for e in range(16)] + [jnp.zeros((112, 128), F32)], axis=0)
    table[...] = wide.T
    rows = {}
    number = 0
    for low, high in ((0, 3), (3, BASIS)):
        for i in range(low, high):
            for j in range(i, BASIS):
                rows[i, j] = rows[j, i] = table[number : number + 1, :]
                number += 1
    al = [table[45 + k : 46 + k, :] for k in range(ITERS)]
    be = [table[53 + k : 54 + k, :] for k in range(ITERS)]
    inv = [table[61 + k : 62 + k, :] for k in range(ITERS)]
    lane = lax.broadcasted_iota(jnp.int32, (1, 128), 1)
    zero = jnp.zeros((1, 128), F32)
    one = jnp.where(lane < 16, 1.0, 0.0)

    def summed(v):
        return jnp.sum(v, axis=1, keepdims=True)

    def form(left, right, size_left, size_right):
        acc = zero
        for i in range(size_left):
            inner = zero
            for j in range(size_right):
                inner = inner + rows[i, j] * right[j]
            acc = acc + left[i] * inner
        return summed(acc)

    search = [one] + [zero] * ITERS
    resid = [one] + [zero] * ITERS
    moves = [zero] * BASIS
    gamma = summed(rows[0, 0])
    lengths = zero
    for k in range(ITERS):
        image = list(search)
        for j in range(k + 1):
            image[j] = image[j] - al[j] * search[j]
            image[j + 1] = image[j + 1] - inv[j] * search[j]
            if j:
                image[j - 1] = image[j - 1] - be[j] * search[j]
        step = gamma / form(search, image, k + 1, k + 2)
        lengths = jnp.where(lane == k, step, lengths)
        moves = [moves[j] + step * search[j] for j in range(BASIS)]
        resid = [resid[j] - step * image[j] for j in range(BASIS)]
        if k + 1 < ITERS:
            after = form(resid, resid, k + 2, k + 2)
            ratio = after / gamma
            search = [resid[j] + ratio * search[j] for j in range(BASIS)]
            gamma = after
    len_out[...] = lengths[:, :ITERS]
    here = lane == gz
    moves = [summed(jnp.where(here, v, 0.0)) for v in moves]
    resid = [summed(jnp.where(here, v, 0.0)) for v in resid]
    for x in range(EDGE):
        for c in range(3):
            dip = kept[x, 27 + c]
            res = jnp.zeros((8, 128), F32)
            for k in range(BASIS):
                u = kept[x, k * 3 + c]
                if k < ITERS:
                    dip = dip + moves[k] * u
                res = res + resid[k] * u
            res = res * kept[x, 30]
            for out, v in ((dip_out, dip), (res_out, res)):
                for t in range(3):
                    w = roll_lanes(v, t * WIDE + 18)
                    for s in range(2):
                        out[x, 3 * s + t, c : c + 1, :] = w[s : s + 1, :EDGE]


def per_device(permanent_field, polar, jitter, neighbors):
    packed = pl.pallas_call(
        pack_kernel,
        out_shape=jax.ShapeDtypeStruct((EDGE, GROUPS, 2, 128), F32),
        in_specs=[pl.BlockSpec(memory_space=pltpu.HBM)] * 4,
        scratch_shapes=[
            pltpu.VMEM((EDGE, EDGE, 3, EDGE), F32),
            pltpu.VMEM((EDGE, EDGE, EDGE), F32),
            pltpu.VMEM((EDGE, EDGE, 3, EDGE), F32),
            pltpu.VMEM((EDGE, EDGE, EDGE, 56), jnp.int32),
            pltpu.SemaphoreType.DMA((4,)),
        ],
        compiler_params=pltpu.CompilerParams(vmem_limit_bytes=60 * 1024 * 1024),
        name="pack",
    )(permanent_field.transpose(0, 1, 3, 2), polar, jitter.transpose(0, 1, 3, 2), neighbors)

    around = [packed] + [
        lax.ppermute(packed, "gy", [((i + k) % 4, i) for i in range(4)]) for k in (1, 2, 3)
    ]
    half = jnp.concatenate(around, axis=2)

    def swap(v):
        return lax.ppermute(v, "gx", [(0, 1), (1, 0)])

    own = jnp.concatenate([half, swap(half)], axis=0)

    def fetch(k):
        pairs = [((i + k) % 16, i) for i in range(16)]
        pairs += [(16 + (i - k) % 16, 16 + i) for i in range(16)]
        return lax.ppermute(own, ("gx",) + GZ, pairs)

    direct = [fetch(k) for k in (1, 2, 3)]
    passed = [swap(v) for v in direct]

    vreg = (8, 128)
    kept, info = pl.pallas_call(
        region_kernel,
        out_shape=(
            jax.ShapeDtypeStruct((EDGE, 31) + vreg, F32),
            jax.ShapeDtypeStruct((16,) + vreg, F32),
        ),
        scratch_shapes=[
            pltpu.VMEM((NX, 36) + vreg, F32),
            pltpu.VMEM((NX, 20) + vreg, F32),
            pltpu.VMEM((NX, 4 * len(OFFSETS)) + vreg, F32),
            pltpu.VMEM((NX, 16) + vreg, F32),
            pltpu.VMEM((BASIS + 1, 3 * NX) + vreg, F32),
        ],
        compiler_params=pltpu.CompilerParams(vmem_limit_bytes=36 * 1024 * 1024),
        name="region",
    )(own, *direct, *passed)

    info = lax.all_to_all(info, GZ, 0, 0, tiled=True)

    dip, res, lengths = pl.pallas_call(
        finish_kernel,
        out_shape=(
            jax.ShapeDtypeStruct((EDGE, EDGE, 3, EDGE), F32),
            jax.ShapeDtypeStruct((EDGE, EDGE, 3, EDGE), F32),
            jax.ShapeDtypeStruct((1, ITERS), F32),
        ),
        scratch_shapes=[pltpu.VMEM((128, 128), F32)],
        compiler_params=pltpu.CompilerParams(vmem_limit_bytes=8 * 1024 * 1024),
        name="finish",
    )(kept, info)
    return dip.transpose(0, 1, 3, 2), res.transpose(0, 1, 3, 2), lengths.reshape(ITERS)


def solution(mesh):
    finer = Mesh(
        mesh.devices.reshape(mesh.shape["gx"], mesh.shape["gy"], 4, 4), ("gx", "gy", "gz_0", "gz_1")
    )
    return jax.shard_map(
        per_device,
        mesh=finer,
        in_specs=(
            P("gx", "gy", GZ, None),
            P("gx", "gy", GZ),
            P("gx", "gy", GZ, None),
            P("gx", "gy", GZ, None),
        ),
        out_specs=(P("gx", "gy", GZ, None), P("gx", "gy", GZ, None), P()),
        check_vma=False,
    )
```

```python
import jax
import jax.numpy as jnp
from jax import lax
from jax.experimental import pallas as pl
from jax.experimental.pallas import tpu as pltpu
from jax.sharding import Mesh
from jax.sharding import PartitionSpec as P


ITERS = 8
BASIS = ITERS + 1
THOLE = 0.39
SPACING = 3.5
EDGE = 6
NX = 12
WIDE = 42
GZ = ("gz_0", "gz_1")
F32 = jnp.float32

OFFSETS = [
    (a, b, c)
    for a in range(-2, 3)
    for b in range(-2, 3)
    for c in range(-2, 3)
    if 1 <= a * a + b * b + c * c <= 5
]
FORWARD = [d for d in OFFSETS if d > (0, 0, 0)]
GROUPS, PER = 5, 7


def lane_iota():
    return lax.broadcasted_iota(jnp.int32, (8, 128), 1)


def third_masks():
    lane = lane_iota()
    return lane < WIDE, lane >= 2 * WIDE


def roll_lanes(v, ahead):
    ahead = ahead % 128
    return v if ahead == 0 else pltpu.roll(v, 128 - ahead, 1)


def roll_rows(v, ahead):
    return pltpu.roll(v, (-ahead) % 8, 0)


def shifted(v, dy, dz, first, last):
    if dy == 0:
        return roll_lanes(v, dz)
    if dy == 1:
        return jnp.where(
            last, roll_rows(roll_lanes(v, dz - 2 * WIDE), 1), roll_lanes(v, dz + WIDE)
        )
    if dy == 2:
        return jnp.where(
            first, roll_lanes(v, dz + 2 * WIDE), roll_rows(roll_lanes(v, dz - WIDE), 1)
        )
    if dy == -1:
        return jnp.where(
            first, roll_rows(roll_lanes(v, dz + 2 * WIDE), -1), roll_lanes(v, dz - WIDE)
        )
    return jnp.where(
        last, roll_lanes(v, dz - 2 * WIDE), roll_rows(roll_lanes(v, dz + WIDE), -1)
    )


def wrap(x):
    return jnp.where(x >= NX, x - NX, jnp.where(x < 0, x + NX, x))


def total(v):
    return jnp.sum(jnp.sum(v, axis=0, keepdims=True), axis=1, keepdims=True)


def unrolled(count, times, body, carry):
    def several(i, carry):
        for t in range(times):
            carry = body(i * times + t, carry)
        return carry

    return lax.fori_loop(0, count // times, several, carry)


def pack_kernel(
    field_in, polar_in, jitter_in, neighbors_in, out, field, polar, jitter, neighbors, arrived
):
    given = (neighbors_in, field_in, jitter_in, polar_in)
    kept = (neighbors, field, jitter, polar)
    copies = [pltpu.make_async_copy(g, k, arrived.at[n]) for n, (g, k) in enumerate(zip(given, kept))]
    for copy in copies:
        copy.start()
    lane = lax.broadcasted_iota(jnp.int32, (1, 128), 1)
    third = jnp.where(lane >= 2 * WIDE, 2, jnp.where(lane >= WIDE, 1, 0))
    inside = lane - third * WIDE
    member = inside // EDGE
    z = inside - member * EDGE
    wanted = []
    for group in range(1, GROUPS):
        code = jnp.full((1, 128), -5000, jnp.int32)
        for n in range(PER):
            d = FORWARD[(group - 1) * PER + n]
            code = jnp.where(member == n, d[0] * 100 + d[1] * 10 + d[2], code)
        wanted.append(jnp.where(lane < 3 * WIDE, code + third * 10 + z, -5000))
    row = lax.broadcasted_iota(jnp.int32, (EDGE, 128), 0)
    column = lax.broadcasted_iota(jnp.int32, (EDGE, 128), 1)
    pick = []
    for t in range(3):
        hit = column * 0 > 0
        for n in range(PER):
            hit = hit | (column == row + (t * WIDE + n * EDGE))
        pick.append((jnp.where(hit, 32.0, 0.0).astype(jnp.bfloat16), jnp.where(hit, 1.0, 0.0).astype(jnp.bfloat16)))

    for copy in copies:
        copy.wait()

    def one(x, carry):
        for s in range(2):
            slots = jnp.zeros((56, 128), F32)
            values = jnp.zeros((1, 128), F32)
            for t in range(3):
                y = 3 * s + t
                entry = neighbors[x, y]
                high = lax.shift_right_arithmetic(entry, 5)
                low = entry & 31
                for part, chosen in zip((high, low), pick[t]):
                    slots = slots + lax.dot_general(
                        part.astype(F32).astype(jnp.bfloat16), chosen, (((0,), (0,)), ((), ())),
                        preferred_element_type=F32,
                    )
                parts = [field[x, y, c : c + 1, :] for c in range(3)]
                parts += [polar[x, y : y + 1, :]]
                parts += [jitter[x, y, c : c + 1, :] for c in range(3)]
                for n in range(PER):
                    wide = jnp.concatenate([parts[n], jnp.zeros((1, 122), F32)], axis=1)
                    start = t * WIDE + n * EDGE
                    values = values + (pltpu.roll(wide, start, 1) if start else wide)
            out[x, 0, s : s + 1, :] = values
            home = (x + 2) * 100 + (2 + 3 * s) * 10 + 2
            for group in range(1, GROUPS):
                target = (wanted[group - 1] + home).astype(F32)
                flag = jnp.max(jnp.where(slots == target, 1.0, 0.0), axis=0, keepdims=True)
                out[x, group, s : s + 1, :] = flag
        return carry

    unrolled(EDGE, 2, one, 0)


def region_kernel(
    own, a1, a2, a3, b1, b2, b3, kept_out, info_out, chan, near, coef, moved, basis,
):
    gx = lax.axis_index("gx")
    gy = lax.axis_index("gy")
    lane = lane_iota()
    first, last = third_masks()
    along = lane - jnp.where(last, 2 * WIDE, jnp.where(first, 0, WIDE))
    is_low = (lane * 0 + gx) == 0

    def gather(x, carry):
        half = x // EDGE
        within = x - half * EDGE
        here = within + jnp.where(half == gx, 0, EDGE)
        there = within + jnp.where(half == gx, EDGE, 0)
        for group in range(GROUPS):
            ahead = [jnp.where(is_low, a[here, group], b[there, group]) for a, b in ((a1, b1), (a2, b2), (a3, b3))]
            back = [jnp.where(is_low, b[there, group], a[here, group]) for a, b in ((a3, b3), (a2, b2), (a1, b1))]
            blocks = back + [own[here, group]] + ahead
            outs = [None] * PER
            for gap in range(-6, 7):
                members = [m for m in range(PER) if 0 <= m + gap < PER]
                mixed = blocks[members[0] + gap]
                for m in members[1:]:
                    mixed = jnp.where(along >= 6 * m, blocks[m + gap], mixed)
                mixed = roll_lanes(mixed, -6 * gap)
                for m in members:
                    outs[m] = (
                        mixed if outs[m] is None
                        else jnp.where(along >= 6 * (m + gap), mixed, outs[m])
                    )
            for member in range(PER):
                acc = pltpu.roll(outs[member], 2 * gy, 0)
                if group * PER + member == 3:
                    acc = jnp.where(lane >= 3 * WIDE, 1.0, acc)
                    chan[x, 35] = 1.0 / acc
                chan[x, group * PER + member] = acc
        return carry

    lax.fori_loop(0, NX, gather, 0)

    def spread(x, carry):
        for c in range(4):
            v = chan[x, 3 + c]
            for dy in range(-2, 3):
                near[x, (dy + 2) * 4 + c] = shifted(v, dy, 0, first, last)
        return carry

    unrolled(NX, 3, spread, 0)

    def pairs(x, carry):
        home = {dz: [roll_lanes(chan[x, 3 + c], -dz) for c in range(4)] for dz in range(-2, 3)}
        for number, d in enumerate(FORWARD):
            other = wrap(x + d[0])
            place = (d[1] + 2) * 4
            polar, *jit = home[d[2]]
            sep = [((near[other, place + 1 + c] - jit[c]) + float(d[c])) * SPACING for c in range(3)]
            dist_sq = sep[0] * sep[0] + sep[1] * sep[1] + sep[2] * sep[2]
            over = lax.rsqrt(dist_sq)
            cube = dist_sq * dist_sq * over
            over_sq = over * over
            over_cube = over_sq * over
            damping = THOLE * cube * lax.rsqrt(polar * near[other, place])
            falloff = jnp.exp(-damping)
            iso = (1.0 - falloff) * over_cube
            radial = 3.0 * (1.0 - (1.0 + damping) * falloff) * over_cube * over_sq
            root = jnp.sqrt(radial)
            here = roll_lanes(chan[x, 7 + number], -d[2]) > 0.5
            values = [jnp.where(here, s * root, 0.0) for s in sep] + [jnp.where(here, iso, 0.0)]
            ahead = OFFSETS.index(d) * 4
            behind = OFFSETS.index((-d[0], -d[1], -d[2])) * 4
            for c in range(4):
                coef[x, ahead + c] = values[c]
                coef[other, behind + c] = shifted(values[c], -d[1], d[2], first, last)
        return carry

    lax.fori_loop(0, NX, pairs, 0)

    def move(x, c, v):
        for dy in range(-2, 3):
            moved[x, (dy + 2) * 3 + c] = shifted(v, dy, 0, first, last)

    def couple(x):
        acc = {dz: [None] * 3 for dz in range(-2, 3)}
        for dx in range(-2, 3):
            other = wrap(x + dx)
            for dy in range(-2, 3):
                v = [moved[other, (dy + 2) * 3 + c] for c in range(3)]
                for dz in range(-2, 3):
                    if (dx, dy, dz) not in OFFSETS:
                        continue
                    number = OFFSETS.index((dx, dy, dz)) * 4
                    s = [coef[x, number + c] for c in range(3)]
                    iso = coef[x, number + 3]
                    dot = s[0] * v[0] + s[1] * v[1] + s[2] * v[2]
                    new = [s[c] * dot - iso * v[c] for c in range(3)]
                    acc[dz] = [n if t is None else t + n for t, n in zip(acc[dz], new)]
        out = acc[0]
        for dz in (1, -1, 2, -2):
            out = [o + roll_lanes(t, dz) for o, t in zip(out, acc[dz])]
        return out

    zero = jnp.zeros((8, 128), F32)
    slab = (along >= 18) & (along < 24)

    def start(x, carry):
        for c in range(3):
            move(x, c, chan[x, 3] * chan[x, c])
        return carry

    unrolled(NX, 4, start, 0)

    def begin(x, carry):
        out = couple(x)
        polar = chan[x, 3]
        for c in range(3):
            basis[0, x * 3 + c] = zero
            basis[1, x * 3 + c] = polar * out[c]
        return carry

    unrolled(NX, 3, begin, 0)

    def again(x, carry):
        for c in range(3):
            move(x, c, basis[1, x * 3 + c])
        return carry

    unrolled(NX, 4, again, 0)

    def extend(k, carry):
        info, before = carry

        def one(x, sums):
            out = couple(x)
            polar = chan[x, 3]
            over = chan[x, 35]
            sums = list(sums)
            for c in range(3):
                u = basis[k + 1, x * 3 + c]
                w = polar * out[c]
                basis[k + 2, x * 3 + c] = w
                sums[0] = sums[0] + out[c] * u
                sums[1] = sums[1] + out[c] * basis[k, x * 3 + c]
                sums[2] = sums[2] + out[c] * w
                sums[3] = sums[3] + (u * over) * u
            return tuple(sums)

        sums = unrolled(NX, 3, one, (zero,) * 4)
        now, past, full, norm = [total(jnp.where(slab, s, 0.0)) for s in sums]
        tiny = 1e-36
        al = jnp.where(norm > tiny, now / jnp.maximum(norm, tiny), 0.0)
        be = jnp.where(before > tiny, past / jnp.maximum(before, tiny), 0.0)
        rest = full - al * now - be * past
        rest = jnp.maximum(rest, 1e-10 * full)
        good = (rest > tiny) & (norm > tiny)
        inv = jnp.where(good, jnp.sqrt(rest / jnp.maximum(norm, tiny)), 1.0)
        inv = jnp.minimum(jnp.maximum(inv, 1e-6), 1e3)
        sc = 1.0 / inv

        def scale(x, carry):
            for c in range(3):
                at = x * 3 + c
                new = (basis[k + 2, at] - al * basis[k + 1, at] - be * basis[k, at]) * sc
                basis[k + 2, at] = new
                move(x, c, new)
            return carry

        unrolled(NX, 4, scale, 0)
        info = jnp.where(lane == 45 + k, al, info)
        info = jnp.where(lane == 53 + k, be, info)
        return jnp.where(lane == 61 + k, inv, info), norm

    info, _ = lax.fori_loop(0, ITERS, extend, (zero, jnp.zeros((1, 1), F32)))

    number = 0
    for low, high in ((0, 3), (3, BASIS)):
        entries = [(i, j) for i in range(low, high) for j in range(i, BASIS)]

        def one(x, sums):
            sums = list(sums)
            for c in range(3):
                u = {j: basis[j + 1, x * 3 + c] for j in range(low, BASIS)}
                for i in range(low, high):
                    weighted = u[i] * chan[x, 35]
                    for n, (p, q) in enumerate(entries):
                        if p == i:
                            sums[n] = sums[n] + weighted * u[q]
            return tuple(sums)

        sums = unrolled(NX, 2, one, (zero,) * len(entries))
        for n in range(len(entries)):
            info = jnp.where(lane == number, total(jnp.where(slab, sums[n], 0.0)), info)
            number += 1

    for e in range(16):
        info_out[e] = info

    def keep(x, carry):
        far = x + EDGE * gx

        def front(v):
            return pltpu.roll(v, 8 - 2 * gy, 0)

        for c in range(3):
            for k in range(BASIS):
                kept_out[x, k * 3 + c] = front(basis[k + 1, far * 3 + c])
            kept_out[x, 27 + c] = front(chan[far, 3] * chan[far, c])
        kept_out[x, 30] = front(chan[far, 35])
        return carry

    unrolled(EDGE, 2, keep, 0)


def finish_kernel(kept, info, dip_out, res_out, len_out, table):
    gz = lax.axis_index("gz_0") * 4 + lax.axis_index("gz_1")
    wide = jnp.concatenate([info[e, 0:1, :] for e in range(16)] + [jnp.zeros((112, 128), F32)], axis=0)
    table[...] = wide.T
    rows = {}
    number = 0
    for low, high in ((0, 3), (3, BASIS)):
        for i in range(low, high):
            for j in range(i, BASIS):
                rows[i, j] = rows[j, i] = table[number : number + 1, :]
                number += 1
    al = [table[45 + k : 46 + k, :] for k in range(ITERS)]
    be = [table[53 + k : 54 + k, :] for k in range(ITERS)]
    inv = [table[61 + k : 62 + k, :] for k in range(ITERS)]
    lane = lax.broadcasted_iota(jnp.int32, (1, 128), 1)
    zero = jnp.zeros((1, 128), F32)
    one = jnp.where(lane < 16, 1.0, 0.0)

    def summed(v):
        return jnp.sum(v, axis=1, keepdims=True)

    def form(left, right, size_left, size_right):
        acc = zero
        for i in range(size_left):
            inner = zero
            for j in range(size_right):
                inner = inner + rows[i, j] * right[j]
            acc = acc + left[i] * inner
        return summed(acc)

    search = [one] + [zero] * ITERS
    resid = [one] + [zero] * ITERS
    moves = [zero] * BASIS
    gamma = summed(rows[0, 0])
    lengths = zero
    for k in range(ITERS):
        image = list(search)
        for j in range(k + 1):
            image[j] = image[j] - al[j] * search[j]
            image[j + 1] = image[j + 1] - inv[j] * search[j]
            if j:
                image[j - 1] = image[j - 1] - be[j] * search[j]
        step = gamma / form(search, image, k + 1, k + 2)
        lengths = jnp.where(lane == k, step, lengths)
        moves = [moves[j] + step * search[j] for j in range(BASIS)]
        resid = [resid[j] - step * image[j] for j in range(BASIS)]
        if k + 1 < ITERS:
            after = form(resid, resid, k + 2, k + 2)
            ratio = after / gamma
            search = [resid[j] + ratio * search[j] for j in range(BASIS)]
            gamma = after
    len_out[...] = lengths[:, :ITERS]
    here = lane == gz
    moves = [summed(jnp.where(here, v, 0.0)) for v in moves]
    resid = [summed(jnp.where(here, v, 0.0)) for v in resid]
    for x in range(EDGE):
        for c in range(3):
            dip = kept[x, 27 + c]
            res = jnp.zeros((8, 128), F32)
            for k in range(BASIS):
                u = kept[x, k * 3 + c]
                if k < ITERS:
                    dip = dip + moves[k] * u
                res = res + resid[k] * u
            res = res * kept[x, 30]
            for out, v in ((dip_out, dip), (res_out, res)):
                for t in range(3):
                    w = roll_lanes(v, t * WIDE + 18)
                    for s in range(2):
                        out[x, 3 * s + t, c : c + 1, :] = w[s : s + 1, :EDGE]


def per_device(permanent_field, polar, jitter, neighbors):
    packed = pl.pallas_call(
        pack_kernel,
        out_shape=jax.ShapeDtypeStruct((EDGE, GROUPS, 2, 128), F32),
        in_specs=[pl.BlockSpec(memory_space=pltpu.HBM)] * 4,
        scratch_shapes=[
            pltpu.VMEM((EDGE, EDGE, 3, EDGE), F32),
            pltpu.VMEM((EDGE, EDGE, EDGE), F32),
            pltpu.VMEM((EDGE, EDGE, 3, EDGE), F32),
            pltpu.VMEM((EDGE, EDGE, EDGE, 56), jnp.int32),
            pltpu.SemaphoreType.DMA((4,)),
        ],
        compiler_params=pltpu.CompilerParams(vmem_limit_bytes=60 * 1024 * 1024),
        name="pack",
    )(permanent_field.transpose(0, 1, 3, 2), polar, jitter.transpose(0, 1, 3, 2), neighbors)

    around = [packed]
    for k in (1, 2, 3):
        around.append(lax.ppermute(packed, "gy", [((i + k) % 4, i) for i in range(4)]))
    half = jnp.concatenate(around, axis=2)

    def swap(v):
        return lax.ppermute(v, "gx", [(0, 1), (1, 0)])

    own = jnp.concatenate([half, swap(half)], axis=0)

    def fetch(k):
        pairs = [((i + k) % 16, i) for i in range(16)]
        pairs += [(16 + (i - k) % 16, 16 + i) for i in range(16)]
        return lax.ppermute(own, ("gx",) + GZ, pairs)

    direct = [fetch(k) for k in (1, 2, 3)]
    passed = []
    for v in direct:
        passed.append(swap(v))

    vreg = (8, 128)
    kept, info = pl.pallas_call(
        region_kernel,
        out_shape=(
            jax.ShapeDtypeStruct((EDGE, 31) + vreg, F32),
            jax.ShapeDtypeStruct((16,) + vreg, F32),
        ),
        scratch_shapes=[
            pltpu.VMEM((NX, 36) + vreg, F32),
            pltpu.VMEM((NX, 20) + vreg, F32),
            pltpu.VMEM((NX, 4 * len(OFFSETS)) + vreg, F32),
            pltpu.VMEM((NX, 16) + vreg, F32),
            pltpu.VMEM((BASIS + 1, 3 * NX) + vreg, F32),
        ],
        compiler_params=pltpu.CompilerParams(vmem_limit_bytes=36 * 1024 * 1024),
        name="region",
    )(own, *direct, *passed)

    info = lax.all_to_all(info, GZ, 0, 0, tiled=True)

    dip, res, lengths = pl.pallas_call(
        finish_kernel,
        out_shape=(
            jax.ShapeDtypeStruct((EDGE, EDGE, 3, EDGE), F32),
            jax.ShapeDtypeStruct((EDGE, EDGE, 3, EDGE), F32),
            jax.ShapeDtypeStruct((1, ITERS), F32),
        ),
        scratch_shapes=[pltpu.VMEM((128, 128), F32)],
        compiler_params=pltpu.CompilerParams(vmem_limit_bytes=8 * 1024 * 1024),
        name="finish",
    )(kept, info)
    return dip.transpose(0, 1, 3, 2), res.transpose(0, 1, 3, 2), lengths.reshape(ITERS)


def solution(mesh):
    finer = Mesh(
        mesh.devices.reshape(mesh.shape["gx"], mesh.shape["gy"], 4, 4), ("gx", "gy", "gz_0", "gz_1")
    )
    return jax.shard_map(
        per_device,
        mesh=finer,
        in_specs=(
            P("gx", "gy", GZ, None),
            P("gx", "gy", GZ),
            P("gx", "gy", GZ, None),
            P("gx", "gy", GZ, None),
        ),
        out_specs=(P("gx", "gy", GZ, None), P("gx", "gy", GZ, None), P()),
        check_vma=False,
    )
```

```python
import jax
import jax.numpy as jnp
from jax import lax
from jax.experimental import pallas as pl
from jax.experimental.pallas import tpu as pltpu
from jax.sharding import Mesh
from jax.sharding import PartitionSpec as P

ITERS = 8
BASIS = ITERS + 1
THOLE = 0.39
SPACING = 3.5
EDGE = 6
NX = 12
WIDE = 42
GZ = ("gz_0", "gz_1")
F32 = jnp.float32

OFFSETS = [
    (a, b, c)
    for a in range(-2, 3)
    for b in range(-2, 3)
    for c in range(-2, 3)
    if 1 <= a * a + b * b + c * c <= 5
]
FORWARD = [d for d in OFFSETS if d > (0, 0, 0)]
GROUPS, PER = 5, 7


FIRSTS = {min(n for n, d in enumerate(FORWARD) if d[2] == dz) for dz in range(-2, 3)}


def lane_iota():
    return lax.broadcasted_iota(jnp.int32, (8, 128), 1)


def third_masks():
    lane = lane_iota()
    return lane < WIDE, lane >= 2 * WIDE


def roll_lanes(v, ahead):
    ahead = ahead % 128
    return v if ahead == 0 else pltpu.roll(v, 128 - ahead, 1)


def roll_rows(v, ahead):
    return pltpu.roll(v, (-ahead) % 8, 0)


def shifted(v, dy, dz, first, last):
    if dy == 0:
        return roll_lanes(v, dz)
    if dy == 1:
        return jnp.where(
            last, roll_rows(roll_lanes(v, dz - 2 * WIDE), 1), roll_lanes(v, dz + WIDE)
        )
    if dy == 2:
        return jnp.where(
            first, roll_lanes(v, dz + 2 * WIDE), roll_rows(roll_lanes(v, dz - WIDE), 1)
        )
    if dy == -1:
        return jnp.where(
            first, roll_rows(roll_lanes(v, dz + 2 * WIDE), -1), roll_lanes(v, dz - WIDE)
        )
    return jnp.where(
        last, roll_lanes(v, dz - 2 * WIDE), roll_rows(roll_lanes(v, dz + WIDE), -1)
    )


def wrap(x):
    if isinstance(x, int):
        return x % NX
    return jnp.where(x >= NX, x - NX, jnp.where(x < 0, x + NX, x))


def total(v):
    return jnp.sum(jnp.sum(v, axis=0, keepdims=True), axis=1, keepdims=True)


def unrolled(count, times, body, carry):
    def several(i, carry):
        for t in range(times):
            carry = body(i * times + t, carry)
        return carry

    return lax.fori_loop(0, count // times, several, carry)


def pack_kernel(
    field_in, polar_in, jitter_in, neighbors_in, out, field, polar, jitter, neighbors, arrived
):
    given = (neighbors_in, field_in, jitter_in, polar_in)
    kept = (neighbors, field, jitter, polar)
    copies = [pltpu.make_async_copy(g, k, arrived.at[n]) for n, (g, k) in enumerate(zip(given, kept))]
    for copy in copies:
        copy.start()
    lane = lax.broadcasted_iota(jnp.int32, (1, 128), 1)
    third = jnp.where(lane >= 2 * WIDE, 2, jnp.where(lane >= WIDE, 1, 0))
    inside = lane - third * WIDE
    member = inside // EDGE
    z = inside - member * EDGE
    wanted = []
    for group in range(1, GROUPS):
        code = jnp.full((1, 128), -5000, jnp.int32)
        for n in range(PER):
            d = FORWARD[(group - 1) * PER + n]
            code = jnp.where(member == n, d[0] * 100 + d[1] * 10 + d[2], code)
        wanted.append(jnp.where(lane < 3 * WIDE, code + third * 10 + z, -5000))
    row = lax.broadcasted_iota(jnp.int32, (EDGE, 128), 0)
    column = lax.broadcasted_iota(jnp.int32, (EDGE, 128), 1)
    pick = []
    for t in range(3):
        hit = column * 0 > 0
        for n in range(PER):
            hit = hit | (column == row + (t * WIDE + n * EDGE))
        pick.append((jnp.where(hit, 32.0, 0.0).astype(jnp.bfloat16), jnp.where(hit, 1.0, 0.0).astype(jnp.bfloat16)))

    for copy in copies:
        copy.wait()

    def one(x, carry):
        for s in range(2):
            slots = jnp.zeros((56, 128), F32)
            values = jnp.zeros((1, 128), F32)
            for t in range(3):
                y = 3 * s + t
                entry = neighbors[x, y]
                high = lax.shift_right_arithmetic(entry, 5)
                low = entry & 31
                for part, chosen in zip((high, low), pick[t]):
                    slots = slots + lax.dot_general(
                        part.astype(F32).astype(jnp.bfloat16), chosen, (((0,), (0,)), ((), ())),
                        preferred_element_type=F32,
                    )
                parts = [field[x, y, c : c + 1, :] for c in range(3)]
                parts += [polar[x, y : y + 1, :]]
                parts += [jitter[x, y, c : c + 1, :] for c in range(3)]
                for n in range(PER):
                    wide = jnp.concatenate([parts[n], jnp.zeros((1, 122), F32)], axis=1)
                    start = t * WIDE + n * EDGE
                    values = values + (pltpu.roll(wide, start, 1) if start else wide)
            out[x, 0, s : s + 1, :] = values
            home = (x + 2) * 100 + (2 + 3 * s) * 10 + 2
            for group in range(1, GROUPS):
                target = (wanted[group - 1] + home).astype(F32)
                flag = jnp.max(jnp.where(slots == target, 1.0, 0.0), axis=0, keepdims=True)
                out[x, group, s : s + 1, :] = flag
        return carry

    unrolled(EDGE, 2, one, 0)


def region_kernel(
    own, a1, a2, a3, b1, b2, b3, kept_out, info_out, chan, near, coef, moved, basis,
    raw, now, past,
):
    gx = lax.axis_index("gx")
    gy = lax.axis_index("gy")
    lane = lane_iota()
    first, last = third_masks()
    along = lane - jnp.where(last, 2 * WIDE, jnp.where(first, 0, WIDE))
    is_low = (lane * 0 + gx) == 0

    def gather(x, carry):
        half = x // EDGE
        within = x - half * EDGE
        here = within + jnp.where(half == gx, 0, EDGE)
        there = within + jnp.where(half == gx, EDGE, 0)
        for group in range(GROUPS):
            ahead = [jnp.where(is_low, a[here, group], b[there, group]) for a, b in ((a1, b1), (a2, b2), (a3, b3))]
            back = [jnp.where(is_low, b[there, group], a[here, group]) for a, b in ((a3, b3), (a2, b2), (a1, b1))]
            blocks = back + [own[here, group]] + ahead
            outs = [None] * PER
            for gap in range(-6, 7):
                members = [m for m in range(PER) if 0 <= m + gap < PER]
                mixed = blocks[members[0] + gap]
                for m in members[1:]:
                    mixed = jnp.where(along >= 6 * m, blocks[m + gap], mixed)
                mixed = roll_lanes(mixed, -6 * gap)
                for m in members:
                    outs[m] = (
                        mixed if outs[m] is None
                        else jnp.where(along >= 6 * (m + gap), mixed, outs[m])
                    )
            for member in range(PER):
                acc = pltpu.roll(outs[member], 2 * gy, 0)
                if group * PER + member == 3:
                    acc = jnp.where(lane >= 3 * WIDE, 1.0, acc)
                    chan[x, 35] = 1.0 / acc
                chan[x, group * PER + member] = acc
        return carry

    unrolled(NX, 2, gather, 0)

    def spread(x, carry):
        for c in range(4):
            v = chan[x, 3 + c]
            for dy in range(-2, 3):
                near[x, (dy + 2) * 4 + c] = shifted(v, dy, 0, first, last)
        return carry

    unrolled(NX, 3, spread, 0)

    def pairs(x, carry):
        for number, d in sorted(enumerate(FORWARD), key=lambda t: t[1][2]):
            if number in FIRSTS:
                home = [roll_lanes(chan[x, 3 + c], -d[2]) for c in range(4)]
            other = wrap(x + d[0])
            place = (d[1] + 2) * 4
            polar, *jit = home
            sep = [((near[other, place + 1 + c] - jit[c]) + float(d[c])) * SPACING for c in range(3)]
            dist_sq = sep[0] * sep[0] + sep[1] * sep[1] + sep[2] * sep[2]
            over = lax.rsqrt(dist_sq)
            cube = dist_sq * dist_sq * over
            over_sq = over * over
            over_cube = over_sq * over
            damping = THOLE * cube * lax.rsqrt(polar * near[other, place])
            falloff = jnp.exp(-damping)
            iso = (1.0 - falloff) * over_cube
            radial = 3.0 * (1.0 - (1.0 + damping) * falloff) * over_cube * over_sq
            root = jnp.sqrt(radial)
            here = roll_lanes(chan[x, 7 + number], -d[2]) > 0.5
            values = [jnp.where(here, s * root, 0.0) for s in sep] + [jnp.where(here, iso, 0.0)]
            ahead = OFFSETS.index(d) * 4
            behind = OFFSETS.index((-d[0], -d[1], -d[2])) * 4
            for c in range(4):
                coef[x, ahead + c] = values[c]
                coef[other, behind + c] = shifted(values[c], -d[1], d[2], first, last)
        return carry

    lax.fori_loop(0, NX, pairs, 0)

    def move(x, c, v):
        for dy in range(-2, 3):
            moved[x, (dy + 2) * 3 + c] = shifted(v, dy, 0, first, last)

    def couple(x):
        acc = {dz: [None] * 3 for dz in range(-2, 3)}
        for dx in range(-2, 3):
            other = wrap(x + dx)
            for dy in range(-2, 3):
                v = [moved[other, (dy + 2) * 3 + c] for c in range(3)]
                for dz in range(-2, 3):
                    if (dx, dy, dz) not in OFFSETS:
                        continue
                    number = OFFSETS.index((dx, dy, dz)) * 4
                    s = [coef[x, number + c] for c in range(3)]
                    iso = coef[x, number + 3]
                    dot = s[0] * v[0] + s[1] * v[1] + s[2] * v[2]
                    new = [s[c] * dot - iso * v[c] for c in range(3)]
                    acc[dz] = [n if t is None else t + n for t, n in zip(acc[dz], new)]
        out = acc[0]
        for dz in (1, -1, 2, -2):
            out = [o + roll_lanes(t, dz) for o, t in zip(out, acc[dz])]
        return out

    zero = jnp.zeros((8, 128), F32)
    slab = (along >= 18) & (along < 24)

    def prepare(x, carry):
        for c in range(3):
            raw[x * 3 + c] = chan[x, 3] * chan[x, c]
            now[x * 3 + c] = zero
            past[x * 3 + c] = zero
        return carry

    unrolled(NX, 4, prepare, 0)

    def next_vector(x, c, al, be, sc):
        return (raw[x * 3 + c] - al * now[x * 3 + c] - be * past[x * 3 + c]) * sc

    def extend(k, carry):
        info, before, al, be, sc = carry
        sums = [zero] * 4

        def scale(x):
            for c in range(3):
                new = next_vector(x, c, al, be, sc)
                past[x * 3 + c] = now[x * 3 + c]
                now[x * 3 + c] = new
                basis[k, x * 3 + c] = new
                move(x, c, new)

        for x in (10, 11, 0, 1, 2):
            scale(x)
        for x in range(NX):
            if 3 <= x + 3 < 10:
                scale(x + 3)
            out = couple(x)
            polar = chan[x, 3]
            over = chan[x, 35]
            for c in range(3):
                u = now[x * 3 + c]
                w = polar * out[c]
                raw[x * 3 + c] = w
                sums[0] = sums[0] + out[c] * u
                sums[1] = sums[1] + out[c] * past[x * 3 + c]
                sums[2] = sums[2] + out[c] * w
                sums[3] = sums[3] + (u * over) * u
        along_now, along_past, full, norm = [total(jnp.where(slab, t, 0.0)) for t in sums]
        live = k > 0
        norm = jnp.where(live, norm, 0.0)
        tiny = 1e-36
        al = jnp.where(norm > tiny, along_now / jnp.maximum(norm, tiny), 0.0)
        be = jnp.where(before > tiny, along_past / jnp.maximum(before, tiny), 0.0)
        rest = full - al * along_now - be * along_past
        rest = jnp.maximum(rest, 1e-10 * full)
        good = (rest > tiny) & (norm > tiny)
        inv = jnp.where(good, jnp.sqrt(rest / jnp.maximum(norm, tiny)), 1.0)
        inv = jnp.minimum(jnp.maximum(inv, 1e-6), 1e3)
        info = jnp.where(lane == 44 + k, jnp.where(live, al, info), info)
        info = jnp.where(lane == 52 + k, jnp.where(live, be, info), info)
        info = jnp.where(lane == 60 + k, jnp.where(live, inv, info), info)
        return info, norm, al, be, 1.0 / inv

    none = jnp.zeros((1, 1), F32)
    info, _, al, be, sc = lax.fori_loop(0, BASIS, extend, (zero, none, none, none, none + 1.0))

    def end(x, carry):
        for c in range(3):
            basis[BASIS, x * 3 + c] = next_vector(x, c, al, be, sc)
        return carry

    unrolled(NX, 4, end, 0)

    number = 0
    for low, high in ((0, 3), (3, BASIS)):
        entries = [(i, j) for i in range(low, high) for j in range(i, BASIS)]

        def one(x, sums):
            sums = list(sums)
            for c in range(3):
                u = {j: basis[j + 1, x * 3 + c] for j in range(low, BASIS)}
                for i in range(low, high):
                    weighted = u[i] * chan[x, 35]
                    for n, (p, q) in enumerate(entries):
                        if p == i:
                            sums[n] = sums[n] + weighted * u[q]
            return tuple(sums)

        sums = unrolled(NX, 2, one, (zero,) * len(entries))
        for n in range(len(entries)):
            info = jnp.where(lane == number, total(jnp.where(slab, sums[n], 0.0)), info)
            number += 1

    for e in range(16):
        info_out[e] = info

    def keep(x, carry):
        far = x + EDGE * gx

        def front(v):
            return pltpu.roll(v, 8 - 2 * gy, 0)

        for c in range(3):
            for k in range(BASIS):
                kept_out[x, k * 3 + c] = front(basis[k + 1, far * 3 + c])
            kept_out[x, 27 + c] = front(basis[0, far * 3 + c])
        kept_out[x, 30] = front(chan[far, 35])
        return carry

    unrolled(EDGE, 2, keep, 0)


def finish_kernel(kept, info, dip_out, res_out, len_out, table):
    gz = lax.axis_index("gz_0") * 4 + lax.axis_index("gz_1")
    wide = jnp.concatenate([info[e, 0:1, :] for e in range(16)] + [jnp.zeros((112, 128), F32)], axis=0)
    table[...] = wide.T
    rows = {}
    number = 0
    for low, high in ((0, 3), (3, BASIS)):
        for i in range(low, high):
            for j in range(i, BASIS):
                rows[i, j] = rows[j, i] = table[number : number + 1, :]
                number += 1
    al = [table[45 + k : 46 + k, :] for k in range(ITERS)]
    be = [table[53 + k : 54 + k, :] for k in range(ITERS)]
    inv = [table[61 + k : 62 + k, :] for k in range(ITERS)]
    lane = lax.broadcasted_iota(jnp.int32, (1, 128), 1)
    zero = jnp.zeros((1, 128), F32)
    one = jnp.where(lane < 16, 1.0, 0.0)

    def summed(v):
        return jnp.sum(v, axis=1, keepdims=True)

    def form(left, right, size_left, size_right):
        acc = zero
        for i in range(size_left):
            inner = zero
            for j in range(size_right):
                inner = inner + rows[i, j] * right[j]
            acc = acc + left[i] * inner
        return summed(acc)

    search = [one] + [zero] * ITERS
    resid = [one] + [zero] * ITERS
    moves = [zero] * BASIS
    gamma = summed(rows[0, 0])
    lengths = zero
    for k in range(ITERS):
        image = list(search)
        for j in range(k + 1):
            image[j] = image[j] - al[j] * search[j]
            image[j + 1] = image[j + 1] - inv[j] * search[j]
            if j:
                image[j - 1] = image[j - 1] - be[j] * search[j]
        step = gamma / form(search, image, k + 1, k + 2)
        lengths = jnp.where(lane == k, step, lengths)
        moves = [moves[j] + step * search[j] for j in range(BASIS)]
        resid = [resid[j] - step * image[j] for j in range(BASIS)]
        if k + 1 < ITERS:
            after = form(resid, resid, k + 2, k + 2)
            ratio = after / gamma
            search = [resid[j] + ratio * search[j] for j in range(BASIS)]
            gamma = after
    len_out[...] = lengths[:, :ITERS]
    here = lane == gz
    moves = [summed(jnp.where(here, v, 0.0)) for v in moves]
    resid = [summed(jnp.where(here, v, 0.0)) for v in resid]
    for x in range(EDGE):
        for c in range(3):
            dip = kept[x, 27 + c]
            res = jnp.zeros((8, 128), F32)
            for k in range(BASIS):
                u = kept[x, k * 3 + c]
                if k < ITERS:
                    dip = dip + moves[k] * u
                res = res + resid[k] * u
            res = res * kept[x, 30]
            for out, v in ((dip_out, dip), (res_out, res)):
                for t in range(3):
                    w = roll_lanes(v, t * WIDE + 18)
                    for s in range(2):
                        out[x, 3 * s + t, c : c + 1, :] = w[s : s + 1, :EDGE]


def per_device(permanent_field, polar, jitter, neighbors):
    packed = pl.pallas_call(
        pack_kernel,
        out_shape=jax.ShapeDtypeStruct((EDGE, GROUPS, 2, 128), F32),
        in_specs=[pl.BlockSpec(memory_space=pltpu.HBM)] * 4,
        scratch_shapes=[
            pltpu.VMEM((EDGE, EDGE, 3, EDGE), F32),
            pltpu.VMEM((EDGE, EDGE, EDGE), F32),
            pltpu.VMEM((EDGE, EDGE, 3, EDGE), F32),
            pltpu.VMEM((EDGE, EDGE, EDGE, 56), jnp.int32),
            pltpu.SemaphoreType.DMA((4,)),
        ],
        compiler_params=pltpu.CompilerParams(vmem_limit_bytes=60 * 1024 * 1024),
        name="pack",
    )(permanent_field.transpose(0, 1, 3, 2), polar, jitter.transpose(0, 1, 3, 2), neighbors)

    around = [packed] + [
        lax.ppermute(packed, "gy", [((i + k) % 4, i) for i in range(4)]) for k in (1, 2, 3)
    ]
    half = jnp.concatenate(around, axis=2)

    def swap(v):
        return lax.ppermute(v, "gx", [(0, 1), (1, 0)])

    own = jnp.concatenate([half, swap(half)], axis=0)

    def fetch(k):
        pairs = [((i + k) % 16, i) for i in range(16)]
        pairs += [(16 + (i - k) % 16, 16 + i) for i in range(16)]
        return lax.ppermute(own, ("gx",) + GZ, pairs)

    direct = [fetch(k) for k in (1, 2, 3)]
    passed = [swap(v) for v in direct]

    vreg = (8, 128)
    kept, info = pl.pallas_call(
        region_kernel,
        out_shape=(
            jax.ShapeDtypeStruct((EDGE, 31) + vreg, F32),
            jax.ShapeDtypeStruct((16,) + vreg, F32),
        ),
        scratch_shapes=[
            pltpu.VMEM((NX, 36) + vreg, F32),
            pltpu.VMEM((NX, 20) + vreg, F32),
            pltpu.VMEM((NX, 4 * len(OFFSETS)) + vreg, F32),
            pltpu.VMEM((NX, 16) + vreg, F32),
            pltpu.VMEM((BASIS + 1, 3 * NX) + vreg, F32),
            pltpu.VMEM((3 * NX,) + vreg, F32),
            pltpu.VMEM((3 * NX,) + vreg, F32),
            pltpu.VMEM((3 * NX,) + vreg, F32),
        ],
        compiler_params=pltpu.CompilerParams(vmem_limit_bytes=36 * 1024 * 1024),
        name="region",
    )(own, *direct, *passed)

    info = lax.all_to_all(info, GZ, 0, 0, tiled=True)

    dip, res, lengths = pl.pallas_call(
        finish_kernel,
        out_shape=(
            jax.ShapeDtypeStruct((EDGE, EDGE, 3, EDGE), F32),
            jax.ShapeDtypeStruct((EDGE, EDGE, 3, EDGE), F32),
            jax.ShapeDtypeStruct((1, ITERS), F32),
        ),
        scratch_shapes=[pltpu.VMEM((128, 128), F32)],
        compiler_params=pltpu.CompilerParams(vmem_limit_bytes=8 * 1024 * 1024),
        name="finish",
    )(kept, info)
    return dip.transpose(0, 1, 3, 2), res.transpose(0, 1, 3, 2), lengths.reshape(ITERS)


def solution(mesh):
    finer = Mesh(
        mesh.devices.reshape(mesh.shape["gx"], mesh.shape["gy"], 4, 4), ("gx", "gy", "gz_0", "gz_1")
    )
    return jax.shard_map(
        per_device,
        mesh=finer,
        in_specs=(
            P("gx", "gy", GZ, None),
            P("gx", "gy", GZ),
            P("gx", "gy", GZ, None),
            P("gx", "gy", GZ, None),
        ),
        out_specs=(P("gx", "gy", GZ, None), P("gx", "gy", GZ, None), P()),
        check_vma=False,
    )
```

```python
import jax
import jax.numpy as jnp
from jax import lax
from jax.experimental import pallas as pl
from jax.experimental.pallas import tpu as pltpu
from jax.sharding import Mesh
from jax.sharding import PartitionSpec as P

ITERS = 8
BASIS = ITERS + 1
THOLE = 0.39
SPACING = 3.5
EDGE = 6
NX = 12
WIDE = 42
GZ = ("gz_0", "gz_1")
F32 = jnp.float32

OFFSETS = [
    (a, b, c)
    for a in range(-2, 3)
    for b in range(-2, 3)
    for c in range(-2, 3)
    if 1 <= a * a + b * b + c * c <= 5
]
FORWARD = [d for d in OFFSETS if d > (0, 0, 0)]
GROUPS, PER = 5, 7


FIRSTS = {min(n for n, d in enumerate(FORWARD) if d[2] == dz) for dz in range(-2, 3)}


def lane_iota():
    return lax.broadcasted_iota(jnp.int32, (8, 128), 1)


def third_masks():
    lane = lane_iota()
    return lane < WIDE, lane >= 2 * WIDE


def roll_lanes(v, ahead):
    ahead = ahead % 128
    return v if ahead == 0 else pltpu.roll(v, 128 - ahead, 1)


def roll_rows(v, ahead):
    return pltpu.roll(v, (-ahead) % 8, 0)


def shifted(v, dy, dz, first, last):
    if dy == 0:
        return roll_lanes(v, dz)
    if dy == 1:
        return jnp.where(
            last, roll_rows(roll_lanes(v, dz - 2 * WIDE), 1), roll_lanes(v, dz + WIDE)
        )
    if dy == 2:
        return jnp.where(
            first, roll_lanes(v, dz + 2 * WIDE), roll_rows(roll_lanes(v, dz - WIDE), 1)
        )
    if dy == -1:
        return jnp.where(
            first, roll_rows(roll_lanes(v, dz + 2 * WIDE), -1), roll_lanes(v, dz - WIDE)
        )
    return jnp.where(
        last, roll_lanes(v, dz - 2 * WIDE), roll_rows(roll_lanes(v, dz + WIDE), -1)
    )


def wrap(x):
    if isinstance(x, int):
        return x % NX
    return jnp.where(x >= NX, x - NX, jnp.where(x < 0, x + NX, x))


def total(v):
    return jnp.sum(jnp.sum(v, axis=0, keepdims=True), axis=1, keepdims=True)


def unrolled(count, times, body, carry):
    def several(i, carry):
        for t in range(times):
            carry = body(i * times + t, carry)
        return carry

    return lax.fori_loop(0, count // times, several, carry)


def pack_kernel(
    field_in, polar_in, jitter_in, neighbors_in, out, field, polar, jitter, neighbors, arrived
):
    given = (neighbors_in, field_in, jitter_in, polar_in)
    kept = (neighbors, field, jitter, polar)
    copies = [pltpu.make_async_copy(g, k, arrived.at[n]) for n, (g, k) in enumerate(zip(given, kept))]
    for copy in copies:
        copy.start()
    lane = lax.broadcasted_iota(jnp.int32, (1, 128), 1)
    third = jnp.where(lane >= 2 * WIDE, 2, jnp.where(lane >= WIDE, 1, 0))
    inside = lane - third * WIDE
    member = inside // EDGE
    z = inside - member * EDGE
    wanted = []
    for group in range(1, GROUPS):
        code = jnp.full((1, 128), -5000, jnp.int32)
        for n in range(PER):
            d = FORWARD[(group - 1) * PER + n]
            code = jnp.where(member == n, d[0] * 100 + d[1] * 10 + d[2], code)
        wanted.append(jnp.where(lane < 3 * WIDE, code + third * 10 + z, -5000))
    row = lax.broadcasted_iota(jnp.int32, (EDGE, 128), 0)
    column = lax.broadcasted_iota(jnp.int32, (EDGE, 128), 1)
    pick = []
    for t in range(3):
        hit = column * 0 > 0
        for n in range(PER):
            hit = hit | (column == row + (t * WIDE + n * EDGE))
        pick.append((jnp.where(hit, 32.0, 0.0).astype(jnp.bfloat16), jnp.where(hit, 1.0, 0.0).astype(jnp.bfloat16)))

    for copy in copies:
        copy.wait()

    def one(x, carry):
        for s in range(2):
            slots = jnp.zeros((56, 128), F32)
            values = jnp.zeros((1, 128), F32)
            for t in range(3):
                y = 3 * s + t
                entry = neighbors[x, y]
                high = lax.shift_right_arithmetic(entry, 5)
                low = entry & 31
                for part, chosen in zip((high, low), pick[t]):
                    slots = slots + lax.dot_general(
                        part.astype(F32).astype(jnp.bfloat16), chosen, (((0,), (0,)), ((), ())),
                        preferred_element_type=F32,
                    )
                parts = [field[x, y, c : c + 1, :] for c in range(3)]
                parts += [polar[x, y : y + 1, :]]
                parts += [jitter[x, y, c : c + 1, :] for c in range(3)]
                for n in range(PER):
                    wide = jnp.concatenate([parts[n], jnp.zeros((1, 122), F32)], axis=1)
                    start = t * WIDE + n * EDGE
                    values = values + (pltpu.roll(wide, start, 1) if start else wide)
            out[x, 0, s : s + 1, :] = values
            home = (x + 2) * 100 + (2 + 3 * s) * 10 + 2
            for group in range(1, GROUPS):
                target = (wanted[group - 1] + home).astype(F32)
                flag = jnp.max(jnp.where(slots == target, 1.0, 0.0), axis=0, keepdims=True)
                out[x, group, s : s + 1, :] = flag
        return carry

    unrolled(EDGE, 2, one, 0)


def region_kernel(
    own, a1, a2, a3, b1, b2, b3, kept_out, info_out, chan, near, coef, moved, basis,
    raw, now, past,
):
    gx = lax.axis_index("gx")
    gy = lax.axis_index("gy")
    lane = lane_iota()
    first, last = third_masks()
    along = lane - jnp.where(last, 2 * WIDE, jnp.where(first, 0, WIDE))
    is_low = (lane * 0 + gx) == 0

    def gather(x, carry):
        half = x // EDGE
        within = x - half * EDGE
        here = within + jnp.where(half == gx, 0, EDGE)
        there = within + jnp.where(half == gx, EDGE, 0)
        for group in range(GROUPS):
            ahead = [jnp.where(is_low, a[here, group], b[there, group]) for a, b in ((a1, b1), (a2, b2), (a3, b3))]
            back = [jnp.where(is_low, b[there, group], a[here, group]) for a, b in ((a3, b3), (a2, b2), (a1, b1))]
            blocks = back + [own[here, group]] + ahead
            outs = [None] * PER
            for gap in range(-6, 7):
                members = [m for m in range(PER) if 0 <= m + gap < PER]
                mixed = blocks[members[0] + gap]
                for m in members[1:]:
                    mixed = jnp.where(along >= 6 * m, blocks[m + gap], mixed)
                mixed = roll_lanes(mixed, -6 * gap)
                for m in members:
                    outs[m] = (
                        mixed if outs[m] is None
                        else jnp.where(along >= 6 * (m + gap), mixed, outs[m])
                    )
            for member in range(PER):
                acc = pltpu.roll(outs[member], 2 * gy, 0)
                if group * PER + member == 3:
                    acc = jnp.where(lane >= 3 * WIDE, 1.0, acc)
                    chan[x, 35] = 1.0 / acc
                chan[x, group * PER + member] = acc
        return carry

    unrolled(NX, 2, gather, 0)

    def spread(x, carry):
        for c in range(4):
            v = chan[x, 3 + c]
            for dy in range(-2, 3):
                near[x, (dy + 2) * 4 + c] = shifted(v, dy, 0, first, last)
        return carry

    unrolled(NX, 3, spread, 0)

    def pairs(x, carry):
        for number, d in sorted(enumerate(FORWARD), key=lambda t: t[1][2]):
            if number in FIRSTS:
                home = [roll_lanes(chan[x, 3 + c], -d[2]) for c in range(4)]
            other = wrap(x + d[0])
            place = (d[1] + 2) * 4
            polar, *jit = home
            sep = [((near[other, place + 1 + c] - jit[c]) + float(d[c])) * SPACING for c in range(3)]
            dist_sq = sep[0] * sep[0] + sep[1] * sep[1] + sep[2] * sep[2]
            over = lax.rsqrt(dist_sq)
            cube = dist_sq * dist_sq * over
            over_sq = over * over
            over_cube = over_sq * over
            damping = THOLE * cube * lax.rsqrt(polar * near[other, place])
            falloff = jnp.exp(-damping)
            iso = (1.0 - falloff) * over_cube
            radial = 3.0 * (1.0 - (1.0 + damping) * falloff) * over_cube * over_sq
            root = jnp.sqrt(radial)
            here = roll_lanes(chan[x, 7 + number], -d[2]) > 0.5
            values = [jnp.where(here, s * root, 0.0) for s in sep] + [jnp.where(here, iso, 0.0)]
            ahead = OFFSETS.index(d) * 4
            behind = OFFSETS.index((-d[0], -d[1], -d[2])) * 4
            for c in range(4):
                coef[x, ahead + c] = values[c]
                coef[other, behind + c] = shifted(values[c], -d[1], d[2], first, last)
        return carry

    lax.fori_loop(0, NX, pairs, 0)

    def move(x, c, v):
        for dy in range(-2, 3):
            moved[x, (dy + 2) * 3 + c] = shifted(v, dy, 0, first, last)

    def couple(x):
        acc = {dz: [None] * 3 for dz in range(-2, 3)}
        for dx in range(-2, 3):
            other = wrap(x + dx)
            for dy in range(-2, 3):
                v = [moved[other, (dy + 2) * 3 + c] for c in range(3)]
                for dz in range(-2, 3):
                    if (dx, dy, dz) not in OFFSETS:
                        continue
                    number = OFFSETS.index((dx, dy, dz)) * 4
                    s = [coef[x, number + c] for c in range(3)]
                    iso = coef[x, number + 3]
                    dot = s[0] * v[0] + s[1] * v[1] + s[2] * v[2]
                    new = [s[c] * dot - iso * v[c] for c in range(3)]
                    acc[dz] = [n if t is None else t + n for t, n in zip(acc[dz], new)]
        out = acc[0]
        for dz in (1, -1, 2, -2):
            out = [o + roll_lanes(t, dz) for o, t in zip(out, acc[dz])]
        return out

    zero = jnp.zeros((8, 128), F32)
    slab = (along >= 18) & (along < 24)

    def prepare(x, carry):
        for c in range(3):
            raw[x * 3 + c] = chan[x, 3] * chan[x, c]
            now[x * 3 + c] = zero
            past[x * 3 + c] = zero
        return carry

    unrolled(NX, 4, prepare, 0)

    def next_vector(x, c, al, be, sc):
        return (raw[x * 3 + c] - al * now[x * 3 + c] - be * past[x * 3 + c]) * sc

    def extend(k, carry):
        info, before, al, be, sc = carry
        sums = [zero] * 4

        def scale(x):
            for c in range(3):
                new = next_vector(x, c, al, be, sc)
                past[x * 3 + c] = now[x * 3 + c]
                now[x * 3 + c] = new
                basis[k, x * 3 + c] = new
                move(x, c, new)

        for x in (10, 11, 0, 1, 2):
            scale(x)
        for x in range(NX):
            if 3 <= x + 3 < 10:
                scale(x + 3)
            out = couple(x)
            polar = chan[x, 3]
            over = chan[x, 35]
            for c in range(3):
                u = now[x * 3 + c]
                w = polar * out[c]
                raw[x * 3 + c] = w
                sums[0] = sums[0] + out[c] * u
                sums[1] = sums[1] + out[c] * past[x * 3 + c]
                sums[2] = sums[2] + out[c] * w
                sums[3] = sums[3] + (u * over) * u
        along_now, along_past, full, norm = [total(jnp.where(slab, t, 0.0)) for t in sums]
        live = k > 0
        norm = jnp.where(live, norm, 0.0)
        tiny = 1e-36
        al = jnp.where(norm > tiny, along_now / jnp.maximum(norm, tiny), 0.0)
        be = jnp.where(before > tiny, along_past / jnp.maximum(before, tiny), 0.0)
        rest = full - al * along_now - be * along_past
        rest = jnp.maximum(rest, 1e-10 * full)
        good = (rest > tiny) & (norm > tiny)
        inv = jnp.where(good, jnp.sqrt(rest / jnp.maximum(norm, tiny)), 1.0)
        inv = jnp.minimum(jnp.maximum(inv, 1e-6), 1e3)
        info = jnp.where(lane == 44 + k, jnp.where(live, al, info), info)
        info = jnp.where(lane == 52 + k, jnp.where(live, be, info), info)
        info = jnp.where(lane == 60 + k, jnp.where(live, inv, info), info)
        return info, norm, al, be, 1.0 / inv

    none = jnp.zeros((1, 1), F32)
    info, _, al, be, sc = lax.fori_loop(0, BASIS, extend, (zero, none, none, none, none + 1.0))

    def end(x, carry):
        for c in range(3):
            basis[BASIS, x * 3 + c] = next_vector(x, c, al, be, sc)
        return carry

    unrolled(NX, 4, end, 0)

    number = 0
    for low, high in ((0, 3), (3, BASIS)):
        entries = [(i, j) for i in range(low, high) for j in range(i, BASIS)]

        def one(x, sums):
            sums = list(sums)
            for c in range(3):
                u = {j: basis[j + 1, x * 3 + c] for j in range(low, BASIS)}
                for i in range(low, high):
                    weighted = u[i] * chan[x, 35]
                    for n, (p, q) in enumerate(entries):
                        if p == i:
                            sums[n] = sums[n] + weighted * u[q]
            return tuple(sums)

        sums = unrolled(NX, 2, one, (zero,) * len(entries))
        for n in range(len(entries)):
            info = jnp.where(lane == number, total(jnp.where(slab, sums[n], 0.0)), info)
            number += 1

    for e in range(16):
        info_out[e] = info

    def keep(x, carry):
        far = x + EDGE * gx

        def front(v):
            return pltpu.roll(v, 8 - 2 * gy, 0)

        for c in range(3):
            for k in range(BASIS):
                kept_out[x, k * 3 + c] = front(basis[k + 1, far * 3 + c])
            kept_out[x, 27 + c] = front(basis[0, far * 3 + c])
        kept_out[x, 30] = front(chan[far, 35])
        return carry

    unrolled(EDGE, 2, keep, 0)


def finish_kernel(kept, info, dip_out, res_out, len_out):
    gz = lax.axis_index("gz_0") * 4 + lax.axis_index("gz_1")
    table = jnp.concatenate([info[e, 0:1, :] for e in range(16)], axis=0)
    wide = (2, 8, 128)

    def column(n):
        return jnp.broadcast_to(table[:, n : n + 1], (16, 128)).reshape(wide)

    rows = {}
    number = 0
    for low, high in ((0, 3), (3, BASIS)):
        for i in range(low, high):
            for j in range(i, BASIS):
                rows[i, j] = rows[j, i] = column(number)
                number += 1
    al = [column(45 + k) for k in range(ITERS)]
    be = [column(53 + k) for k in range(ITERS)]
    inv = [column(61 + k) for k in range(ITERS)]
    zero = jnp.zeros(wide, F32)
    slab = lax.broadcasted_iota(jnp.int32, wide, 0) * 8 + lax.broadcasted_iota(jnp.int32, wide, 1)
    lane = lax.broadcasted_iota(jnp.int32, (8, 128), 1)

    def summed(v):
        t = v[0] + v[1]
        for by in (4, 2, 1):
            t = t + pltpu.roll(t, by, 0)
        return t

    def form(left, right, size_left, size_right):
        acc = zero
        for i in range(size_left):
            inner = rows[i, 0] * right[0]
            for j in range(1, size_right):
                inner = inner + rows[i, j] * right[j]
            acc = acc + left[i] * inner
        return summed(acc)

    search = [zero + 1.0] + [zero] * ITERS
    resid = [zero + 1.0] + [zero] * ITERS
    moves = [zero] * BASIS
    gamma = summed(rows[0, 0])
    lengths = jnp.zeros((8, 128), F32)
    for k in range(ITERS):
        image = list(search)
        for j in range(k + 1):
            image[j] = image[j] - al[j] * search[j]
            image[j + 1] = image[j + 1] - inv[j] * search[j]
            if j:
                image[j - 1] = image[j - 1] - be[j] * search[j]
        step = gamma / form(search, image, k + 1, k + 2)
        lengths = jnp.where(lane == k, step, lengths)
        moves = [moves[j] + step[None] * search[j] if j <= k else moves[j] for j in range(BASIS)]
        resid = [resid[j] - step[None] * image[j] if j <= k + 1 else resid[j] for j in range(BASIS)]
        if k + 1 < ITERS:
            after = form(resid, resid, k + 2, k + 2)
            ratio = after / gamma
            search = [resid[j] + ratio[None] * search[j] if j <= k + 1 else zero for j in range(BASIS)]
            gamma = after
    len_out[...] = lengths[0:1, :ITERS]
    here = slab == gz
    moves = [summed(jnp.where(here, v, 0.0)) for v in moves]
    resid = [summed(jnp.where(here, v, 0.0)) for v in resid]
    for x in range(EDGE):
        for c in range(3):
            dip = kept[x, 27 + c]
            res = jnp.zeros((8, 128), F32)
            for k in range(BASIS):
                u = kept[x, k * 3 + c]
                if k < ITERS:
                    dip = dip + moves[k] * u
                res = res + resid[k] * u
            res = res * kept[x, 30]
            for out, v in ((dip_out, dip), (res_out, res)):
                for t in range(3):
                    w = roll_lanes(v, t * WIDE + 18)
                    for s in range(2):
                        out[x, 3 * s + t, c : c + 1, :] = w[s : s + 1, :EDGE]


def per_device(permanent_field, polar, jitter, neighbors):
    packed = pl.pallas_call(
        pack_kernel,
        out_shape=jax.ShapeDtypeStruct((EDGE, GROUPS, 2, 128), F32),
        in_specs=[pl.BlockSpec(memory_space=pltpu.HBM)] * 4,
        scratch_shapes=[
            pltpu.VMEM((EDGE, EDGE, 3, EDGE), F32),
            pltpu.VMEM((EDGE, EDGE, EDGE), F32),
            pltpu.VMEM((EDGE, EDGE, 3, EDGE), F32),
            pltpu.VMEM((EDGE, EDGE, EDGE, 56), jnp.int32),
            pltpu.SemaphoreType.DMA((4,)),
        ],
        compiler_params=pltpu.CompilerParams(vmem_limit_bytes=8 * 1024 * 1024),
        name="pack",
    )(*(pltpu.with_memory_space_constraint(v, pltpu.HBM) for v in (permanent_field.transpose(0, 1, 3, 2), polar, jitter.transpose(0, 1, 3, 2), neighbors)))

    around = [packed] + [
        lax.ppermute(packed, "gy", [((i + k) % 4, i) for i in range(4)]) for k in (1, 2, 3)
    ]
    half = jnp.concatenate(around, axis=2)

    def swap(v):
        return lax.ppermute(v, "gx", [(0, 1), (1, 0)])

    own = jnp.concatenate([half, swap(half)], axis=0)

    def fetch(k):
        pairs = [((i + k) % 16, i) for i in range(16)]
        pairs += [(16 + (i - k) % 16, 16 + i) for i in range(16)]
        return lax.ppermute(own, ("gx",) + GZ, pairs)

    direct = [fetch(k) for k in (1, 2, 3)]
    passed = [swap(v) for v in direct]

    vreg = (8, 128)
    kept, info = pl.pallas_call(
        region_kernel,
        out_shape=(
            jax.ShapeDtypeStruct((EDGE, 31) + vreg, F32),
            jax.ShapeDtypeStruct((16,) + vreg, F32),
        ),
        scratch_shapes=[
            pltpu.VMEM((NX, 36) + vreg, F32),
            pltpu.VMEM((NX, 20) + vreg, F32),
            pltpu.VMEM((NX, 4 * len(OFFSETS)) + vreg, F32),
            pltpu.VMEM((NX, 16) + vreg, F32),
            pltpu.VMEM((BASIS + 1, 3 * NX) + vreg, F32),
            pltpu.VMEM((3 * NX,) + vreg, F32),
            pltpu.VMEM((3 * NX,) + vreg, F32),
            pltpu.VMEM((3 * NX,) + vreg, F32),
        ],
        compiler_params=pltpu.CompilerParams(vmem_limit_bytes=36 * 1024 * 1024),
        name="region",
    )(own, *direct, *passed)

    info = lax.all_to_all(info, GZ, 0, 0, tiled=True)

    dip, res, lengths = pl.pallas_call(
        finish_kernel,
        out_shape=(
            jax.ShapeDtypeStruct((EDGE, EDGE, 3, EDGE), F32),
            jax.ShapeDtypeStruct((EDGE, EDGE, 3, EDGE), F32),
            jax.ShapeDtypeStruct((1, ITERS), F32),
        ),
        compiler_params=pltpu.CompilerParams(vmem_limit_bytes=8 * 1024 * 1024),
        name="finish",
    )(kept, info)
    return dip.transpose(0, 1, 3, 2), res.transpose(0, 1, 3, 2), lengths.reshape(ITERS)


def solution(mesh):
    finer = Mesh(
        mesh.devices.reshape(mesh.shape["gx"], mesh.shape["gy"], 4, 4), ("gx", "gy", "gz_0", "gz_1")
    )
    return jax.shard_map(
        per_device,
        mesh=finer,
        in_specs=(
            P("gx", "gy", GZ, None),
            P("gx", "gy", GZ),
            P("gx", "gy", GZ, None),
            P("gx", "gy", GZ, None),
        ),
        out_specs=(P("gx", "gy", GZ, None), P("gx", "gy", GZ, None), P()),
        check_vma=False,
    )
```

```python
import jax
import jax.numpy as jnp
from jax import lax
from jax.experimental import pallas as pl
from jax.experimental.pallas import tpu as pltpu
from jax.sharding import Mesh
from jax.sharding import PartitionSpec as P

ITERS = 8
BASIS = ITERS + 1
THOLE = 0.39
SPACING = 3.5
EDGE = 6
NX = 12
WIDE = 42
GZ = ("gz_0", "gz_1")
F32 = jnp.float32

OFFSETS = [
    (a, b, c)
    for a in range(-2, 3)
    for b in range(-2, 3)
    for c in range(-2, 3)
    if 1 <= a * a + b * b + c * c <= 5
]
FORWARD = [d for d in OFFSETS if d > (0, 0, 0)]
GROUPS, PER = 5, 7


FIRSTS = {min(n for n, d in enumerate(FORWARD) if d[2] == dz) for dz in range(-2, 3)}


def lane_iota():
    return lax.broadcasted_iota(jnp.int32, (8, 128), 1)


def third_masks():
    lane = lane_iota()
    return lane < WIDE, lane >= 2 * WIDE


def roll_lanes(v, ahead):
    ahead = ahead % 128
    return v if ahead == 0 else pltpu.roll(v, 128 - ahead, 1)


def roll_rows(v, ahead):
    return pltpu.roll(v, (-ahead) % 8, 0)


def shifted(v, dy, dz, first, last):
    if dy == 0:
        return roll_lanes(v, dz)
    if dy == 1:
        return jnp.where(
            last, roll_rows(roll_lanes(v, dz - 2 * WIDE), 1), roll_lanes(v, dz + WIDE)
        )
    if dy == 2:
        return jnp.where(
            first, roll_lanes(v, dz + 2 * WIDE), roll_rows(roll_lanes(v, dz - WIDE), 1)
        )
    if dy == -1:
        return jnp.where(
            first, roll_rows(roll_lanes(v, dz + 2 * WIDE), -1), roll_lanes(v, dz - WIDE)
        )
    return jnp.where(
        last, roll_lanes(v, dz - 2 * WIDE), roll_rows(roll_lanes(v, dz + WIDE), -1)
    )


def wrap(x):
    if isinstance(x, int):
        return x % NX
    return jnp.where(x >= NX, x - NX, jnp.where(x < 0, x + NX, x))


def total(v):
    return jnp.sum(jnp.sum(v, axis=0, keepdims=True), axis=1, keepdims=True)


def unrolled(count, times, body, carry):
    def several(i, carry):
        for t in range(times):
            carry = body(i * times + t, carry)
        return carry

    return lax.fori_loop(0, count // times, several, carry)


def pack_kernel(
    field_in, polar_in, jitter_in, neighbors_in, out, field, polar, jitter, neighbors, arrived
):
    given = (neighbors_in, field_in, jitter_in, polar_in)
    kept = (neighbors, field, jitter, polar)
    copies = [pltpu.make_async_copy(g, k, arrived.at[n]) for n, (g, k) in enumerate(zip(given, kept))]
    for copy in copies:
        copy.start()
    lane = lax.broadcasted_iota(jnp.int32, (1, 128), 1)
    third = jnp.where(lane >= 2 * WIDE, 2, jnp.where(lane >= WIDE, 1, 0))
    inside = lane - third * WIDE
    member = inside // EDGE
    z = inside - member * EDGE
    wanted = []
    for group in range(1, GROUPS):
        code = jnp.full((1, 128), -5000, jnp.int32)
        for n in range(PER):
            d = FORWARD[(group - 1) * PER + n]
            code = jnp.where(member == n, d[0] * 100 + d[1] * 10 + d[2], code)
        wanted.append(jnp.where(lane < 3 * WIDE, code + third * 10 + z, -5000))
    row = lax.broadcasted_iota(jnp.int32, (EDGE, 128), 0)
    column = lax.broadcasted_iota(jnp.int32, (EDGE, 128), 1)
    pick = []
    for t in range(3):
        hit = column * 0 > 0
        for n in range(PER):
            hit = hit | (column == row + (t * WIDE + n * EDGE))
        pick.append((jnp.where(hit, 32.0, 0.0).astype(jnp.bfloat16), jnp.where(hit, 1.0, 0.0).astype(jnp.bfloat16)))

    for copy in copies:
        copy.wait()

    def one(x, carry):
        for s in range(2):
            slots = jnp.zeros((56, 128), F32)
            values = jnp.zeros((1, 128), F32)
            for t in range(3):
                y = 3 * s + t
                entry = neighbors[x, y]
                high = lax.shift_right_arithmetic(entry, 5)
                low = entry & 31
                for part, chosen in zip((high, low), pick[t]):
                    slots = slots + lax.dot_general(
                        part.astype(F32).astype(jnp.bfloat16), chosen, (((0,), (0,)), ((), ())),
                        preferred_element_type=F32,
                    )
                parts = [field[x, y, c : c + 1, :] for c in range(3)]
                parts += [polar[x, y : y + 1, :]]
                parts += [jitter[x, y, c : c + 1, :] for c in range(3)]
                for n in range(PER):
                    wide = jnp.concatenate([parts[n], jnp.zeros((1, 122), F32)], axis=1)
                    start = t * WIDE + n * EDGE
                    values = values + (pltpu.roll(wide, start, 1) if start else wide)
            out[x, 0, s : s + 1, :] = values
            home = (x + 2) * 100 + (2 + 3 * s) * 10 + 2
            for group in range(1, GROUPS):
                target = (wanted[group - 1] + home).astype(F32)
                flag = jnp.max(jnp.where(slots == target, 1.0, 0.0), axis=0, keepdims=True)
                out[x, group, s : s + 1, :] = flag
        return carry

    unrolled(EDGE, 2, one, 0)


def region_kernel(
    own, a1, a2, a3, b1, b2, b3, kept_out, info_out, chan, near, coef, moved, basis,
    raw, now, past,
):
    gx = lax.axis_index("gx")
    gy = lax.axis_index("gy")
    lane = lane_iota()
    first, last = third_masks()
    along = lane - jnp.where(last, 2 * WIDE, jnp.where(first, 0, WIDE))
    is_low = (lane * 0 + gx) == 0

    def gather(x, carry):
        half = x // EDGE
        within = x - half * EDGE
        here = within + jnp.where(half == gx, 0, EDGE)
        there = within + jnp.where(half == gx, EDGE, 0)
        for group in range(GROUPS):
            ahead = [jnp.where(is_low, a[here, group], b[there, group]) for a, b in ((a1, b1), (a2, b2), (a3, b3))]
            back = [jnp.where(is_low, b[there, group], a[here, group]) for a, b in ((a3, b3), (a2, b2), (a1, b1))]
            blocks = back + [own[here, group]] + ahead
            outs = [None] * PER
            for gap in range(-6, 7):
                members = [m for m in range(PER) if 0 <= m + gap < PER]
                mixed = blocks[members[0] + gap]
                for m in members[1:]:
                    mixed = jnp.where(along >= 6 * m, blocks[m + gap], mixed)
                mixed = roll_lanes(mixed, -6 * gap)
                for m in members:
                    outs[m] = (
                        mixed if outs[m] is None
                        else jnp.where(along >= 6 * (m + gap), mixed, outs[m])
                    )
            for member in range(PER):
                acc = pltpu.roll(outs[member], 2 * gy, 0)
                if group * PER + member == 3:
                    acc = jnp.where(lane >= 3 * WIDE, 1.0, acc)
                    chan[x, 35] = 1.0 / acc
                chan[x, group * PER + member] = acc
        return carry

    unrolled(NX, 2, gather, 0)

    def spread(x, carry):
        for c in range(4):
            v = chan[x, 3 + c]
            for dy in range(-2, 3):
                near[x, (dy + 2) * 4 + c] = shifted(v, dy, 0, first, last)
        return carry

    unrolled(NX, 3, spread, 0)

    def pairs(x, carry):
        for number, d in sorted(enumerate(FORWARD), key=lambda t: t[1][2]):
            if number in FIRSTS:
                home = [roll_lanes(chan[x, 3 + c], -d[2]) for c in range(4)]
            other = wrap(x + d[0])
            place = (d[1] + 2) * 4
            polar, *jit = home
            sep = [((near[other, place + 1 + c] - jit[c]) + float(d[c])) * SPACING for c in range(3)]
            dist_sq = sep[0] * sep[0] + sep[1] * sep[1] + sep[2] * sep[2]
            over = lax.rsqrt(dist_sq)
            cube = dist_sq * dist_sq * over
            over_sq = over * over
            over_cube = over_sq * over
            damping = THOLE * cube * lax.rsqrt(polar * near[other, place])
            falloff = jnp.exp(-damping)
            iso = (1.0 - falloff) * over_cube
            radial = 3.0 * (1.0 - (1.0 + damping) * falloff) * over_cube * over_sq
            root = jnp.sqrt(radial)
            here = roll_lanes(chan[x, 7 + number], -d[2]) > 0.5
            values = [jnp.where(here, s * root, 0.0) for s in sep] + [jnp.where(here, iso, 0.0)]
            ahead = OFFSETS.index(d) * 4
            behind = OFFSETS.index((-d[0], -d[1], -d[2])) * 4
            for c in range(4):
                coef[x, ahead + c] = values[c]
                coef[other, behind + c] = shifted(values[c], -d[1], d[2], first, last)
        return carry

    lax.fori_loop(0, NX, pairs, 0)

    def move(x, c, v):
        for dy in range(-2, 3):
            moved[x, (dy + 2) * 3 + c] = shifted(v, dy, 0, first, last)

    def couple(x):
        acc = {dz: [None] * 3 for dz in range(-2, 3)}
        for dx in range(-2, 3):
            other = wrap(x + dx)
            for dy in range(-2, 3):
                v = [moved[other, (dy + 2) * 3 + c] for c in range(3)]
                for dz in range(-2, 3):
                    if (dx, dy, dz) not in OFFSETS:
                        continue
                    number = OFFSETS.index((dx, dy, dz)) * 4
                    s = [coef[x, number + c] for c in range(3)]
                    iso = coef[x, number + 3]
                    dot = s[0] * v[0] + s[1] * v[1] + s[2] * v[2]
                    new = [s[c] * dot - iso * v[c] for c in range(3)]
                    acc[dz] = [n if t is None else t + n for t, n in zip(acc[dz], new)]
        out = acc[0]
        for dz in (1, -1, 2, -2):
            out = [o + roll_lanes(t, dz) for o, t in zip(out, acc[dz])]
        return out

    zero = jnp.zeros((8, 128), F32)
    slab = (along >= 18) & (along < 24)

    def prepare(x, carry):
        for c in range(3):
            raw[x * 3 + c] = chan[x, 3] * chan[x, c]
            now[x * 3 + c] = zero
            past[x * 3 + c] = zero
        return carry

    unrolled(NX, 4, prepare, 0)

    def next_vector(x, c, al, be, sc):
        return (raw[x * 3 + c] - al * now[x * 3 + c] - be * past[x * 3 + c]) * sc

    def extend(k, carry):
        info, before, al, be, sc = carry
        sums = [zero] * 4

        def scale(x):
            for c in range(3):
                new = next_vector(x, c, al, be, sc)
                past[x * 3 + c] = now[x * 3 + c]
                now[x * 3 + c] = new
                basis[k, x * 3 + c] = new
                move(x, c, new)

        for x in (10, 11, 0, 1, 2):
            scale(x)
        for x in range(NX):
            if 3 <= x + 3 < 10:
                scale(x + 3)
            out = couple(x)
            polar = chan[x, 3]
            over = chan[x, 35]
            for c in range(3):
                u = now[x * 3 + c]
                w = polar * out[c]
                raw[x * 3 + c] = w
                sums[0] = sums[0] + out[c] * u
                sums[1] = sums[1] + out[c] * past[x * 3 + c]
                sums[2] = sums[2] + out[c] * w
                sums[3] = sums[3] + (u * over) * u
        along_now, along_past, full, norm = [total(jnp.where(slab, t, 0.0)) for t in sums]
        live = k > 0
        norm = jnp.where(live, norm, 0.0)
        tiny = 1e-36
        al = jnp.where(norm > tiny, along_now / jnp.maximum(norm, tiny), 0.0)
        be = jnp.where(before > tiny, along_past / jnp.maximum(before, tiny), 0.0)
        rest = full - al * along_now - be * along_past
        rest = jnp.maximum(rest, 1e-10 * full)
        good = (rest > tiny) & (norm > tiny)
        inv = jnp.where(good, jnp.sqrt(rest / jnp.maximum(norm, tiny)), 1.0)
        inv = jnp.minimum(jnp.maximum(inv, 1e-6), 1e3)
        info = jnp.where(lane == 44 + k, jnp.where(live, al, info), info)
        info = jnp.where(lane == 52 + k, jnp.where(live, be, info), info)
        info = jnp.where(lane == 60 + k, jnp.where(live, inv, info), info)
        return info, norm, al, be, 1.0 / inv

    none = jnp.zeros((1, 1), F32)
    info, _, al, be, sc = lax.fori_loop(0, BASIS, extend, (zero, none, none, none, none + 1.0))

    def end(x, carry):
        for c in range(3):
            basis[BASIS, x * 3 + c] = next_vector(x, c, al, be, sc)
        return carry

    unrolled(NX, 4, end, 0)

    number = 0
    for low, high in ((0, 3), (3, BASIS)):
        entries = [(i, j) for i in range(low, high) for j in range(i, BASIS)]

        def one(x, sums):
            sums = list(sums)
            for c in range(3):
                u = {j: basis[j + 1, x * 3 + c] for j in range(low, BASIS)}
                for i in range(low, high):
                    weighted = u[i] * chan[x, 35]
                    for n, (p, q) in enumerate(entries):
                        if p == i:
                            sums[n] = sums[n] + weighted * u[q]
            return tuple(sums)

        sums = unrolled(NX, 2, one, (zero,) * len(entries))
        for n in range(len(entries)):
            info = jnp.where(lane == number, total(jnp.where(slab, sums[n], 0.0)), info)
            number += 1

    for e in range(16):
        info_out[e] = info[0:1, :]

    def keep(x, carry):
        far = x + EDGE * gx

        def front(v):
            return pltpu.roll(v, 8 - 2 * gy, 0)

        for c in range(3):
            for k in range(BASIS):
                kept_out[x, k * 3 + c] = front(basis[k + 1, far * 3 + c])
            kept_out[x, 27 + c] = front(basis[0, far * 3 + c])
        kept_out[x, 30] = front(chan[far, 35])
        return carry

    unrolled(EDGE, 2, keep, 0)


def finish_kernel(kept, info, dip_out, res_out, len_out):
    gz = lax.axis_index("gz_0") * 4 + lax.axis_index("gz_1")
    table = jnp.concatenate([info[e] for e in range(16)], axis=0)
    wide = (2, 8, 128)

    def column(n):
        return jnp.broadcast_to(table[:, n : n + 1], (16, 128)).reshape(wide)

    rows = {}
    number = 0
    for low, high in ((0, 3), (3, BASIS)):
        for i in range(low, high):
            for j in range(i, BASIS):
                rows[i, j] = rows[j, i] = column(number)
                number += 1
    al = [column(45 + k) for k in range(ITERS)]
    be = [column(53 + k) for k in range(ITERS)]
    inv = [column(61 + k) for k in range(ITERS)]
    zero = jnp.zeros(wide, F32)
    slab = lax.broadcasted_iota(jnp.int32, wide, 0) * 8 + lax.broadcasted_iota(jnp.int32, wide, 1)
    lane = lax.broadcasted_iota(jnp.int32, (8, 128), 1)

    def summed(v):
        t = v[0] + v[1]
        for by in (4, 2, 1):
            t = t + pltpu.roll(t, by, 0)
        return t

    def form(left, right, size_left, size_right):
        acc = zero
        for i in range(size_left):
            inner = rows[i, 0] * right[0]
            for j in range(1, size_right):
                inner = inner + rows[i, j] * right[j]
            acc = acc + left[i] * inner
        return summed(acc)

    search = [zero + 1.0] + [zero] * ITERS
    resid = [zero + 1.0] + [zero] * ITERS
    moves = [zero] * BASIS
    gamma = summed(rows[0, 0])
    lengths = jnp.zeros((8, 128), F32)
    for k in range(ITERS):
        image = list(search)
        for j in range(k + 1):
            image[j] = image[j] - al[j] * search[j]
            image[j + 1] = image[j + 1] - inv[j] * search[j]
            if j:
                image[j - 1] = image[j - 1] - be[j] * search[j]
        step = gamma / form(search, image, k + 1, k + 2)
        lengths = jnp.where(lane == k, step, lengths)
        moves = [moves[j] + step[None] * search[j] if j <= k else moves[j] for j in range(BASIS)]
        resid = [resid[j] - step[None] * image[j] if j <= k + 1 else resid[j] for j in range(BASIS)]
        if k + 1 < ITERS:
            after = form(resid, resid, k + 2, k + 2)
            ratio = after / gamma
            search = [resid[j] + ratio[None] * search[j] if j <= k + 1 else zero for j in range(BASIS)]
            gamma = after
    len_out[...] = lengths[0:1, :ITERS]
    here = slab == gz
    moves = [summed(jnp.where(here, v, 0.0)) for v in moves]
    resid = [summed(jnp.where(here, v, 0.0)) for v in resid]
    for x in range(EDGE):
        for c in range(3):
            dip = kept[x, 27 + c]
            res = jnp.zeros((8, 128), F32)
            for k in range(BASIS):
                u = kept[x, k * 3 + c]
                if k < ITERS:
                    dip = dip + moves[k] * u
                res = res + resid[k] * u
            res = res * kept[x, 30]
            for out, v in ((dip_out, dip), (res_out, res)):
                for t in range(3):
                    w = roll_lanes(v, t * WIDE + 18)
                    for s in range(2):
                        out[x, 3 * s + t, c : c + 1, :] = w[s : s + 1, :EDGE]


def per_device(permanent_field, polar, jitter, neighbors):
    packed = pl.pallas_call(
        pack_kernel,
        out_shape=jax.ShapeDtypeStruct((EDGE, GROUPS, 2, 128), F32),
        in_specs=[pl.BlockSpec(memory_space=pltpu.HBM)] * 4,
        scratch_shapes=[
            pltpu.VMEM((EDGE, EDGE, 3, EDGE), F32),
            pltpu.VMEM((EDGE, EDGE, EDGE), F32),
            pltpu.VMEM((EDGE, EDGE, 3, EDGE), F32),
            pltpu.VMEM((EDGE, EDGE, EDGE, 56), jnp.int32),
            pltpu.SemaphoreType.DMA((4,)),
        ],
        compiler_params=pltpu.CompilerParams(vmem_limit_bytes=8 * 1024 * 1024),
        name="pack",
    )(*(pltpu.with_memory_space_constraint(v, pltpu.HBM) for v in (permanent_field.transpose(0, 1, 3, 2), polar, jitter.transpose(0, 1, 3, 2), neighbors)))

    def swap(v):
        return lax.ppermute(v, "gx", [(0, 1), (1, 0)])

    both = jnp.concatenate([packed, swap(packed)], axis=0)
    beside = lax.ppermute(
        both,
        ("gx", "gy"),
        [((i + 1) % 4, i) for i in range(4)] + [(4 + (i - 1) % 4, 4 + i) for i in range(4)],
    )
    across = lax.ppermute(both, "gy", [((i + 2) % 4, i) for i in range(4)])
    other = swap(beside)
    other = jnp.concatenate([other[EDGE:], other[:EDGE]], axis=0)
    low = lax.axis_index("gx") == 0
    own = jnp.concatenate(
        [both, jnp.where(low, beside, other), across, jnp.where(low, other, beside)], axis=2
    )

    def fetch(k):
        pairs = [((i + k) % 16, i) for i in range(16)]
        pairs += [(16 + (i - k) % 16, 16 + i) for i in range(16)]
        return lax.ppermute(own, ("gx",) + GZ, pairs)

    direct = [fetch(k) for k in (1, 2, 3)]
    passed = [swap(v) for v in direct]

    vreg = (8, 128)
    kept, info = pl.pallas_call(
        region_kernel,
        out_shape=(
            jax.ShapeDtypeStruct((EDGE, 31) + vreg, F32),
            jax.ShapeDtypeStruct((16, 1, 128), F32),
        ),
        scratch_shapes=[
            pltpu.VMEM((NX, 36) + vreg, F32),
            pltpu.VMEM((NX, 20) + vreg, F32),
            pltpu.VMEM((NX, 4 * len(OFFSETS)) + vreg, F32),
            pltpu.VMEM((NX, 16) + vreg, F32),
            pltpu.VMEM((BASIS + 1, 3 * NX) + vreg, F32),
            pltpu.VMEM((3 * NX,) + vreg, F32),
            pltpu.VMEM((3 * NX,) + vreg, F32),
            pltpu.VMEM((3 * NX,) + vreg, F32),
        ],
        compiler_params=pltpu.CompilerParams(vmem_limit_bytes=36 * 1024 * 1024),
        name="region",
    )(own, *direct, *passed)

    info = lax.all_to_all(info, GZ, 0, 0, tiled=True)

    dip, res, lengths = pl.pallas_call(
        finish_kernel,
        out_shape=(
            jax.ShapeDtypeStruct((EDGE, EDGE, 3, EDGE), F32),
            jax.ShapeDtypeStruct((EDGE, EDGE, 3, EDGE), F32),
            jax.ShapeDtypeStruct((1, ITERS), F32),
        ),
        compiler_params=pltpu.CompilerParams(vmem_limit_bytes=8 * 1024 * 1024),
        name="finish",
    )(kept, info)
    return dip.transpose(0, 1, 3, 2), res.transpose(0, 1, 3, 2), lengths.reshape(ITERS)


def solution(mesh):
    finer = Mesh(
        mesh.devices.reshape(mesh.shape["gx"], mesh.shape["gy"], 4, 4), ("gx", "gy", "gz_0", "gz_1")
    )
    return jax.shard_map(
        per_device,
        mesh=finer,
        in_specs=(
            P("gx", "gy", GZ, None),
            P("gx", "gy", GZ),
            P("gx", "gy", GZ, None),
            P("gx", "gy", GZ, None),
        ),
        out_specs=(P("gx", "gy", GZ, None), P("gx", "gy", GZ, None), P()),
        check_vma=False,
    )
```

```python
import jax
import jax.numpy as jnp
from jax import lax
from jax.experimental import pallas as pl
from jax.experimental.pallas import tpu as pltpu
from jax.sharding import Mesh
from jax.sharding import PartitionSpec as P

ITERS = 8
BASIS = ITERS + 1
THOLE = 0.39
SPACING = 3.5
LOG2E = 1.4426950408889634
EDGE = 6
NX = 12
WIDE = 42
GZ = ("gz_0", "gz_1")
F32 = jnp.float32

OFFSETS = [
    (a, b, c)
    for a in range(-2, 3)
    for b in range(-2, 3)
    for c in range(-2, 3)
    if 1 <= a * a + b * b + c * c <= 5
]
FORWARD = [d for d in OFFSETS if d > (0, 0, 0)]
GROUPS, PER = 5, 7


def lane_iota():
    return lax.broadcasted_iota(jnp.int32, (8, 128), 1)


def third_masks():
    lane = lane_iota()
    return lane < WIDE, lane >= 2 * WIDE


def roll_lanes(v, ahead):
    ahead = ahead % 128
    return v if ahead == 0 else pltpu.roll(v, 128 - ahead, 1)


def roll_rows(v, ahead):
    return pltpu.roll(v, (-ahead) % 8, 0)


def shifted(v, dy, dz, first, last):
    if dy == 0:
        return roll_lanes(v, dz)
    if dy == 1:
        return jnp.where(
            last, roll_rows(roll_lanes(v, dz - 2 * WIDE), 1), roll_lanes(v, dz + WIDE)
        )
    if dy == 2:
        return jnp.where(
            first, roll_lanes(v, dz + 2 * WIDE), roll_rows(roll_lanes(v, dz - WIDE), 1)
        )
    if dy == -1:
        return jnp.where(
            first, roll_rows(roll_lanes(v, dz + 2 * WIDE), -1), roll_lanes(v, dz - WIDE)
        )
    return jnp.where(
        last, roll_lanes(v, dz - 2 * WIDE), roll_rows(roll_lanes(v, dz + WIDE), -1)
    )


def wrap(x):
    if isinstance(x, int):
        return x % NX
    return jnp.where(x >= NX, x - NX, jnp.where(x < 0, x + NX, x))


def total(v):
    return jnp.sum(jnp.sum(v, axis=0, keepdims=True), axis=1, keepdims=True)


def unrolled(count, times, body, carry):
    def several(i, carry):
        for t in range(times):
            carry = body(i * times + t, carry)
        return carry

    return lax.fori_loop(0, count // times, several, carry)


def pack_kernel(
    field_in, polar_in, jitter_in, neighbors_in, out, field, polar, jitter, neighbors, arrived
):
    given = (neighbors_in, field_in, jitter_in, polar_in)
    kept = (neighbors, field, jitter, polar)
    copies = [pltpu.make_async_copy(g, k, arrived.at[n]) for n, (g, k) in enumerate(zip(given, kept))]
    for copy in copies:
        copy.start()
    lane = lax.broadcasted_iota(jnp.int32, (1, 128), 1)
    third = jnp.where(lane >= 2 * WIDE, 2, jnp.where(lane >= WIDE, 1, 0))
    inside = lane - third * WIDE
    member = inside // EDGE
    z = inside - member * EDGE
    wanted = []
    for group in range(1, GROUPS):
        code = jnp.full((1, 128), -5000, jnp.int32)
        for n in range(PER):
            d = FORWARD[(group - 1) * PER + n]
            code = jnp.where(member == n, d[0] * 100 + d[1] * 10 + d[2], code)
        wanted.append(jnp.where(lane < 3 * WIDE, code + third * 10 + z, -5000))
    row = lax.broadcasted_iota(jnp.int32, (EDGE, 128), 0)
    column = lax.broadcasted_iota(jnp.int32, (EDGE, 128), 1)
    pick = []
    for t in range(3):
        hit = column * 0 > 0
        for n in range(PER):
            hit = hit | (column == row + (t * WIDE + n * EDGE))
        pick.append((jnp.where(hit, 32.0, 0.0).astype(jnp.bfloat16), jnp.where(hit, 1.0, 0.0).astype(jnp.bfloat16)))

    for copy in copies:
        copy.wait()

    def one(x, carry):
        for s in range(2):
            slots = jnp.zeros((56, 128), F32)
            values = jnp.zeros((1, 128), F32)
            for t in range(3):
                y = 3 * s + t
                entry = neighbors[x, y]
                high = lax.shift_right_arithmetic(entry, 5)
                low = entry & 31
                for part, chosen in zip((high, low), pick[t]):
                    slots = slots + lax.dot_general(
                        part.astype(F32).astype(jnp.bfloat16), chosen, (((0,), (0,)), ((), ())),
                        preferred_element_type=F32,
                    )
                parts = [field[x, y, c : c + 1, :] for c in range(3)]
                parts += [polar[x, y : y + 1, :]]
                parts += [jitter[x, y, c : c + 1, :] for c in range(3)]
                for n in range(PER):
                    wide = jnp.concatenate([parts[n], jnp.zeros((1, 122), F32)], axis=1)
                    start = t * WIDE + n * EDGE
                    values = values + (pltpu.roll(wide, start, 1) if start else wide)
            out[x, 0, s : s + 1, :] = values
            home = (x + 2) * 100 + (2 + 3 * s) * 10 + 2
            for group in range(1, GROUPS):
                target = (wanted[group - 1] + home).astype(F32)
                flag = jnp.max(jnp.where(slots == target, 1.0, 0.0), axis=0, keepdims=True)
                out[x, group, s : s + 1, :] = flag
        return carry

    unrolled(EDGE, 2, one, 0)


def region_kernel(
    own, a1, a2, a3, b1, b2, b3, kept_out, info_out, chan, near, home, coef, moved, basis,
    raw, now, past,
):
    gx = lax.axis_index("gx")
    gy = lax.axis_index("gy")
    lane = lane_iota()
    first, last = third_masks()
    along = lane - jnp.where(last, 2 * WIDE, jnp.where(first, 0, WIDE))
    is_low = (lane * 0 + gx) == 0

    def gather(x, carry):
        half = x // EDGE
        within = x - half * EDGE
        here = within + jnp.where(half == gx, 0, EDGE)
        there = within + jnp.where(half == gx, EDGE, 0)
        for group in range(GROUPS):
            ahead = [jnp.where(is_low, a[here, group], b[there, group]) for a, b in ((a1, b1), (a2, b2), (a3, b3))]
            back = [jnp.where(is_low, b[there, group], a[here, group]) for a, b in ((a3, b3), (a2, b2), (a1, b1))]
            blocks = back + [own[here, group]] + ahead
            outs = [None] * PER
            for gap in range(-6, 7):
                members = [m for m in range(PER) if 0 <= m + gap < PER]
                mixed = blocks[members[0] + gap]
                for m in members[1:]:
                    mixed = jnp.where(along >= 6 * m, blocks[m + gap], mixed)
                mixed = roll_lanes(mixed, -6 * gap)
                for m in members:
                    outs[m] = (
                        mixed if outs[m] is None
                        else jnp.where(along >= 6 * (m + gap), mixed, outs[m])
                    )
            for member in range(PER):
                acc = pltpu.roll(outs[member], 2 * gy, 0)
                if 4 <= group * PER + member < 7:
                    acc = acc * SPACING
                if group * PER + member == 3:
                    acc = jnp.where(lane >= 3 * WIDE, 1.0, acc)
                    chan[x, 35] = 1.0 / acc
                chan[x, group * PER + member] = acc
        return carry

    unrolled(NX, 2, gather, 0)

    def spread(x, carry):
        for c in range(4):
            v = chan[x, 3 + c]
            for step in range(-2, 3):
                near[x, (step + 2) * 4 + c] = shifted(v, step, 0, first, last)
                home[x, (step + 2) * 4 + c] = roll_lanes(v, -step)
        return carry

    unrolled(NX, 3, spread, 0)

    def pairs(x, carry):
        for number, d in sorted(enumerate(FORWARD), key=lambda t: t[1][2]):
            other = wrap(x + d[0])
            place = (d[1] + 2) * 4
            polar, *jit = [home[x, (d[2] + 2) * 4 + c] for c in range(4)]
            sep = [near[other, place + 1 + c] - jit[c] for c in range(3)]
            sep = [t + d[c] * SPACING if d[c] else t for c, t in enumerate(sep)]
            dist_sq = sep[0] * sep[0] + sep[1] * sep[1] + sep[2] * sep[2]
            over = lax.rsqrt(dist_sq)
            cube = dist_sq * dist_sq * over
            over_sq = over * over
            over_cube = over_sq * over
            damping = cube * (THOLE * lax.rsqrt(polar * near[other, place]))
            falloff = jnp.exp2(damping * -LOG2E)
            flag = roll_lanes(chan[x, 7 + number], -d[2])
            iso = (over_cube - falloff * over_cube) * flag
            radial = (3.0 - (3.0 + 3.0 * damping) * falloff) * (over_cube * over_sq)
            root = radial * lax.rsqrt(radial) * flag
            ahead = OFFSETS.index(d) * 4
            behind = OFFSETS.index((-d[0], -d[1], -d[2])) * 4
            for c in range(3):
                coef[x, ahead + c] = sep[c] * root
            coef[x, ahead + 3] = iso
            root = shifted(root, -d[1], d[2], first, last)
            coef[other, behind + 3] = shifted(iso, -d[1], d[2], first, last)
            for c in range(3):
                back = near[x, (2 - d[1]) * 4 + 1 + c] - home[other, (2 - d[2]) * 4 + 1 + c]
                back = back - d[c] * SPACING if d[c] else back
                coef[other, behind + c] = back * root
        return carry

    lax.fori_loop(0, NX, pairs, 0)

    def move(x, c, v):
        for dy in range(-2, 3):
            moved[x, (dy + 2) * 3 + c] = shifted(v, dy, 0, first, last)

    def couple(x):
        acc = {dz: [None] * 3 for dz in range(-2, 3)}
        for dx in range(-2, 3):
            other = wrap(x + dx)
            for dy in range(-2, 3):
                v = [moved[other, (dy + 2) * 3 + c] for c in range(3)]
                for dz in range(-2, 3):
                    if (dx, dy, dz) not in OFFSETS:
                        continue
                    number = OFFSETS.index((dx, dy, dz)) * 4
                    s = [coef[x, number + c] for c in range(3)]
                    iso = coef[x, number + 3]
                    dot = s[0] * v[0] + s[1] * v[1] + s[2] * v[2]
                    new = [s[c] * dot - iso * v[c] for c in range(3)]
                    acc[dz] = [n if t is None else t + n for t, n in zip(acc[dz], new)]
        out = acc[0]
        for dz in (1, -1, 2, -2):
            out = [o + roll_lanes(t, dz) for o, t in zip(out, acc[dz])]
        return out

    zero = jnp.zeros((8, 128), F32)
    slab = (along >= 18) & (along < 24)

    def prepare(x, carry):
        for c in range(3):
            raw[x * 3 + c] = chan[x, 3] * chan[x, c]
            now[x * 3 + c] = zero
            past[x * 3 + c] = zero
        return carry

    unrolled(NX, 4, prepare, 0)

    def next_vector(x, c, al, be, sc):
        return (raw[x * 3 + c] - al * now[x * 3 + c] - be * past[x * 3 + c]) * sc

    def extend(k, carry):
        info, before, al, be, sc = carry
        sums = [zero] * 4

        def scale(x):
            for c in range(3):
                new = next_vector(x, c, al, be, sc)
                past[x * 3 + c] = now[x * 3 + c]
                now[x * 3 + c] = new
                basis[k, x * 3 + c] = new
                move(x, c, new)

        for x in (10, 11, 0, 1, 2):
            scale(x)
        for x in range(NX):
            if 3 <= x + 3 < 10:
                scale(x + 3)
            out = couple(x)
            polar = chan[x, 3]
            over = chan[x, 35]
            for c in range(3):
                u = now[x * 3 + c]
                w = polar * out[c]
                raw[x * 3 + c] = w
                sums[0] = sums[0] + out[c] * u
                sums[1] = sums[1] + out[c] * past[x * 3 + c]
                sums[2] = sums[2] + out[c] * w
                sums[3] = sums[3] + (u * over) * u
        along_now, along_past, full, norm = [total(jnp.where(slab, t, 0.0)) for t in sums]
        live = k > 0
        norm = jnp.where(live, norm, 0.0)
        tiny = 1e-36
        over = jnp.where(norm > tiny, 1.0 / jnp.maximum(norm, tiny), 0.0)
        over_past = jnp.where(before > tiny, 1.0 / jnp.maximum(before, tiny), 0.0)
        al = along_now * over
        be = along_past * over_past
        rest = full - al * along_now - be * along_past
        rest = jnp.maximum(rest, 1e-10 * full)
        good = (rest > tiny) & (norm > tiny)
        sc = jnp.where(good, lax.rsqrt(jnp.maximum(rest * over, 1e-12)), 1.0)
        sc = jnp.maximum(sc, 1e-3)
        inv = 1.0 / sc
        info = jnp.where(lane == 44 + k, jnp.where(live, al, info), info)
        info = jnp.where(lane == 52 + k, jnp.where(live, be, info), info)
        info = jnp.where(lane == 60 + k, jnp.where(live, inv, info), info)
        return info, norm, al, be, sc

    none = jnp.zeros((1, 1), F32)
    info, _, al, be, sc = lax.fori_loop(0, BASIS, extend, (zero, none, none, none, none + 1.0))

    def end(x, carry):
        for c in range(3):
            basis[BASIS, x * 3 + c] = next_vector(x, c, al, be, sc)
        return carry

    unrolled(NX, 4, end, 0)

    number = 0
    for low, high in ((0, 3), (3, BASIS)):
        entries = [(i, j) for i in range(low, high) for j in range(i, BASIS)]

        def one(x, sums):
            sums = list(sums)
            for c in range(3):
                u = {j: basis[j + 1, x * 3 + c] for j in range(low, BASIS)}
                for i in range(low, high):
                    weighted = u[i] * chan[x, 35]
                    for n, (p, q) in enumerate(entries):
                        if p == i:
                            sums[n] = sums[n] + weighted * u[q]
            return tuple(sums)

        sums = unrolled(NX, 2, one, (zero,) * len(entries))
        for n in range(len(entries)):
            info = jnp.where(lane == number, total(jnp.where(slab, sums[n], 0.0)), info)
            number += 1

    for e in range(16):
        info_out[e] = info

    def keep(x, carry):
        far = x + EDGE * gx

        def front(v):
            return pltpu.roll(v, 8 - 2 * gy, 0)

        for c in range(3):
            for k in range(BASIS):
                kept_out[x, k * 3 + c] = front(basis[k + 1, far * 3 + c])
            kept_out[x, 27 + c] = front(basis[0, far * 3 + c])
        kept_out[x, 30] = front(chan[far, 35])
        return carry

    unrolled(EDGE, 2, keep, 0)


def finish_kernel(kept, info, dip_out, res_out, len_out):
    gz = lax.axis_index("gz_0") * 4 + lax.axis_index("gz_1")
    table = jnp.concatenate([info[e, 0:1, :] for e in range(16)], axis=0)
    wide = (2, 8, 128)

    def column(n):
        return jnp.broadcast_to(table[:, n : n + 1], (16, 128)).reshape(wide)

    rows = {}
    number = 0
    for low, high in ((0, 3), (3, BASIS)):
        for i in range(low, high):
            for j in range(i, BASIS):
                rows[i, j] = rows[j, i] = column(number)
                number += 1
    al = [column(45 + k) for k in range(ITERS)]
    be = [column(53 + k) for k in range(ITERS)]
    inv = [column(61 + k) for k in range(ITERS)]
    zero = jnp.zeros(wide, F32)
    slab = lax.broadcasted_iota(jnp.int32, wide, 0) * 8 + lax.broadcasted_iota(jnp.int32, wide, 1)
    lane = lax.broadcasted_iota(jnp.int32, (8, 128), 1)

    def summed(v):
        t = v[0] + v[1]
        for by in (4, 2, 1):
            t = t + pltpu.roll(t, by, 0)
        return t

    def form(left, right, size_left, size_right):
        acc = zero
        for i in range(size_left):
            inner = rows[i, 0] * right[0]
            for j in range(1, size_right):
                inner = inner + rows[i, j] * right[j]
            acc = acc + left[i] * inner
        return summed(acc)

    search = [zero + 1.0] + [zero] * ITERS
    resid = [zero + 1.0] + [zero] * ITERS
    moves = [zero] * BASIS
    gamma = summed(rows[0, 0])
    lengths = jnp.zeros((8, 128), F32)
    for k in range(ITERS):
        image = list(search)
        for j in range(k + 1):
            image[j] = image[j] - al[j] * search[j]
            image[j + 1] = image[j + 1] - inv[j] * search[j]
            if j:
                image[j - 1] = image[j - 1] - be[j] * search[j]
        step = gamma / form(search, image, k + 1, k + 2)
        lengths = jnp.where(lane == k, step, lengths)
        moves = [moves[j] + step[None] * search[j] if j <= k else moves[j] for j in range(BASIS)]
        resid = [resid[j] - step[None] * image[j] if j <= k + 1 else resid[j] for j in range(BASIS)]
        if k + 1 < ITERS:
            after = form(resid, resid, k + 2, k + 2)
            ratio = after / gamma
            search = [resid[j] + ratio[None] * search[j] if j <= k + 1 else zero for j in range(BASIS)]
            gamma = after
    len_out[...] = lengths[0:1, :ITERS]
    here = slab == gz
    moves = [summed(jnp.where(here, v, 0.0)) for v in moves]
    resid = [summed(jnp.where(here, v, 0.0)) for v in resid]
    for x in range(EDGE):
        for c in range(3):
            dip = kept[x, 27 + c]
            res = jnp.zeros((8, 128), F32)
            for k in range(BASIS):
                u = kept[x, k * 3 + c]
                if k < ITERS:
                    dip = dip + moves[k] * u
                res = res + resid[k] * u
            res = res * kept[x, 30]
            for out, v in ((dip_out, dip), (res_out, res)):
                for t in range(3):
                    w = roll_lanes(v, t * WIDE + 18)
                    for s in range(2):
                        out[x, 3 * s + t, c : c + 1, :] = w[s : s + 1, :EDGE]


def per_device(permanent_field, polar, jitter, neighbors):
    packed = pl.pallas_call(
        pack_kernel,
        out_shape=jax.ShapeDtypeStruct((EDGE, GROUPS, 2, 128), F32),
        in_specs=[pl.BlockSpec(memory_space=pltpu.HBM)] * 4,
        scratch_shapes=[
            pltpu.VMEM((EDGE, EDGE, 3, EDGE), F32),
            pltpu.VMEM((EDGE, EDGE, EDGE), F32),
            pltpu.VMEM((EDGE, EDGE, 3, EDGE), F32),
            pltpu.VMEM((EDGE, EDGE, EDGE, 56), jnp.int32),
            pltpu.SemaphoreType.DMA((4,)),
        ],
        compiler_params=pltpu.CompilerParams(vmem_limit_bytes=8 * 1024 * 1024),
        name="pack",
    )(*(pltpu.with_memory_space_constraint(v, pltpu.HBM) for v in (permanent_field.transpose(0, 1, 3, 2), polar, jitter.transpose(0, 1, 3, 2), neighbors)))

    around = [packed] + [
        lax.ppermute(packed, "gy", [((i + k) % 4, i) for i in range(4)]) for k in (1, 2, 3)
    ]
    half = jnp.concatenate(around, axis=2)

    def swap(v):
        return lax.ppermute(v, "gx", [(0, 1), (1, 0)])

    own = jnp.concatenate([half, swap(half)], axis=0)

    def fetch(k):
        pairs = [((i + k) % 16, i) for i in range(16)]
        pairs += [(16 + (i - k) % 16, 16 + i) for i in range(16)]
        return lax.ppermute(own, ("gx",) + GZ, pairs)

    direct = [fetch(k) for k in (1, 2, 3)]
    passed = [swap(v) for v in direct]

    vreg = (8, 128)
    kept, info = pl.pallas_call(
        region_kernel,
        out_shape=(
            jax.ShapeDtypeStruct((EDGE, 31) + vreg, F32),
            jax.ShapeDtypeStruct((16,) + vreg, F32),
        ),
        scratch_shapes=[
            pltpu.VMEM((NX, 36) + vreg, F32),
            pltpu.VMEM((NX, 20) + vreg, F32),
            pltpu.VMEM((NX, 20) + vreg, F32),
            pltpu.VMEM((NX, 4 * len(OFFSETS)) + vreg, F32),
            pltpu.VMEM((NX, 16) + vreg, F32),
            pltpu.VMEM((BASIS + 1, 3 * NX) + vreg, F32),
            pltpu.VMEM((3 * NX,) + vreg, F32),
            pltpu.VMEM((3 * NX,) + vreg, F32),
            pltpu.VMEM((3 * NX,) + vreg, F32),
        ],
        compiler_params=pltpu.CompilerParams(vmem_limit_bytes=36 * 1024 * 1024),
        name="region",
    )(own, *direct, *passed)

    info = lax.all_to_all(info, GZ, 0, 0, tiled=True)

    dip, res, lengths = pl.pallas_call(
        finish_kernel,
        out_shape=(
            jax.ShapeDtypeStruct((EDGE, EDGE, 3, EDGE), F32),
            jax.ShapeDtypeStruct((EDGE, EDGE, 3, EDGE), F32),
            jax.ShapeDtypeStruct((1, ITERS), F32),
        ),
        compiler_params=pltpu.CompilerParams(vmem_limit_bytes=8 * 1024 * 1024),
        name="finish",
    )(kept, info)
    return dip.transpose(0, 1, 3, 2), res.transpose(0, 1, 3, 2), lengths.reshape(ITERS)


def solution(mesh):
    finer = Mesh(
        mesh.devices.reshape(mesh.shape["gx"], mesh.shape["gy"], 4, 4), ("gx", "gy", "gz_0", "gz_1")
    )
    return jax.shard_map(
        per_device,
        mesh=finer,
        in_specs=(
            P("gx", "gy", GZ, None),
            P("gx", "gy", GZ),
            P("gx", "gy", GZ, None),
            P("gx", "gy", GZ, None),
        ),
        out_specs=(P("gx", "gy", GZ, None), P("gx", "gy", GZ, None), P()),
        check_vma=False,
    )
```

```python
import jax
import jax.numpy as jnp
from jax import lax
from jax.experimental import pallas as pl
from jax.experimental.pallas import tpu as pltpu
from jax.sharding import Mesh
from jax.sharding import PartitionSpec as P

ITERS = 8
BASIS = ITERS + 1
THOLE = 0.39
SPACING = 3.5
LOG2E = 1.4426950408889634
EDGE = 6
NX = 12
WIDE = 42
GZ = ("gz_0", "gz_1")
F32 = jnp.float32

OFFSETS = [
    (a, b, c)
    for a in range(-2, 3)
    for b in range(-2, 3)
    for c in range(-2, 3)
    if 1 <= a * a + b * b + c * c <= 5
]
FORWARD = [d for d in OFFSETS if d > (0, 0, 0)]
GROUPS, PER = 5, 7


def lane_iota():
    return lax.broadcasted_iota(jnp.int32, (8, 128), 1)


def third_masks():
    lane = lane_iota()
    return lane < WIDE, lane >= 2 * WIDE


def roll_lanes(v, ahead):
    ahead = ahead % 128
    return v if ahead == 0 else pltpu.roll(v, 128 - ahead, 1)


def roll_rows(v, ahead):
    return pltpu.roll(v, (-ahead) % 8, 0)


def shifted(v, dy, dz, first, last):
    if dy == 0:
        return roll_lanes(v, dz)
    if dy == 1:
        return jnp.where(
            last, roll_rows(roll_lanes(v, dz - 2 * WIDE), 1), roll_lanes(v, dz + WIDE)
        )
    if dy == 2:
        return jnp.where(
            first, roll_lanes(v, dz + 2 * WIDE), roll_rows(roll_lanes(v, dz - WIDE), 1)
        )
    if dy == -1:
        return jnp.where(
            first, roll_rows(roll_lanes(v, dz + 2 * WIDE), -1), roll_lanes(v, dz - WIDE)
        )
    return jnp.where(
        last, roll_lanes(v, dz - 2 * WIDE), roll_rows(roll_lanes(v, dz + WIDE), -1)
    )


def wrap(x):
    if isinstance(x, int):
        return x % NX
    return jnp.where(x >= NX, x - NX, jnp.where(x < 0, x + NX, x))


def total(v):
    return jnp.sum(jnp.sum(v, axis=0, keepdims=True), axis=1, keepdims=True)


def unrolled(count, times, body, carry):
    def several(i, carry):
        for t in range(times):
            carry = body(i * times + t, carry)
        return carry

    return lax.fori_loop(0, count // times, several, carry)


def pack_kernel(
    field_in, polar_in, jitter_in, neighbors_in, out, field, polar, jitter, neighbors, arrived
):
    given = (neighbors_in, field_in, jitter_in, polar_in)
    kept = (neighbors, field, jitter, polar)
    copies = [pltpu.make_async_copy(g, k, arrived.at[n]) for n, (g, k) in enumerate(zip(given, kept))]
    for copy in copies:
        copy.start()
    lane = lax.broadcasted_iota(jnp.int32, (1, 128), 1)
    third = jnp.where(lane >= 2 * WIDE, 2, jnp.where(lane >= WIDE, 1, 0))
    inside = lane - third * WIDE
    member = inside // EDGE
    z = inside - member * EDGE
    wanted = []
    for group in range(1, GROUPS):
        code = jnp.full((1, 128), -5000, jnp.int32)
        for n in range(PER):
            d = FORWARD[(group - 1) * PER + n]
            code = jnp.where(member == n, d[0] * 100 + d[1] * 10 + d[2], code)
        wanted.append(jnp.where(lane < 3 * WIDE, code + third * 10 + z, -5000))
    row = lax.broadcasted_iota(jnp.int32, (EDGE, 128), 0)
    column = lax.broadcasted_iota(jnp.int32, (EDGE, 128), 1)
    pick = []
    for t in range(3):
        hit = column * 0 > 0
        for n in range(PER):
            hit = hit | (column == row + (t * WIDE + n * EDGE))
        pick.append((jnp.where(hit, 32.0, 0.0).astype(jnp.bfloat16), jnp.where(hit, 1.0, 0.0).astype(jnp.bfloat16)))

    for copy in copies:
        copy.wait()

    def one(x, carry):
        for s in range(2):
            slots = jnp.zeros((56, 128), F32)
            values = jnp.zeros((1, 128), F32)
            for t in range(3):
                y = 3 * s + t
                entry = neighbors[x, y]
                high = lax.shift_right_arithmetic(entry, 5)
                low = entry & 31
                for part, chosen in zip((high, low), pick[t]):
                    slots = slots + lax.dot_general(
                        part.astype(F32).astype(jnp.bfloat16), chosen, (((0,), (0,)), ((), ())),
                        preferred_element_type=F32,
                    )
                parts = [field[x, y, c : c + 1, :] for c in range(3)]
                parts += [polar[x, y : y + 1, :]]
                parts += [jitter[x, y, c : c + 1, :] for c in range(3)]
                for n in range(PER):
                    wide = jnp.concatenate([parts[n], jnp.zeros((1, 122), F32)], axis=1)
                    start = t * WIDE + n * EDGE
                    values = values + (pltpu.roll(wide, start, 1) if start else wide)
            out[x, 0, s : s + 1, :] = values
            home = (x + 2) * 100 + (2 + 3 * s) * 10 + 2
            for group in range(1, GROUPS):
                target = (wanted[group - 1] + home).astype(F32)
                flag = jnp.max(jnp.where(slots == target, 1.0, 0.0), axis=0, keepdims=True)
                out[x, group, s : s + 1, :] = flag
        return carry

    unrolled(EDGE, 6, one, 0)


def region_kernel(
    own, a1, a2, a3, b1, b2, b3, kept_out, info_out, chan, near, home, coef, moved, basis,
    raw, now, past,
):
    gx = lax.axis_index("gx")
    gy = lax.axis_index("gy")
    lane = lane_iota()
    first, last = third_masks()
    along = lane - jnp.where(last, 2 * WIDE, jnp.where(first, 0, WIDE))
    is_low = (lane * 0 + gx) == 0

    def gather(x, carry):
        half = x // EDGE
        within = x - half * EDGE
        here = within + jnp.where(half == gx, 0, EDGE)
        there = within + jnp.where(half == gx, EDGE, 0)
        for group in range(GROUPS):
            ahead = [jnp.where(is_low, a[here, group], b[there, group]) for a, b in ((a1, b1), (a2, b2), (a3, b3))]
            back = [jnp.where(is_low, b[there, group], a[here, group]) for a, b in ((a3, b3), (a2, b2), (a1, b1))]
            blocks = back + [own[here, group]] + ahead
            outs = [None] * PER
            for gap in range(-6, 7):
                members = [m for m in range(PER) if 0 <= m + gap < PER]
                mixed = blocks[members[0] + gap]
                for m in members[1:]:
                    mixed = jnp.where(along >= 6 * m, blocks[m + gap], mixed)
                mixed = roll_lanes(mixed, -6 * gap)
                for m in members:
                    outs[m] = (
                        mixed if outs[m] is None
                        else jnp.where(along >= 6 * (m + gap), mixed, outs[m])
                    )
            for member in range(PER):
                acc = pltpu.roll(outs[member], 2 * gy, 0)
                if 4 <= group * PER + member < 7:
                    acc = acc * SPACING
                if group * PER + member == 3:
                    acc = jnp.where(lane >= 3 * WIDE, 1.0, acc)
                    chan[x, 35] = 1.0 / acc
                chan[x, group * PER + member] = acc
        return carry

    unrolled(NX, 2, gather, 0)

    def spread(x, carry):
        for c in range(4):
            v = chan[x, 3 + c]
            for step in range(-2, 3):
                near[x, (step + 2) * 4 + c] = shifted(v, step, 0, first, last)
                home[x, (step + 2) * 4 + c] = roll_lanes(v, -step)
        return carry

    unrolled(NX, 6, spread, 0)

    def pairs(x, carry):
        for number, d in sorted(enumerate(FORWARD), key=lambda t: t[1][2]):
            other = wrap(x + d[0])
            place = (d[1] + 2) * 4
            polar, *jit = [home[x, (d[2] + 2) * 4 + c] for c in range(4)]
            sep = [near[other, place + 1 + c] - jit[c] for c in range(3)]
            sep = [t + d[c] * SPACING if d[c] else t for c, t in enumerate(sep)]
            dist_sq = sep[0] * sep[0] + sep[1] * sep[1] + sep[2] * sep[2]
            over = lax.rsqrt(dist_sq)
            cube = dist_sq * dist_sq * over
            over_sq = over * over
            over_cube = over_sq * over
            damping = cube * (THOLE * lax.rsqrt(polar * near[other, place]))
            falloff = jnp.exp2(damping * -LOG2E)
            flag = roll_lanes(chan[x, 7 + number], -d[2])
            iso = (over_cube - falloff * over_cube) * flag
            radial = (3.0 - (3.0 + 3.0 * damping) * falloff) * (over_cube * over_sq)
            root = radial * lax.rsqrt(radial) * flag
            ahead = OFFSETS.index(d) * 4
            behind = OFFSETS.index((-d[0], -d[1], -d[2])) * 4
            for c in range(3):
                coef[x, ahead + c] = sep[c] * root
            coef[x, ahead + 3] = iso
            root = shifted(root, -d[1], d[2], first, last)
            coef[other, behind + 3] = shifted(iso, -d[1], d[2], first, last)
            for c in range(3):
                back = near[x, (2 - d[1]) * 4 + 1 + c] - home[other, (2 - d[2]) * 4 + 1 + c]
                back = back - d[c] * SPACING if d[c] else back
                coef[other, behind + c] = back * root
        return carry

    lax.fori_loop(0, NX, pairs, 0)

    def move(x, c, v):
        for dy in range(-2, 3):
            moved[x, (dy + 2) * 3 + c] = shifted(v, dy, 0, first, last)

    def couple(x):
        acc = {dz: [None] * 3 for dz in range(-2, 3)}
        for dx in range(-2, 3):
            other = wrap(x + dx)
            for dy in range(-2, 3):
                v = [moved[other, (dy + 2) * 3 + c] for c in range(3)]
                for dz in range(-2, 3):
                    if (dx, dy, dz) not in OFFSETS:
                        continue
                    number = OFFSETS.index((dx, dy, dz)) * 4
                    s = [coef[x, number + c] for c in range(3)]
                    iso = coef[x, number + 3]
                    dot = s[0] * v[0] + s[1] * v[1] + s[2] * v[2]
                    new = [s[c] * dot - iso * v[c] for c in range(3)]
                    acc[dz] = [n if t is None else t + n for t, n in zip(acc[dz], new)]
        out = acc[0]
        for dz in (1, -1, 2, -2):
            out = [o + roll_lanes(t, dz) for o, t in zip(out, acc[dz])]
        return out

    zero = jnp.zeros((8, 128), F32)
    slab = (along >= 18) & (along < 24)

    def prepare(x, carry):
        for c in range(3):
            raw[x * 3 + c] = chan[x, 3] * chan[x, c]
            now[x * 3 + c] = zero
            past[x * 3 + c] = zero
        return carry

    unrolled(NX, 4, prepare, 0)

    def next_vector(x, c, al, be, sc):
        return (raw[x * 3 + c] - al * now[x * 3 + c] - be * past[x * 3 + c]) * sc

    def extend(k, carry):
        info, before, al, be, sc = carry
        sums = [zero] * 4

        def scale(x):
            for c in range(3):
                new = next_vector(x, c, al, be, sc)
                past[x * 3 + c] = now[x * 3 + c]
                now[x * 3 + c] = new
                basis[k, x * 3 + c] = new
                move(x, c, new)

        for x in (10, 11, 0, 1, 2):
            scale(x)
        for x in range(NX):
            if 3 <= x + 3 < 10:
                scale(x + 3)
            out = couple(x)
            polar = chan[x, 3]
            over = chan[x, 35]
            for c in range(3):
                u = now[x * 3 + c]
                w = polar * out[c]
                raw[x * 3 + c] = w
                sums[0] = sums[0] + out[c] * u
                sums[1] = sums[1] + out[c] * past[x * 3 + c]
                sums[2] = sums[2] + out[c] * w
                sums[3] = sums[3] + (u * over) * u
        along_now, along_past, full, norm = [total(jnp.where(slab, t, 0.0)) for t in sums]
        live = k > 0
        norm = jnp.where(live, norm, 0.0)
        tiny = 1e-36
        over = jnp.where(norm > tiny, 1.0 / jnp.maximum(norm, tiny), 0.0)
        over_past = jnp.where(before > tiny, 1.0 / jnp.maximum(before, tiny), 0.0)
        al = along_now * over
        be = along_past * over_past
        rest = full - al * along_now - be * along_past
        rest = jnp.maximum(rest, 1e-10 * full)
        good = (rest > tiny) & (norm > tiny)
        sc = jnp.where(good, lax.rsqrt(jnp.maximum(rest * over, 1e-12)), 1.0)
        sc = jnp.maximum(sc, 1e-3)
        inv = 1.0 / sc
        info = jnp.where(lane == 44 + k, jnp.where(live, al, info), info)
        info = jnp.where(lane == 52 + k, jnp.where(live, be, info), info)
        info = jnp.where(lane == 60 + k, jnp.where(live, inv, info), info)
        return info, norm, al, be, sc

    none = jnp.zeros((1, 1), F32)
    info, _, al, be, sc = lax.fori_loop(0, BASIS, extend, (zero, none, none, none, none + 1.0))

    def end(x, carry):
        for c in range(3):
            basis[BASIS, x * 3 + c] = next_vector(x, c, al, be, sc)
        return carry

    unrolled(NX, 4, end, 0)

    number = 0
    for low, high in ((0, 3), (3, BASIS)):
        entries = [(i, j) for i in range(low, high) for j in range(i, BASIS)]

        def one(x, sums):
            sums = list(sums)
            for c in range(3):
                u = {j: basis[j + 1, x * 3 + c] for j in range(low, BASIS)}
                for i in range(low, high):
                    weighted = u[i] * chan[x, 35]
                    for n, (p, q) in enumerate(entries):
                        if p == i:
                            sums[n] = sums[n] + weighted * u[q]
            return tuple(sums)

        sums = unrolled(NX, 2, one, (zero,) * len(entries))
        for n in range(len(entries)):
            info = jnp.where(lane == number, total(jnp.where(slab, sums[n], 0.0)), info)
            number += 1

    for e in range(16):
        info_out[e] = info

    def keep(x, carry):
        far = x + EDGE * gx

        def front(v):
            return pltpu.roll(v, 8 - 2 * gy, 0)

        for c in range(3):
            for k in range(BASIS):
                kept_out[x, k * 3 + c] = front(basis[k + 1, far * 3 + c])
            kept_out[x, 27 + c] = front(basis[0, far * 3 + c])
        kept_out[x, 30] = front(chan[far, 35])
        return carry

    unrolled(EDGE, 2, keep, 0)


def finish_kernel(kept, info, dip_out, res_out, len_out):
    gz = lax.axis_index("gz_0") * 4 + lax.axis_index("gz_1")
    table = jnp.concatenate([info[e, 0:1, :] for e in range(16)], axis=0)
    wide = (2, 8, 128)

    def column(n):
        return jnp.broadcast_to(table[:, n : n + 1], (16, 128)).reshape(wide)

    rows = {}
    number = 0
    for low, high in ((0, 3), (3, BASIS)):
        for i in range(low, high):
            for j in range(i, BASIS):
                rows[i, j] = rows[j, i] = column(number)
                number += 1
    al = [column(45 + k) for k in range(ITERS)]
    be = [column(53 + k) for k in range(ITERS)]
    inv = [column(61 + k) for k in range(ITERS)]
    zero = jnp.zeros(wide, F32)
    slab = lax.broadcasted_iota(jnp.int32, wide, 0) * 8 + lax.broadcasted_iota(jnp.int32, wide, 1)
    lane = lax.broadcasted_iota(jnp.int32, (8, 128), 1)

    def summed(v):
        t = v[0] + v[1]
        for by in (4, 2, 1):
            t = t + pltpu.roll(t, by, 0)
        return t

    def form(left, right, size_left, size_right):
        acc = zero
        for i in range(size_left):
            inner = rows[i, 0] * right[0]
            for j in range(1, size_right):
                inner = inner + rows[i, j] * right[j]
            acc = acc + left[i] * inner
        return summed(acc)

    search = [zero + 1.0] + [zero] * ITERS
    resid = [zero + 1.0] + [zero] * ITERS
    moves = [zero] * BASIS
    gamma = summed(rows[0, 0])
    lengths = jnp.zeros((8, 128), F32)
    for k in range(ITERS):
        image = list(search)
        for j in range(k + 1):
            image[j] = image[j] - al[j] * search[j]
            image[j + 1] = image[j + 1] - inv[j] * search[j]
            if j:
                image[j - 1] = image[j - 1] - be[j] * search[j]
        step = gamma / form(search, image, k + 1, k + 2)
        lengths = jnp.where(lane == k, step, lengths)
        moves = [moves[j] + step[None] * search[j] if j <= k else moves[j] for j in range(BASIS)]
        resid = [resid[j] - step[None] * image[j] if j <= k + 1 else resid[j] for j in range(BASIS)]
        if k + 1 < ITERS:
            after = form(resid, resid, k + 2, k + 2)
            ratio = after / gamma
            search = [resid[j] + ratio[None] * search[j] if j <= k + 1 else zero for j in range(BASIS)]
            gamma = after
    len_out[...] = lengths[0:1, :ITERS]
    here = slab == gz
    moves = [summed(jnp.where(here, v, 0.0)) for v in moves]
    resid = [summed(jnp.where(here, v, 0.0)) for v in resid]
    for x in range(EDGE):
        for c in range(3):
            dip = kept[x, 27 + c]
            res = jnp.zeros((8, 128), F32)
            for k in range(BASIS):
                u = kept[x, k * 3 + c]
                if k < ITERS:
                    dip = dip + moves[k] * u
                res = res + resid[k] * u
            res = res * kept[x, 30]
            for out, v in ((dip_out, dip), (res_out, res)):
                for t in range(3):
                    w = roll_lanes(v, t * WIDE + 18)
                    for s in range(2):
                        out[x, 3 * s + t, c : c + 1, :] = w[s : s + 1, :EDGE]


def per_device(permanent_field, polar, jitter, neighbors):
    packed = pl.pallas_call(
        pack_kernel,
        out_shape=jax.ShapeDtypeStruct((EDGE, GROUPS, 2, 128), F32),
        in_specs=[pl.BlockSpec(memory_space=pltpu.HBM)] * 4,
        scratch_shapes=[
            pltpu.VMEM((EDGE, EDGE, 3, EDGE), F32),
            pltpu.VMEM((EDGE, EDGE, EDGE), F32),
            pltpu.VMEM((EDGE, EDGE, 3, EDGE), F32),
            pltpu.VMEM((EDGE, EDGE, EDGE, 56), jnp.int32),
            pltpu.SemaphoreType.DMA((4,)),
        ],
        compiler_params=pltpu.CompilerParams(vmem_limit_bytes=8 * 1024 * 1024),
        name="pack",
    )(*(pltpu.with_memory_space_constraint(v, pltpu.HBM) for v in (permanent_field.transpose(0, 1, 3, 2), polar, jitter.transpose(0, 1, 3, 2), neighbors)))

    around = [packed] + [
        lax.ppermute(packed, "gy", [((i + k) % 4, i) for i in range(4)]) for k in (1, 2, 3)
    ]
    half = jnp.concatenate(around, axis=2)

    def swap(v):
        return lax.ppermute(v, "gx", [(0, 1), (1, 0)])

    own = jnp.concatenate([half, swap(half)], axis=0)

    def fetch(k):
        pairs = [((i + k) % 16, i) for i in range(16)]
        pairs += [(16 + (i - k) % 16, 16 + i) for i in range(16)]
        return lax.ppermute(own, ("gx",) + GZ, pairs)

    direct = [fetch(k) for k in (1, 2, 3)]
    passed = [swap(v) for v in direct]

    vreg = (8, 128)
    kept, info = pl.pallas_call(
        region_kernel,
        out_shape=(
            jax.ShapeDtypeStruct((EDGE, 31) + vreg, F32),
            jax.ShapeDtypeStruct((16,) + vreg, F32),
        ),
        scratch_shapes=[
            pltpu.VMEM((NX, 36) + vreg, F32),
            pltpu.VMEM((NX, 20) + vreg, F32),
            pltpu.VMEM((NX, 20) + vreg, F32),
            pltpu.VMEM((NX, 4 * len(OFFSETS)) + vreg, F32),
            pltpu.VMEM((NX, 16) + vreg, F32),
            pltpu.VMEM((BASIS + 1, 3 * NX) + vreg, F32),
            pltpu.VMEM((3 * NX,) + vreg, F32),
            pltpu.VMEM((3 * NX,) + vreg, F32),
            pltpu.VMEM((3 * NX,) + vreg, F32),
        ],
        compiler_params=pltpu.CompilerParams(vmem_limit_bytes=36 * 1024 * 1024),
        name="region",
    )(own, *direct, *passed)

    info = lax.all_to_all(info, GZ, 0, 0, tiled=True)

    dip, res, lengths = pl.pallas_call(
        finish_kernel,
        out_shape=(
            jax.ShapeDtypeStruct((EDGE, EDGE, 3, EDGE), F32),
            jax.ShapeDtypeStruct((EDGE, EDGE, 3, EDGE), F32),
            jax.ShapeDtypeStruct((1, ITERS), F32),
        ),
        compiler_params=pltpu.CompilerParams(vmem_limit_bytes=8 * 1024 * 1024),
        name="finish",
    )(kept, info)
    return dip.transpose(0, 1, 3, 2), res.transpose(0, 1, 3, 2), lengths.reshape(ITERS)


def solution(mesh):
    finer = Mesh(
        mesh.devices.reshape(mesh.shape["gx"], mesh.shape["gy"], 4, 4), ("gx", "gy", "gz_0", "gz_1")
    )
    return jax.shard_map(
        per_device,
        mesh=finer,
        in_specs=(
            P("gx", "gy", GZ, None),
            P("gx", "gy", GZ),
            P("gx", "gy", GZ, None),
            P("gx", "gy", GZ, None),
        ),
        out_specs=(P("gx", "gy", GZ, None), P("gx", "gy", GZ, None), P()),
        check_vma=False,
    )
```

```python
import jax
import jax.numpy as jnp
from jax import lax
from jax.experimental import pallas as pl
from jax.experimental.pallas import tpu as pltpu
from jax.sharding import Mesh
from jax.sharding import PartitionSpec as P

ITERS = 8
BASIS = ITERS + 1
THOLE = 0.39
SPACING = 3.5
LOG2E = 1.4426950408889634
EDGE = 6
NX = 12
WIDE = 42
GZ = ("gz_0", "gz_1")
F32 = jnp.float32

OFFSETS = [
    (a, b, c)
    for a in range(-2, 3)
    for b in range(-2, 3)
    for c in range(-2, 3)
    if 1 <= a * a + b * b + c * c <= 5
]
FORWARD = [d for d in OFFSETS if d > (0, 0, 0)]
GROUPS, PER = 5, 7


def lane_iota():
    return lax.broadcasted_iota(jnp.int32, (8, 128), 1)


def third_masks():
    lane = lane_iota()
    return lane < WIDE, lane >= 2 * WIDE


def roll_lanes(v, ahead):
    ahead = ahead % 128
    return v if ahead == 0 else pltpu.roll(v, 128 - ahead, 1)


def roll_rows(v, ahead):
    return pltpu.roll(v, (-ahead) % 8, 0)


def shifted(v, dy, dz, first, last):
    if dy == 0:
        return roll_lanes(v, dz)
    if dy == 1:
        return jnp.where(
            last, roll_rows(roll_lanes(v, dz - 2 * WIDE), 1), roll_lanes(v, dz + WIDE)
        )
    if dy == 2:
        return jnp.where(
            first, roll_lanes(v, dz + 2 * WIDE), roll_rows(roll_lanes(v, dz - WIDE), 1)
        )
    if dy == -1:
        return jnp.where(
            first, roll_rows(roll_lanes(v, dz + 2 * WIDE), -1), roll_lanes(v, dz - WIDE)
        )
    return jnp.where(
        last, roll_lanes(v, dz - 2 * WIDE), roll_rows(roll_lanes(v, dz + WIDE), -1)
    )


def wrap(x):
    if isinstance(x, int):
        return x % NX
    return jnp.where(x >= NX, x - NX, jnp.where(x < 0, x + NX, x))


def total(v):
    return jnp.sum(jnp.sum(v, axis=0, keepdims=True), axis=1, keepdims=True)


def unrolled(count, times, body, carry):
    def several(i, carry):
        for t in range(times):
            carry = body(i * times + t, carry)
        return carry

    return lax.fori_loop(0, count // times, several, carry)


def pack_kernel(
    field_in, polar_in, jitter_in, neighbors_in, out, field, polar, jitter, neighbors, arrived
):
    given = (neighbors_in, field_in, jitter_in, polar_in)
    kept = (neighbors, field, jitter, polar)
    copies = [pltpu.make_async_copy(g, k, arrived.at[n]) for n, (g, k) in enumerate(zip(given, kept))]
    for copy in copies:
        copy.start()
    lane = lax.broadcasted_iota(jnp.int32, (1, 128), 1)
    third = jnp.where(lane >= 2 * WIDE, 2, jnp.where(lane >= WIDE, 1, 0))
    inside = lane - third * WIDE
    member = inside // EDGE
    z = inside - member * EDGE
    wanted = []
    for group in range(1, GROUPS):
        code = jnp.full((1, 128), -5000, jnp.int32)
        for n in range(PER):
            d = FORWARD[(group - 1) * PER + n]
            code = jnp.where(member == n, d[0] * 100 + d[1] * 10 + d[2], code)
        wanted.append(jnp.where(lane < 3 * WIDE, code + third * 10 + z, -5000))
    row = lax.broadcasted_iota(jnp.int32, (EDGE, 128), 0)
    column = lax.broadcasted_iota(jnp.int32, (EDGE, 128), 1)
    pick = []
    for t in range(3):
        hit = column * 0 > 0
        for n in range(PER):
            hit = hit | (column == row + (t * WIDE + n * EDGE))
        pick.append((jnp.where(hit, 32.0, 0.0).astype(jnp.bfloat16), jnp.where(hit, 1.0, 0.0).astype(jnp.bfloat16)))

    for copy in copies:
        copy.wait()

    def one(x, carry):
        for s in range(2):
            slots = jnp.zeros((56, 128), F32)
            values = jnp.zeros((1, 128), F32)
            for t in range(3):
                y = 3 * s + t
                entry = neighbors[x, y]
                high = lax.shift_right_arithmetic(entry, 5)
                low = entry & 31
                for part, chosen in zip((high, low), pick[t]):
                    slots = slots + lax.dot_general(
                        part.astype(F32).astype(jnp.bfloat16), chosen, (((0,), (0,)), ((), ())),
                        preferred_element_type=F32,
                    )
                parts = [field[x, y, c : c + 1, :] for c in range(3)]
                parts += [polar[x, y : y + 1, :]]
                parts += [jitter[x, y, c : c + 1, :] for c in range(3)]
                for n in range(PER):
                    wide = jnp.concatenate([parts[n], jnp.zeros((1, 122), F32)], axis=1)
                    start = t * WIDE + n * EDGE
                    values = values + (pltpu.roll(wide, start, 1) if start else wide)
            out[x, 0, s : s + 1, :] = values
            home = (x + 2) * 100 + (2 + 3 * s) * 10 + 2
            for group in range(1, GROUPS):
                target = (wanted[group - 1] + home).astype(F32)
                flag = jnp.max(jnp.where(slots == target, 1.0, 0.0), axis=0, keepdims=True)
                out[x, group, s : s + 1, :] = flag
        return carry

    unrolled(EDGE, 6, one, 0)


def region_kernel(
    own, a1, a2, a3, b1, b2, b3, kept_out, info_out, chan, near, home, coef, moved, basis,
    raw, now, past,
):
    gx = lax.axis_index("gx")
    gy = lax.axis_index("gy")
    lane = lane_iota()
    first, last = third_masks()
    along = lane - jnp.where(last, 2 * WIDE, jnp.where(first, 0, WIDE))
    is_low = (lane * 0 + gx) == 0

    def gather(x, carry):
        half = x // EDGE
        within = x - half * EDGE
        here = within + jnp.where(half == gx, 0, EDGE)
        there = within + jnp.where(half == gx, EDGE, 0)
        for group in range(GROUPS):
            ahead = [jnp.where(is_low, a[here, group], b[there, group]) for a, b in ((a1, b1), (a2, b2), (a3, b3))]
            back = [jnp.where(is_low, b[there, group], a[here, group]) for a, b in ((a3, b3), (a2, b2), (a1, b1))]
            blocks = back + [own[here, group]] + ahead
            outs = [None] * PER
            for gap in range(-6, 7):
                members = [m for m in range(PER) if 0 <= m + gap < PER]
                mixed = blocks[members[0] + gap]
                for m in members[1:]:
                    mixed = jnp.where(along >= 6 * m, blocks[m + gap], mixed)
                mixed = roll_lanes(mixed, -6 * gap)
                for m in members:
                    outs[m] = (
                        mixed if outs[m] is None
                        else jnp.where(along >= 6 * (m + gap), mixed, outs[m])
                    )
            for member in range(PER):
                acc = pltpu.roll(outs[member], 2 * gy, 0)
                if 4 <= group * PER + member < 7:
                    acc = acc * SPACING
                if group * PER + member == 3:
                    acc = jnp.where(lane >= 3 * WIDE, 1.0, acc)
                    chan[x, 35] = 1.0 / acc
                chan[x, group * PER + member] = acc
        return carry

    unrolled(NX, 3, gather, 0)

    def spread(x, carry):
        for c in range(4):
            v = chan[x, 3 + c]
            for step in range(-2, 3):
                near[x, (step + 2) * 4 + c] = shifted(v, step, 0, first, last)
                home[x, (step + 2) * 4 + c] = roll_lanes(v, -step)
        return carry

    unrolled(NX, 6, spread, 0)

    def pairs(x, carry):
        for number, d in sorted(enumerate(FORWARD), key=lambda t: t[1][2]):
            other = wrap(x + d[0])
            place = (d[1] + 2) * 4
            polar, *jit = [home[x, (d[2] + 2) * 4 + c] for c in range(4)]
            sep = [near[other, place + 1 + c] - jit[c] for c in range(3)]
            sep = [t + d[c] * SPACING if d[c] else t for c, t in enumerate(sep)]
            dist_sq = sep[0] * sep[0] + sep[1] * sep[1] + sep[2] * sep[2]
            over = lax.rsqrt(dist_sq)
            cube = dist_sq * dist_sq * over
            over_sq = over * over
            over_cube = over_sq * over
            damping = cube * (THOLE * lax.rsqrt(polar * near[other, place]))
            falloff = jnp.exp2(damping * -LOG2E)
            flag = roll_lanes(chan[x, 7 + number], -d[2])
            iso = (over_cube - falloff * over_cube) * flag
            radial = (3.0 - (3.0 + 3.0 * damping) * falloff) * (over_cube * over_sq)
            root = radial * lax.rsqrt(radial) * flag
            ahead = OFFSETS.index(d) * 4
            behind = OFFSETS.index((-d[0], -d[1], -d[2])) * 4
            for c in range(3):
                coef[x, ahead + c] = sep[c] * root
            coef[x, ahead + 3] = iso
            root = shifted(root, -d[1], d[2], first, last)
            coef[other, behind + 3] = shifted(iso, -d[1], d[2], first, last)
            for c in range(3):
                back = near[x, (2 - d[1]) * 4 + 1 + c] - home[other, (2 - d[2]) * 4 + 1 + c]
                back = back - d[c] * SPACING if d[c] else back
                coef[other, behind + c] = back * root
        return carry

    lax.fori_loop(0, NX, pairs, 0)

    def move(x, c, v):
        for dy in range(-2, 3):
            moved[x, (dy + 2) * 3 + c] = shifted(v, dy, 0, first, last)

    def couple(x):
        acc = {dz: [None] * 3 for dz in range(-2, 3)}
        for dx in range(-2, 3):
            other = wrap(x + dx)
            for dy in range(-2, 3):
                v = [moved[other, (dy + 2) * 3 + c] for c in range(3)]
                for dz in range(-2, 3):
                    if (dx, dy, dz) not in OFFSETS:
                        continue
                    number = OFFSETS.index((dx, dy, dz)) * 4
                    s = [coef[x, number + c] for c in range(3)]
                    iso = coef[x, number + 3]
                    dot = s[0] * v[0] + s[1] * v[1] + s[2] * v[2]
                    new = [s[c] * dot - iso * v[c] for c in range(3)]
                    acc[dz] = [n if t is None else t + n for t, n in zip(acc[dz], new)]
        out = acc[0]
        for dz in (1, -1, 2, -2):
            out = [o + roll_lanes(t, dz) for o, t in zip(out, acc[dz])]
        return out

    zero = jnp.zeros((8, 128), F32)
    slab = (along >= 18) & (along < 24)

    def prepare(x, carry):
        for c in range(3):
            raw[x * 3 + c] = chan[x, 3] * chan[x, c]
            now[x * 3 + c] = zero
            past[x * 3 + c] = zero
        return carry

    unrolled(NX, 12, prepare, 0)

    def next_vector(x, c, al, be, sc):
        return (raw[x * 3 + c] - al * now[x * 3 + c] - be * past[x * 3 + c]) * sc

    def extend(k, carry):
        info, before, al, be, sc = carry
        sums = [zero] * 4

        def scale(x):
            for c in range(3):
                new = next_vector(x, c, al, be, sc)
                past[x * 3 + c] = now[x * 3 + c]
                now[x * 3 + c] = new
                basis[k, x * 3 + c] = new
                move(x, c, new)

        for x in (10, 11, 0, 1, 2):
            scale(x)
        for x in range(NX):
            if 3 <= x + 3 < 10:
                scale(x + 3)
            out = couple(x)
            polar = chan[x, 3]
            over = chan[x, 35]
            for c in range(3):
                u = now[x * 3 + c]
                w = polar * out[c]
                raw[x * 3 + c] = w
                sums[0] = sums[0] + out[c] * u
                sums[1] = sums[1] + out[c] * past[x * 3 + c]
                sums[2] = sums[2] + out[c] * w
                sums[3] = sums[3] + (u * over) * u
        along_now, along_past, full, norm = [total(jnp.where(slab, t, 0.0)) for t in sums]
        live = k > 0
        norm = jnp.where(live, norm, 0.0)
        tiny = 1e-36
        over = jnp.where(norm > tiny, 1.0 / jnp.maximum(norm, tiny), 0.0)
        over_past = jnp.where(before > tiny, 1.0 / jnp.maximum(before, tiny), 0.0)
        al = along_now * over
        be = along_past * over_past
        rest = full - al * along_now - be * along_past
        rest = jnp.maximum(rest, 1e-10 * full)
        good = (rest > tiny) & (norm > tiny)
        sc = jnp.where(good, lax.rsqrt(jnp.maximum(rest * over, 1e-12)), 1.0)
        sc = jnp.maximum(sc, 1e-3)
        inv = 1.0 / sc
        info = jnp.where(lane == 44 + k, jnp.where(live, al, info), info)
        info = jnp.where(lane == 52 + k, jnp.where(live, be, info), info)
        info = jnp.where(lane == 60 + k, jnp.where(live, inv, info), info)
        return info, norm, al, be, sc

    none = jnp.zeros((1, 1), F32)
    info, _, al, be, sc = lax.fori_loop(0, BASIS, extend, (zero, none, none, none, none + 1.0))

    def end(x, carry):
        for c in range(3):
            basis[BASIS, x * 3 + c] = next_vector(x, c, al, be, sc)
        return carry

    unrolled(NX, 12, end, 0)

    number = 0
    for low, high in ((0, 3), (3, BASIS)):
        entries = [(i, j) for i in range(low, high) for j in range(i, BASIS)]

        def one(x, sums):
            sums = list(sums)
            for c in range(3):
                u = {j: basis[j + 1, x * 3 + c] for j in range(low, BASIS)}
                for i in range(low, high):
                    weighted = u[i] * chan[x, 35]
                    for n, (p, q) in enumerate(entries):
                        if p == i:
                            sums[n] = sums[n] + weighted * u[q]
            return tuple(sums)

        sums = unrolled(NX, 2, one, (zero,) * len(entries))
        for n in range(len(entries)):
            info = jnp.where(lane == number, total(jnp.where(slab, sums[n], 0.0)), info)
            number += 1

    for e in range(16):
        info_out[e] = info

    def keep(x, carry):
        far = x + EDGE * gx

        def front(v):
            return pltpu.roll(v, 8 - 2 * gy, 0)

        for c in range(3):
            for k in range(BASIS):
                kept_out[x, k * 3 + c] = front(basis[k + 1, far * 3 + c])
            kept_out[x, 27 + c] = front(basis[0, far * 3 + c])
        kept_out[x, 30] = front(chan[far, 35])
        return carry

    unrolled(EDGE, 2, keep, 0)


def finish_kernel(kept, info, dip_out, res_out, len_out):
    gz = lax.axis_index("gz_0") * 4 + lax.axis_index("gz_1")
    table = jnp.concatenate([info[e, 0:1, :] for e in range(16)], axis=0)
    wide = (2, 8, 128)

    def column(n):
        return jnp.broadcast_to(table[:, n : n + 1], (16, 128)).reshape(wide)

    rows = {}
    number = 0
    for low, high in ((0, 3), (3, BASIS)):
        for i in range(low, high):
            for j in range(i, BASIS):
                rows[i, j] = rows[j, i] = column(number)
                number += 1
    al = [column(45 + k) for k in range(ITERS)]
    be = [column(53 + k) for k in range(ITERS)]
    inv = [column(61 + k) for k in range(ITERS)]
    zero = jnp.zeros(wide, F32)
    slab = lax.broadcasted_iota(jnp.int32, wide, 0) * 8 + lax.broadcasted_iota(jnp.int32, wide, 1)
    lane = lax.broadcasted_iota(jnp.int32, (8, 128), 1)

    def summed(v):
        t = v[0] + v[1]
        for by in (4, 2, 1):
            t = t + pltpu.roll(t, by, 0)
        return t

    def form(left, right, size_left, size_right):
        acc = zero
        for i in range(size_left):
            inner = rows[i, 0] * right[0]
            for j in range(1, size_right):
                inner = inner + rows[i, j] * right[j]
            acc = acc + left[i] * inner
        return summed(acc)

    search = [zero + 1.0] + [zero] * ITERS
    resid = [zero + 1.0] + [zero] * ITERS
    moves = [zero] * BASIS
    gamma = summed(rows[0, 0])
    lengths = jnp.zeros((8, 128), F32)
    for k in range(ITERS):
        image = list(search)
        for j in range(k + 1):
            image[j] = image[j] - al[j] * search[j]
            image[j + 1] = image[j + 1] - inv[j] * search[j]
            if j:
                image[j - 1] = image[j - 1] - be[j] * search[j]
        step = gamma / form(search, image, k + 1, k + 2)
        lengths = jnp.where(lane == k, step, lengths)
        moves = [moves[j] + step[None] * search[j] if j <= k else moves[j] for j in range(BASIS)]
        resid = [resid[j] - step[None] * image[j] if j <= k + 1 else resid[j] for j in range(BASIS)]
        if k + 1 < ITERS:
            after = form(resid, resid, k + 2, k + 2)
            ratio = after / gamma
            search = [resid[j] + ratio[None] * search[j] if j <= k + 1 else zero for j in range(BASIS)]
            gamma = after
    len_out[...] = lengths[0:1, :ITERS]
    here = slab == gz
    moves = [summed(jnp.where(here, v, 0.0)) for v in moves]
    resid = [summed(jnp.where(here, v, 0.0)) for v in resid]
    for x in range(EDGE):
        for c in range(3):
            dip = kept[x, 27 + c]
            res = jnp.zeros((8, 128), F32)
            for k in range(BASIS):
                u = kept[x, k * 3 + c]
                if k < ITERS:
                    dip = dip + moves[k] * u
                res = res + resid[k] * u
            res = res * kept[x, 30]
            for out, v in ((dip_out, dip), (res_out, res)):
                for t in range(3):
                    w = roll_lanes(v, t * WIDE + 18)
                    for s in range(2):
                        out[x, 3 * s + t, c : c + 1, :] = w[s : s + 1, :EDGE]


def per_device(permanent_field, polar, jitter, neighbors):
    packed = pl.pallas_call(
        pack_kernel,
        out_shape=jax.ShapeDtypeStruct((EDGE, GROUPS, 2, 128), F32),
        in_specs=[pl.BlockSpec(memory_space=pltpu.HBM)] * 4,
        scratch_shapes=[
            pltpu.VMEM((EDGE, EDGE, 3, EDGE), F32),
            pltpu.VMEM((EDGE, EDGE, EDGE), F32),
            pltpu.VMEM((EDGE, EDGE, 3, EDGE), F32),
            pltpu.VMEM((EDGE, EDGE, EDGE, 56), jnp.int32),
            pltpu.SemaphoreType.DMA((4,)),
        ],
        compiler_params=pltpu.CompilerParams(vmem_limit_bytes=8 * 1024 * 1024),
        name="pack",
    )(*(pltpu.with_memory_space_constraint(v, pltpu.HBM) for v in (permanent_field.transpose(0, 1, 3, 2), polar, jitter.transpose(0, 1, 3, 2), neighbors)))

    around = [packed] + [
        lax.ppermute(packed, "gy", [((i + k) % 4, i) for i in range(4)]) for k in (1, 2, 3)
    ]
    half = jnp.concatenate(around, axis=2)

    def swap(v):
        return lax.ppermute(v, "gx", [(0, 1), (1, 0)])

    own = jnp.concatenate([half, swap(half)], axis=0)

    def fetch(k):
        pairs = [((i + k) % 16, i) for i in range(16)]
        pairs += [(16 + (i - k) % 16, 16 + i) for i in range(16)]
        return lax.ppermute(own, ("gx",) + GZ, pairs)

    direct = [fetch(k) for k in (1, 2, 3)]
    passed = [swap(v) for v in direct]

    vreg = (8, 128)
    kept, info = pl.pallas_call(
        region_kernel,
        out_shape=(
            jax.ShapeDtypeStruct((EDGE, 31) + vreg, F32),
            jax.ShapeDtypeStruct((16,) + vreg, F32),
        ),
        scratch_shapes=[
            pltpu.VMEM((NX, 36) + vreg, F32),
            pltpu.VMEM((NX, 20) + vreg, F32),
            pltpu.VMEM((NX, 20) + vreg, F32),
            pltpu.VMEM((NX, 4 * len(OFFSETS)) + vreg, F32),
            pltpu.VMEM((NX, 16) + vreg, F32),
            pltpu.VMEM((BASIS + 1, 3 * NX) + vreg, F32),
            pltpu.VMEM((3 * NX,) + vreg, F32),
            pltpu.VMEM((3 * NX,) + vreg, F32),
            pltpu.VMEM((3 * NX,) + vreg, F32),
        ],
        compiler_params=pltpu.CompilerParams(vmem_limit_bytes=36 * 1024 * 1024),
        name="region",
    )(own, *direct, *passed)

    info = lax.all_to_all(info, GZ, 0, 0, tiled=True)

    dip, res, lengths = pl.pallas_call(
        finish_kernel,
        out_shape=(
            jax.ShapeDtypeStruct((EDGE, EDGE, 3, EDGE), F32),
            jax.ShapeDtypeStruct((EDGE, EDGE, 3, EDGE), F32),
            jax.ShapeDtypeStruct((1, ITERS), F32),
        ),
        compiler_params=pltpu.CompilerParams(vmem_limit_bytes=8 * 1024 * 1024),
        name="finish",
    )(kept, info)
    return dip.transpose(0, 1, 3, 2), res.transpose(0, 1, 3, 2), lengths.reshape(ITERS)


def solution(mesh):
    finer = Mesh(
        mesh.devices.reshape(mesh.shape["gx"], mesh.shape["gy"], 4, 4), ("gx", "gy", "gz_0", "gz_1")
    )
    return jax.shard_map(
        per_device,
        mesh=finer,
        in_specs=(
            P("gx", "gy", GZ, None),
            P("gx", "gy", GZ),
            P("gx", "gy", GZ, None),
            P("gx", "gy", GZ, None),
        ),
        out_specs=(P("gx", "gy", GZ, None), P("gx", "gy", GZ, None), P()),
        check_vma=False,
    )
```

```python
import jax
import jax.numpy as jnp
from jax import lax
from jax.experimental import pallas as pl
from jax.experimental.pallas import tpu as pltpu
from jax.sharding import Mesh
from jax.sharding import PartitionSpec as P

ITERS = 8
BASIS = ITERS + 1
THOLE = 0.39
SPACING = 3.5
LOG2E = 1.4426950408889634
EDGE = 6
NX = 12
WIDE = 42
GZ = ("gz_0", "gz_1")
F32 = jnp.float32

OFFSETS = [
    (a, b, c)
    for a in range(-2, 3)
    for b in range(-2, 3)
    for c in range(-2, 3)
    if 1 <= a * a + b * b + c * c <= 5
]
FORWARD = [d for d in OFFSETS if d > (0, 0, 0)]
GROUPS, PER = 5, 7


def lane_iota():
    return lax.broadcasted_iota(jnp.int32, (8, 128), 1)


def third_masks():
    lane = lane_iota()
    return lane < WIDE, lane >= 2 * WIDE


def roll_lanes(v, ahead):
    ahead = ahead % 128
    return v if ahead == 0 else pltpu.roll(v, 128 - ahead, 1)


def roll_rows(v, ahead):
    return pltpu.roll(v, (-ahead) % 8, 0)


def shifted(v, dy, dz, first, last):
    if dy == 0:
        return roll_lanes(v, dz)
    if dy == 1:
        return jnp.where(
            last, roll_rows(roll_lanes(v, dz - 2 * WIDE), 1), roll_lanes(v, dz + WIDE)
        )
    if dy == 2:
        return jnp.where(
            first, roll_lanes(v, dz + 2 * WIDE), roll_rows(roll_lanes(v, dz - WIDE), 1)
        )
    if dy == -1:
        return jnp.where(
            first, roll_rows(roll_lanes(v, dz + 2 * WIDE), -1), roll_lanes(v, dz - WIDE)
        )
    return jnp.where(
        last, roll_lanes(v, dz - 2 * WIDE), roll_rows(roll_lanes(v, dz + WIDE), -1)
    )


def wrap(x):
    if isinstance(x, int):
        return x % NX
    return jnp.where(x >= NX, x - NX, jnp.where(x < 0, x + NX, x))


def total(v):
    return jnp.sum(jnp.sum(v, axis=0, keepdims=True), axis=1, keepdims=True)


def unrolled(count, times, body, carry):
    def several(i, carry):
        for t in range(times):
            carry = body(i * times + t, carry)
        return carry

    return lax.fori_loop(0, count // times, several, carry)


def pack_kernel(
    field_in, polar_in, jitter_in, neighbors_in, out, field, polar, jitter, neighbors, arrived
):
    given = (neighbors_in, field_in, jitter_in, polar_in)
    kept = (neighbors, field, jitter, polar)
    copies = [pltpu.make_async_copy(g, k, arrived.at[n]) for n, (g, k) in enumerate(zip(given, kept))]
    for copy in copies:
        copy.start()
    lane = lax.broadcasted_iota(jnp.int32, (1, 128), 1)
    third = jnp.where(lane >= 2 * WIDE, 2, jnp.where(lane >= WIDE, 1, 0))
    inside = lane - third * WIDE
    member = inside // EDGE
    z = inside - member * EDGE
    wanted = []
    for group in range(1, GROUPS):
        code = jnp.full((1, 128), -5000, jnp.int32)
        for n in range(PER):
            d = FORWARD[(group - 1) * PER + n]
            code = jnp.where(member == n, d[0] * 100 + d[1] * 10 + d[2], code)
        wanted.append(jnp.where(lane < 3 * WIDE, code + third * 10 + z, -5000))
    row = lax.broadcasted_iota(jnp.int32, (EDGE, 128), 0)
    column = lax.broadcasted_iota(jnp.int32, (EDGE, 128), 1)
    pick = []
    for t in range(3):
        hit = column * 0 > 0
        for n in range(PER):
            hit = hit | (column == row + (t * WIDE + n * EDGE))
        pick.append((jnp.where(hit, 32.0, 0.0).astype(jnp.bfloat16), jnp.where(hit, 1.0, 0.0).astype(jnp.bfloat16)))

    for copy in copies:
        copy.wait()

    def one(x, carry):
        for s in range(2):
            slots = jnp.zeros((56, 128), F32)
            values = jnp.zeros((1, 128), F32)
            for t in range(3):
                y = 3 * s + t
                entry = neighbors[x, y]
                high = lax.shift_right_arithmetic(entry, 5)
                low = entry & 31
                for part, chosen in zip((high, low), pick[t]):
                    slots = slots + lax.dot_general(
                        part.astype(F32).astype(jnp.bfloat16), chosen, (((0,), (0,)), ((), ())),
                        preferred_element_type=F32,
                    )
                parts = [field[x, y, c : c + 1, :] for c in range(3)]
                parts += [polar[x, y : y + 1, :]]
                parts += [jitter[x, y, c : c + 1, :] for c in range(3)]
                for n in range(PER):
                    wide = jnp.concatenate([parts[n], jnp.zeros((1, 122), F32)], axis=1)
                    start = t * WIDE + n * EDGE
                    values = values + (pltpu.roll(wide, start, 1) if start else wide)
            out[x, 0, s : s + 1, :] = values
            home = (x + 2) * 100 + (2 + 3 * s) * 10 + 2
            for group in range(1, GROUPS):
                target = (wanted[group - 1] + home).astype(F32)
                flag = jnp.max(jnp.where(slots == target, 1.0, 0.0), axis=0, keepdims=True)
                out[x, group, s : s + 1, :] = flag
        return carry

    unrolled(EDGE, 6, one, 0)


def region_kernel(
    own, a1, a2, a3, b1, b2, b3, kept_out, info_out, chan, near, home, coef, moved, basis,
    raw, now, past,
):
    gx = lax.axis_index("gx")
    gy = lax.axis_index("gy")
    lane = lane_iota()
    first, last = third_masks()
    along = lane - jnp.where(last, 2 * WIDE, jnp.where(first, 0, WIDE))
    is_low = (lane * 0 + gx) == 0

    def gather(x, carry):
        half = x // EDGE
        within = x - half * EDGE
        here = within + jnp.where(half == gx, 0, EDGE)
        there = within + jnp.where(half == gx, EDGE, 0)
        for group in range(GROUPS):
            ahead = [jnp.where(is_low, a[here, group], b[there, group]) for a, b in ((a1, b1), (a2, b2), (a3, b3))]
            back = [jnp.where(is_low, b[there, group], a[here, group]) for a, b in ((a3, b3), (a2, b2), (a1, b1))]
            blocks = back + [own[here, group]] + ahead
            outs = [None] * PER
            for gap in range(-6, 7):
                members = [m for m in range(PER) if 0 <= m + gap < PER]
                mixed = blocks[members[0] + gap]
                for m in members[1:]:
                    mixed = jnp.where(along >= 6 * m, blocks[m + gap], mixed)
                mixed = roll_lanes(mixed, -6 * gap)
                for m in members:
                    outs[m] = (
                        mixed if outs[m] is None
                        else jnp.where(along >= 6 * (m + gap), mixed, outs[m])
                    )
            for member in range(PER):
                acc = pltpu.roll(outs[member], 2 * gy, 0)
                if 4 <= group * PER + member < 7:
                    acc = acc * SPACING
                if group * PER + member == 3:
                    acc = jnp.where(lane >= 3 * WIDE, 1.0, acc)
                    chan[x, 35] = 1.0 / acc
                chan[x, group * PER + member] = acc
        return carry

    unrolled(NX, 3, gather, 0)

    def spread(x, carry):
        for c in range(4):
            v = chan[x, 3 + c]
            for step in range(-2, 3):
                near[x, (step + 2) * 4 + c] = shifted(v, step, 0, first, last)
                home[x, (step + 2) * 4 + c] = roll_lanes(v, -step)
        return carry

    unrolled(NX, 6, spread, 0)

    def pairs(x, carry):
        for number, d in sorted(enumerate(FORWARD), key=lambda t: t[1][2]):
            other = wrap(x + d[0])
            place = (d[1] + 2) * 4
            polar, *jit = [home[x, (d[2] + 2) * 4 + c] for c in range(4)]
            sep = [near[other, place + 1 + c] - jit[c] for c in range(3)]
            sep = [t + d[c] * SPACING if d[c] else t for c, t in enumerate(sep)]
            dist_sq = sep[0] * sep[0] + sep[1] * sep[1] + sep[2] * sep[2]
            over = lax.rsqrt(dist_sq)
            cube = dist_sq * dist_sq * over
            over_sq = over * over
            over_cube = over_sq * over
            damping = cube * (THOLE * lax.rsqrt(polar * near[other, place]))
            falloff = jnp.exp2(damping * -LOG2E)
            flag = roll_lanes(chan[x, 7 + number], -d[2])
            iso = (over_cube - falloff * over_cube) * flag
            radial = (3.0 - (3.0 + 3.0 * damping) * falloff) * (over_cube * over_sq)
            root = radial * lax.rsqrt(radial) * flag
            ahead = OFFSETS.index(d) * 4
            behind = OFFSETS.index((-d[0], -d[1], -d[2])) * 4
            for c in range(3):
                coef[x, ahead + c] = sep[c] * root
            coef[x, ahead + 3] = iso
            root = shifted(root, -d[1], d[2], first, last)
            coef[other, behind + 3] = shifted(iso, -d[1], d[2], first, last)
            for c in range(3):
                back = near[x, (2 - d[1]) * 4 + 1 + c] - home[other, (2 - d[2]) * 4 + 1 + c]
                back = back - d[c] * SPACING if d[c] else back
                coef[other, behind + c] = back * root
        return carry

    lax.fori_loop(0, NX, pairs, 0)

    def move(x, c, v):
        for dy in range(-2, 3):
            moved[x, (dy + 2) * 3 + c] = shifted(v, dy, 0, first, last)

    def couple(x):
        acc = {dz: [None] * 3 for dz in range(-2, 3)}
        for dx in range(-2, 3):
            other = wrap(x + dx)
            for dy in range(-2, 3):
                v = [moved[other, (dy + 2) * 3 + c] for c in range(3)]
                for dz in range(-2, 3):
                    if (dx, dy, dz) not in OFFSETS:
                        continue
                    number = OFFSETS.index((dx, dy, dz)) * 4
                    s = [coef[x, number + c] for c in range(3)]
                    iso = coef[x, number + 3]
                    dot = s[0] * v[0] + s[1] * v[1] + s[2] * v[2]
                    new = [s[c] * dot - iso * v[c] for c in range(3)]
                    acc[dz] = [n if t is None else t + n for t, n in zip(acc[dz], new)]
        out = acc[0]
        for dz in (1, -1, 2, -2):
            out = [o + roll_lanes(t, dz) for o, t in zip(out, acc[dz])]
        return out

    zero = jnp.zeros((8, 128), F32)
    slab = (along >= 18) & (along < 24)

    def prepare(x, carry):
        for c in range(3):
            raw[x * 3 + c] = chan[x, 3] * chan[x, c]
            now[x * 3 + c] = zero
            past[x * 3 + c] = zero
        return carry

    unrolled(NX, 12, prepare, 0)

    def next_vector(x, c, al, be, sc):
        return (raw[x * 3 + c] - al * now[x * 3 + c] - be * past[x * 3 + c]) * sc

    def extend(k, carry):
        info, before, al, be, sc = carry
        sums = [zero] * 4

        def scale(x):
            for c in range(3):
                new = next_vector(x, c, al, be, sc)
                past[x * 3 + c] = now[x * 3 + c]
                now[x * 3 + c] = new
                basis[k, x * 3 + c] = new
                move(x, c, new)

        for x in (10, 11, 0, 1, 2):
            scale(x)
        for x in range(NX):
            if 3 <= x + 3 < 10:
                scale(x + 3)
            out = couple(x)
            polar = chan[x, 3]
            over = chan[x, 35]
            for c in range(3):
                u = now[x * 3 + c]
                w = polar * out[c]
                raw[x * 3 + c] = w
                sums[0] = sums[0] + out[c] * u
                sums[1] = sums[1] + out[c] * past[x * 3 + c]
                sums[2] = sums[2] + out[c] * w
                sums[3] = sums[3] + (u * over) * u
        along_now, along_past, full, norm = [total(jnp.where(slab, t, 0.0)) for t in sums]
        live = k > 0
        norm = jnp.where(live, norm, 0.0)
        tiny = 1e-36
        over = jnp.where(norm > tiny, 1.0 / jnp.maximum(norm, tiny), 0.0)
        over_past = jnp.where(before > tiny, 1.0 / jnp.maximum(before, tiny), 0.0)
        al = along_now * over
        be = along_past * over_past
        rest = full - al * along_now - be * along_past
        rest = jnp.maximum(rest, 1e-10 * full)
        good = (rest > tiny) & (norm > tiny)
        sc = jnp.where(good, lax.rsqrt(jnp.maximum(rest * over, 1e-12)), 1.0)
        sc = jnp.maximum(sc, 1e-3)
        inv = 1.0 / sc
        info = jnp.where(lane == 44 + k, jnp.where(live, al, info), info)
        info = jnp.where(lane == 52 + k, jnp.where(live, be, info), info)
        info = jnp.where(lane == 60 + k, jnp.where(live, inv, info), info)
        return info, norm, al, be, sc

    none = jnp.zeros((1, 1), F32)
    info, _, al, be, sc = lax.fori_loop(0, BASIS, extend, (zero, none, none, none, none + 1.0))

    def end(x, carry):
        for c in range(3):
            basis[BASIS, x * 3 + c] = next_vector(x, c, al, be, sc)
        return carry

    unrolled(NX, 12, end, 0)

    number = 0
    for low, high in ((0, 3), (3, BASIS)):
        entries = [(i, j) for i in range(low, high) for j in range(i, BASIS)]

        def one(x, sums):
            sums = list(sums)
            for c in range(3):
                u = {j: basis[j + 1, x * 3 + c] for j in range(low, BASIS)}
                for i in range(low, high):
                    weighted = u[i] * chan[x, 35]
                    for n, (p, q) in enumerate(entries):
                        if p == i:
                            sums[n] = sums[n] + weighted * u[q]
            return tuple(sums)

        sums = unrolled(NX, 3, one, (zero,) * len(entries))
        for n in range(len(entries)):
            info = jnp.where(lane == number, total(jnp.where(slab, sums[n], 0.0)), info)
            number += 1

    for e in range(16):
        info_out[e] = info

    def keep(x, carry):
        far = x + EDGE * gx

        def front(v):
            return pltpu.roll(v, 8 - 2 * gy, 0)

        for c in range(3):
            for k in range(BASIS):
                kept_out[x, k * 3 + c] = front(basis[k + 1, far * 3 + c])
            kept_out[x, 27 + c] = front(basis[0, far * 3 + c])
        kept_out[x, 30] = front(chan[far, 35])
        return carry

    unrolled(EDGE, 6, keep, 0)


def finish_kernel(kept, info, dip_out, res_out, len_out):
    gz = lax.axis_index("gz_0") * 4 + lax.axis_index("gz_1")
    table = jnp.concatenate([info[e, 0:1, :] for e in range(16)], axis=0)
    wide = (2, 8, 128)

    def column(n):
        return jnp.broadcast_to(table[:, n : n + 1], (16, 128)).reshape(wide)

    rows = {}
    number = 0
    for low, high in ((0, 3), (3, BASIS)):
        for i in range(low, high):
            for j in range(i, BASIS):
                rows[i, j] = rows[j, i] = column(number)
                number += 1
    al = [column(45 + k) for k in range(ITERS)]
    be = [column(53 + k) for k in range(ITERS)]
    inv = [column(61 + k) for k in range(ITERS)]
    zero = jnp.zeros(wide, F32)
    slab = lax.broadcasted_iota(jnp.int32, wide, 0) * 8 + lax.broadcasted_iota(jnp.int32, wide, 1)
    lane = lax.broadcasted_iota(jnp.int32, (8, 128), 1)

    def summed(v):
        t = v[0] + v[1]
        for by in (4, 2, 1):
            t = t + pltpu.roll(t, by, 0)
        return t

    def form(left, right, size_left, size_right):
        acc = zero
        for i in range(size_left):
            inner = rows[i, 0] * right[0]
            for j in range(1, size_right):
                inner = inner + rows[i, j] * right[j]
            acc = acc + left[i] * inner
        return summed(acc)

    search = [zero + 1.0] + [zero] * ITERS
    resid = [zero + 1.0] + [zero] * ITERS
    moves = [zero] * BASIS
    gamma = summed(rows[0, 0])
    lengths = jnp.zeros((8, 128), F32)
    for k in range(ITERS):
        image = list(search)
        for j in range(k + 1):
            image[j] = image[j] - al[j] * search[j]
            image[j + 1] = image[j + 1] - inv[j] * search[j]
            if j:
                image[j - 1] = image[j - 1] - be[j] * search[j]
        step = gamma / form(search, image, k + 1, k + 2)
        lengths = jnp.where(lane == k, step, lengths)
        moves = [moves[j] + step[None] * search[j] if j <= k else moves[j] for j in range(BASIS)]
        resid = [resid[j] - step[None] * image[j] if j <= k + 1 else resid[j] for j in range(BASIS)]
        if k + 1 < ITERS:
            after = form(resid, resid, k + 2, k + 2)
            ratio = after / gamma
            search = [resid[j] + ratio[None] * search[j] if j <= k + 1 else zero for j in range(BASIS)]
            gamma = after
    len_out[...] = lengths[0:1, :ITERS]
    here = slab == gz
    moves = [summed(jnp.where(here, v, 0.0)) for v in moves]
    resid = [summed(jnp.where(here, v, 0.0)) for v in resid]
    for x in range(EDGE):
        for c in range(3):
            dip = kept[x, 27 + c]
            res = jnp.zeros((8, 128), F32)
            for k in range(BASIS):
                u = kept[x, k * 3 + c]
                if k < ITERS:
                    dip = dip + moves[k] * u
                res = res + resid[k] * u
            res = res * kept[x, 30]
            for out, v in ((dip_out, dip), (res_out, res)):
                for t in range(3):
                    w = roll_lanes(v, t * WIDE + 18)
                    for s in range(2):
                        out[x, 3 * s + t, c : c + 1, :] = w[s : s + 1, :EDGE]


def per_device(permanent_field, polar, jitter, neighbors):
    packed = pl.pallas_call(
        pack_kernel,
        out_shape=jax.ShapeDtypeStruct((EDGE, GROUPS, 2, 128), F32),
        in_specs=[pl.BlockSpec(memory_space=pltpu.HBM)] * 4,
        scratch_shapes=[
            pltpu.VMEM((EDGE, EDGE, 3, EDGE), F32),
            pltpu.VMEM((EDGE, EDGE, EDGE), F32),
            pltpu.VMEM((EDGE, EDGE, 3, EDGE), F32),
            pltpu.VMEM((EDGE, EDGE, EDGE, 56), jnp.int32),
            pltpu.SemaphoreType.DMA((4,)),
        ],
        compiler_params=pltpu.CompilerParams(vmem_limit_bytes=8 * 1024 * 1024),
        name="pack",
    )(*(pltpu.with_memory_space_constraint(v, pltpu.HBM) for v in (permanent_field.transpose(0, 1, 3, 2), polar, jitter.transpose(0, 1, 3, 2), neighbors)))

    around = [packed] + [
        lax.ppermute(packed, "gy", [((i + k) % 4, i) for i in range(4)]) for k in (1, 2, 3)
    ]
    half = jnp.concatenate(around, axis=2)

    def swap(v):
        return lax.ppermute(v, "gx", [(0, 1), (1, 0)])

    own = jnp.concatenate([half, swap(half)], axis=0)

    def fetch(k):
        pairs = [((i + k) % 16, i) for i in range(16)]
        pairs += [(16 + (i - k) % 16, 16 + i) for i in range(16)]
        return lax.ppermute(own, ("gx",) + GZ, pairs)

    direct = [fetch(k) for k in (1, 2, 3)]
    passed = [swap(v) for v in direct]

    vreg = (8, 128)
    kept, info = pl.pallas_call(
        region_kernel,
        out_shape=(
            jax.ShapeDtypeStruct((EDGE, 31) + vreg, F32),
            jax.ShapeDtypeStruct((16,) + vreg, F32),
        ),
        scratch_shapes=[
            pltpu.VMEM((NX, 36) + vreg, F32),
            pltpu.VMEM((NX, 20) + vreg, F32),
            pltpu.VMEM((NX, 20) + vreg, F32),
            pltpu.VMEM((NX, 4 * len(OFFSETS)) + vreg, F32),
            pltpu.VMEM((NX, 16) + vreg, F32),
            pltpu.VMEM((BASIS + 1, 3 * NX) + vreg, F32),
            pltpu.VMEM((3 * NX,) + vreg, F32),
            pltpu.VMEM((3 * NX,) + vreg, F32),
            pltpu.VMEM((3 * NX,) + vreg, F32),
        ],
        compiler_params=pltpu.CompilerParams(vmem_limit_bytes=36 * 1024 * 1024),
        name="region",
    )(own, *direct, *passed)

    info = lax.all_to_all(info, GZ, 0, 0, tiled=True)

    dip, res, lengths = pl.pallas_call(
        finish_kernel,
        out_shape=(
            jax.ShapeDtypeStruct((EDGE, EDGE, 3, EDGE), F32),
            jax.ShapeDtypeStruct((EDGE, EDGE, 3, EDGE), F32),
            jax.ShapeDtypeStruct((1, ITERS), F32),
        ),
        compiler_params=pltpu.CompilerParams(vmem_limit_bytes=8 * 1024 * 1024),
        name="finish",
    )(kept, info)
    return dip.transpose(0, 1, 3, 2), res.transpose(0, 1, 3, 2), lengths.reshape(ITERS)


def solution(mesh):
    finer = Mesh(
        mesh.devices.reshape(mesh.shape["gx"], mesh.shape["gy"], 4, 4), ("gx", "gy", "gz_0", "gz_1")
    )
    return jax.shard_map(
        per_device,
        mesh=finer,
        in_specs=(
            P("gx", "gy", GZ, None),
            P("gx", "gy", GZ),
            P("gx", "gy", GZ, None),
            P("gx", "gy", GZ, None),
        ),
        out_specs=(P("gx", "gy", GZ, None), P("gx", "gy", GZ, None), P()),
        check_vma=False,
    )
```
